32 devices in a mesh: member: 1 (over z), ty: 4 (over y), tx: 4 (over x), panel: 2 (over core).
Axes of the slice: x: 4, y: 4, z: 1, core: 2. Of those that a mesh axis runs over, the one named last changes fastest.
The devices are a block of a 4x4x8 slice.
Arguments:
- tracer: float32 [6, 1440, 1440], P(('member', 'panel'), 'tx', 'ty')
- wind_a: float32 [6, 1440, 1440], P('panel', 'tx', 'ty')
- wind_b: float32 [6, 1440, 1440], P('panel', 'tx', 'ty')
- wind_scale: float32 [16], replicated
Outputs:
- output: float32 [6, 1440, 1440], P(('member', 'panel'), 'tx', 'ty')
All inputs are finite; a program needn't handle non-finite values.
Results may differ from the reference program's by a relative error of at most 0.001.
Values sent between devices are 32-bit elements.
A program may use at most 768 MiB of HBM per device.

```python
import math
import jax
import jax.numpy as jnp
from jax import lax

N = 1440
STEPS = 16

C_SPEED = 2.5
CFL_STEP = 0.12
DALPHA = 0.5 * math.pi / N
DT = CFL_STEP * DALPHA
EDGE_TABLE = (
    ((3, 1, 0), (1, 0, 0), (5, 3, 0), (4, 2, 0)),
    ((0, 1, 0), (2, 0, 0), (5, 1, 1), (4, 1, 0)),
    ((1, 1, 0), (3, 0, 0), (5, 2, 1), (4, 3, 1)),
    ((2, 1, 0), (0, 0, 0), (5, 0, 0), (4, 0, 1)),
    ((3, 3, 1), (1, 3, 0), (0, 3, 0), (2, 3, 1)),
    ((3, 2, 0), (1, 2, 1), (2, 2, 1), (0, 2, 0)),
)
TANGENT_A = ((0.0, 1.0, 0.0), (-1.0, 0.0, 0.0), (0.0, -1.0, 0.0), (1.0, 0.0, 0.0), (0.0, 1.0, 0.0), (0.0, 1.0, 0.0))
TANGENT_B = ((0.0, 0.0, 1.0), (0.0, 0.0, 1.0), (0.0, 0.0, 1.0), (0.0, 0.0, 1.0), (-1.0, 0.0, 0.0), (1.0, 0.0, 0.0))


def edge_sign(side_id, edge_id):
    out_sign = 1.0 if edge_id in (1, 3) else -1.0
    return out_sign if side_id in (0, 2) else -out_sign


def out_strips(field_a, field_b):
    return (field_a[:, 0:2, :],
            jnp.flip(field_a[:, -2:, :], axis=1),
            jnp.swapaxes(field_b[:, :, 0:2], 1, 2),
            jnp.swapaxes(jnp.flip(field_b[:, :, -2:], axis=2), 1, 2))


def to_blocks(ghosts):
    return (jnp.flip(ghosts[0], axis=1), ghosts[1],
            jnp.swapaxes(jnp.flip(ghosts[2], axis=1), 1, 2), jnp.swapaxes(ghosts[3], 1, 2))


def sphere_blocks(field_a, field_b, signed):
    strips = out_strips(field_a, field_b)
    ghosts = []
    for side_id in range(4):
        per_panel = []
        for panel_id in range(6):
            src_panel, edge_id, flipped = EDGE_TABLE[panel_id][side_id]
            one_strip = strips[edge_id][src_panel]
            if flipped:
                one_strip = jnp.flip(one_strip, axis=1)
            if signed:
                one_strip = edge_sign(side_id, edge_id) * one_strip
            per_panel.append(one_strip)
        ghosts.append(jnp.stack(per_panel))
    return to_blocks(ghosts)


def extend_field(field_now, blocks):
    return (jnp.concatenate([blocks[0], field_now, blocks[1]], axis=1),
            jnp.concatenate([blocks[2], field_now, blocks[3]], axis=2))


def wind_faces(blocks, wind_a, wind_b):
    ext_a = jnp.concatenate([blocks[0][:, 1:2, :], wind_a, blocks[1][:, 0:1, :]], axis=1)
    ext_b = jnp.concatenate([blocks[2][:, :, 1:2], wind_b, blocks[3][:, :, 0:1]], axis=2)
    return 0.5 * (ext_a[:, :-1, :] + ext_a[:, 1:, :]), 0.5 * (ext_b[:, :, :-1] + ext_b[:, :, 1:])


def face_flux_div(ext_arr, wind_face, step_scale, axis_id):
    face_count = ext_arr.shape[axis_id] - 3
    far_left = lax.slice_in_dim(ext_arr, 0, face_count, axis=axis_id)
    near_left = lax.slice_in_dim(ext_arr, 1, face_count + 1, axis=axis_id)
    near_right = lax.slice_in_dim(ext_arr, 2, face_count + 2, axis=axis_id)
    far_right = lax.slice_in_dim(ext_arr, 3, face_count + 3, axis=axis_id)
    face_val = (7.0 * (near_left + near_right) - (far_left + far_right)) / 12.0
    face_flux = step_scale * wind_face * face_val - (0.5 * C_SPEED) * (near_right - near_left)
    return (lax.slice_in_dim(face_flux, 1, face_count, axis=axis_id)
            - lax.slice_in_dim(face_flux, 0, face_count - 1, axis=axis_id))


def tendency(ext_a, ext_b, face_a, face_b, step_scale, inv_area):
    div_total = face_flux_div(ext_a, face_a, step_scale, 1) + face_flux_div(ext_b, face_b, step_scale, 2)
    return -div_total * inv_area


def inverse_area(row_ids, col_ids, cells):
    dalpha = 0.5 * math.pi / cells
    tan_a = jnp.tan((row_ids.astype(jnp.float32) + 0.5) * dalpha - 0.25 * math.pi)[:, None]
    tan_b = jnp.tan((col_ids.astype(jnp.float32) + 0.5) * dalpha - 0.25 * math.pi)[None, :]
    r_sq = 1.0 + tan_a * tan_a + tan_b * tan_b
    sqrt_g = (1.0 + tan_a * tan_a) * (1.0 + tan_b * tan_b) / (r_sq * jnp.sqrt(r_sq))
    return 1.0 / (dalpha * sqrt_g)


def sphere_points():
    centre_tan = jnp.tan((jnp.arange(N, dtype=jnp.float32) + 0.5) * DALPHA - 0.25 * math.pi)
    tan_a = jnp.broadcast_to(centre_tan[:, None], (N, N))
    tan_b = jnp.broadcast_to(centre_tan[None, :], (N, N))
    ones_grid = jnp.ones((N, N), jnp.float32)
    comp_x = jnp.stack([ones_grid, -tan_a, -ones_grid, tan_a, -tan_b, tan_b])
    comp_y = jnp.stack([tan_a, ones_grid, -tan_a, -ones_grid, tan_a, tan_a])
    comp_z = jnp.stack([tan_b, tan_b, tan_b, tan_b, ones_grid, -ones_grid])
    cube_pts = jnp.stack([comp_x, comp_y, comp_z], axis=-1)
    return tan_a, tan_b, cube_pts / jnp.linalg.norm(cube_pts, axis=-1, keepdims=True)


def flux_winds(tan_a, tan_b, velocity):
    along_a = jnp.sum(velocity * jnp.array(TANGENT_A, jnp.float32)[:, None, None, :], axis=-1)
    along_b = jnp.sum(velocity * jnp.array(TANGENT_B, jnp.float32)[:, None, None, :], axis=-1)
    sq_a = tan_a * tan_a
    sq_b = tan_b * tan_b
    r_sq = 1.0 + sq_a + sq_b
    cross_ab = tan_a * tan_b
    wind_a = (1.0 + sq_b) * ((1.0 + sq_a) * along_a + cross_ab * along_b) / r_sq
    wind_b = (1.0 + sq_a) * (cross_ab * along_a + (1.0 + sq_b) * along_b) / r_sq
    return wind_a, wind_b


def random_unit(key_vec):
    raw_vec = jax.random.normal(key_vec, (3,), jnp.float32)
    return raw_vec / jnp.linalg.norm(raw_vec)


def setup_inputs(seed: int = 0, part: int = 0) -> dict:
    base_key = jax.random.key(seed)
    shared_key, part_key = jax.random.split(base_key)
    part_key = jax.random.fold_in(part_key, part)
    tan_a, tan_b, sphere_pts = sphere_points()
    key_axis, key_rate, key_scale = jax.random.split(shared_key, 3)
    rot_axis = random_unit(key_axis) * jax.random.uniform(key_rate, (), jnp.float32, 0.6, 1.0)
    velocity = jnp.cross(rot_axis, sphere_pts)
    wind_a, wind_b = flux_winds(tan_a, tan_b, velocity)
    wind_scale = jax.random.uniform(key_scale, (STEPS,), jnp.float32, -0.2, 1.0)
    key_front, key_wave, key_phase = jax.random.split(part_key, 3)
    front_part = jnp.tanh((N / 12.0) * (sphere_pts @ random_unit(key_front)))
    wave_phase = jax.random.uniform(key_phase, (), jnp.float32, 0.0, 2.0 * math.pi)
    wave_part = jnp.sin((N / 6.0) * (sphere_pts @ random_unit(key_wave)) + wave_phase)
    tracer = 0.8 * front_part + 0.5 * wave_part
    return {'tracer': tracer.astype(jnp.float32), 'wind_a': wind_a.astype(jnp.float32),
            'wind_b': wind_b.astype(jnp.float32), 'wind_scale': wind_scale}


def reference(tracer, wind_a, wind_b, wind_scale):
    cell_ids = jnp.arange(N)
    inv_area = inverse_area(cell_ids, cell_ids, N)
    face_a, face_b = wind_faces(sphere_blocks(wind_a, wind_b, True), wind_a, wind_b)

    def tend_of(tracer_now, step_scale):
        ext_a, ext_b = extend_field(tracer_now, sphere_blocks(tracer_now, tracer_now, False))
        return tendency(ext_a, ext_b, face_a, face_b, step_scale, inv_area)

    def one_step(tracer_now, step_scale):
        stage_one = tracer_now + DT * tend_of(tracer_now, step_scale)
        stage_two = stage_one + DT * tend_of(stage_one, step_scale)
        return 0.5 * (tracer_now + stage_two), None

    return lax.scan(one_step, tracer, wind_scale)[0]
```

```python
import math
import jax
import jax.numpy as jnp
from jax import lax
from jax.experimental import pallas as pl
from jax.experimental.pallas import tpu as pltpu
from jax.sharding import PartitionSpec as P

C_SPEED = 2.5
CFL_STEP = 0.12
EDGE_CODE = (
    (310, 100, 530, 420), (10, 200, 511, 410), (110, 300, 521, 431),
    (210, 0, 500, 401), (331, 130, 30, 231), (320, 121, 221, 20),
)
H = 12
KR = 48
NPAN = 3
NC = 3
SB = 8
LN = 128
GL = 4
STEPS_PER_BLOCK = 3
BETA_ROWS = 4
F32 = jnp.float32
PLANES = range(NC)
SIDES = range(4)


def turned_sign(side_id, edge_id):
    return int(side_id % 2 == edge_id % 2)


def small_tan(v):
    sq = v * v
    sin_sum, cos_sum = jnp.full_like(v, 1.0), jnp.full_like(v, 1.0)
    for n in (6, 5, 4, 3, 2, 1):
        sin_sum = 1.0 - sq * sin_sum * (1.0 / (2 * n * (2 * n + 1)))
        cos_sum = 1.0 - sq * cos_sum * (1.0 / (2 * n * (2 * n - 1)))
    return v * sin_sum / cos_sum


def lanes_of(shape):
    return lax.broadcasted_iota(jnp.int32, shape, len(shape) - 1)


def rows_of(shape):
    return lax.broadcasted_iota(jnp.int32, shape, len(shape) - 2)


def make_kernel(tile_count, steps, n_blocks, tile_rows):
    last = tile_count - 1
    cells = tile_rows * tile_count
    dalpha = 0.5 * math.pi / cells

    def kernel(ws_ref, q_in, a_in, b_in, out_ref, QA, QB, WW, CQ, KK, NN, TT, ZS, SEND, RECV, CSEND, CRECV,
               send_sem, recv_sem, csend_sem, crecv_sem):
        dev = lax.axis_index('panel')
        tx = lax.axis_index('tx')
        ty = lax.axis_index('ty')
        WA, WB = 0, NPAN

        def at_edge(side):
            return (tx == 0, tx == last, ty == 0, ty == last)[side]

        def edge_codes(p):
            g = NPAN * dev + p
            out = []
            for side in SIDES:
                codes = [row[side] * 2 + turned_sign(side, row[side] // 10 % 10) for row in EDGE_CODE]
                code = jnp.int32(codes[0])
                for n in range(1, len(codes)):
                    code = jnp.where(g == n, codes[n], code)
                turned, code = lax.rem(code, 2), lax.div(code, 2)
                panel = lax.div(code, 100)
                rest = code - 100 * panel
                dside = lax.div(rest, 10)
                flip = rest - 10 * dside
                out.append((lax.div(panel, NPAN), lax.rem(panel, NPAN), dside, jnp.where(at_edge(side), flip, 0),
                            jnp.where(at_edge(side), turned, 0), flip))
            return out

        def dest(codes, p, side, off):
            along = (ty if side < 2 else tx) + off
            edge = at_edge(side)
            d_dev, d_slot, dside, flip_here, _, flip = codes[side]
            al = along + flip * (last - 2 * along)
            c_tx = jnp.where(dside == 0, 0, jnp.where(dside == 1, last, al))
            c_ty = jnp.where(dside == 2, 0, jnp.where(dside == 3, last, al))
            step = 2 * (side % 2) - 1
            in_tx, in_ty = (tx + step, ty + off) if side < 2 else (tx + off, ty + step)
            device = {'tx': jnp.where(edge, c_tx, in_tx), 'ty': jnp.where(edge, c_ty, in_ty),
                      'panel': jnp.where(edge, d_dev, dev)}
            return device, jnp.where(edge, d_slot, p), jnp.where(edge, dside, side ^ 1), flip_here

        def corner_plan(codes, p, sa, sb):
            out_b = at_edge(2 + sb)
            plans = []
            for side, end, off in ((sa, sb, 2 * sb - 1), (2 + sb, sa, 2 * sa - 1)):
                device, slot, dside, flip = dest(codes, p, side, off)
                x = end + flip * (1 - 2 * end)
                e = 1 - x
                plans.append((device, slot, jnp.where(dside < 2, 2 * dside + e, 2 * e + (dside - 2)), side, x))
            (dv_a, sl_a, dc_a, s_a, x_a), (dv_b, sl_b, dc_b, s_b, x_b) = plans
            device = {key: jnp.where(out_b, dv_b[key], dv_a[key]) for key in dv_a}
            return (device, jnp.where(out_b, sl_b, sl_a), jnp.where(out_b, dc_b, dc_a),
                    jnp.where(out_b, s_b, s_a), jnp.where(out_b, x_b, x_a))

        def has_corner(sa, sb):
            return jnp.logical_not(jnp.logical_and(at_edge(sa), at_edge(2 + sb)))

        def is_here(device):
            return jnp.logical_and(jnp.logical_and(device['tx'] == tx, device['ty'] == ty), device['panel'] == dev)

        corners = [(sa, sb) for sa in range(2) for sb in range(2)]
        mesh_ids = pl.DeviceIdType.MESH

        barrier = pltpu.get_barrier_semaphore()

        @pl.loop(0, NPAN)
        def _(p):
            codes = edge_codes(p)
            for side in SIDES:
                pl.semaphore_signal(barrier, inc=1, device_id=dest(codes, p, side, 0)[0], device_id_type=mesh_ids)
            for sa, sb in corners:
                @pl.when(has_corner(sa, sb))
                def _():
                    pl.semaphore_signal(barrier, inc=1, device_id=corner_plan(codes, p, sa, sb)[0], device_id_type=mesh_ids)

        def load_field(in_ref, dst, base):
            @pl.loop(0, NPAN)
            def _(p):
                for it in PLANES:
                    for jt in PLANES:
                        TT[it, pl.ds(H + LN * jt, LN), :] = in_ref[p, pl.ds(LN * it, LN), pl.ds(LN * jt, LN)].T
                    for c in PLANES:
                        NN[c, pl.ds(H + LN * it, LN), :] = TT[it, pl.ds(c, LN, stride=NC), :].T

                @pl.loop(0, KR // SB)
                def _(kb):
                    for c in PLANES:
                        for k in range(SB):
                            dst[base + p, c, pl.ds(pl.multiple_of(64 * kb + SB * (k + 2), SB), SB), :] = NN[c, pl.ds(SB * kb + k, SB, stride=KR), :]

        def store_field(src):
            @pl.loop(0, NPAN)
            def _(p):
                @pl.loop(0, KR // SB)
                def _(kb):
                    for c in PLANES:
                        for k in range(SB):
                            NN[c, pl.ds(SB * kb + k, SB, stride=KR), :] = src[p, c, pl.ds(pl.multiple_of(64 * kb + SB * (k + 2), SB), SB), :]
                for it in PLANES:
                    for c in PLANES:
                        TT[it, pl.ds(c, LN, stride=NC), :] = NN[c, pl.ds(H + LN * it, LN), :].T
                    for jt in PLANES:
                        out_ref[p, pl.ds(LN * it, LN), pl.ds(LN * jt, LN)] = TT[it, pl.ds(H + LN * jt, LN), :].T

        def pack_rows(ref, src, f, p):
            for c in PLANES:
                SEND[f, p, 0, c] = ref[src, c, pl.ds(SB * (H + 2), H, stride=SB), :]
                high = ref[src, c, pl.ds(SB * 26 + 7, H, stride=SB), :]
                for m in range(H):
                    SEND[f, p, 1, c, m:m + 1, :] = high[11 - m:12 - m, :]

        def pack_cols(ref, src, f, p):
            for cp in PLANES:
                for c in PLANES:
                    blk = jnp.concatenate([ref[src, c, pl.ds(SB * (cp + 2) + s, 16, stride=24), :] for s in range(SB)], axis=0)
                    t = blk.T
                    for q in SIDES:
                        lo, hi = 3 * q + c, 3 * q + 2 - c
                        SEND[f, p, 2, cp, lo:lo + 1, :] = t[4 + q:5 + q, :]
                        SEND[f, p, 3, cp, hi:hi + 1, :] = t[123 - q:124 - q, :]

        def flip_and_sign(codes, f, p, winds):
            for side in SIDES:
                _, _, _, flip, turned, _ = codes[side]

                @pl.when(flip == 1)
                def _():
                    inside = lanes_of((NC * H, LN))
                    inside = jnp.logical_and(inside >= GL, inside < LN - GL)
                    old = jnp.concatenate([SEND[f, p, side, NC - 1 - c] for c in PLANES], axis=0)
                    mirror = (rows_of((LN, LN)) + lanes_of((LN, LN)) == LN - 1).astype(F32)
                    new = jnp.dot(jnp.where(inside, old, 0.0), mirror, precision=lax.Precision.HIGHEST,
                                  preferred_element_type=F32)
                    for c in PLANES:
                        SEND[f, p, side, c] = new[H * c:H * (c + 1)]
                if winds:
                    @pl.when(jnp.where(f == 1, turned, flip) == 1)
                    def _():
                        for c in PLANES:
                            SEND[f, p, side, c] = -SEND[f, p, side, c]

        def pack_corners(codes, f, p):
            lane = lanes_of((H, LN))
            for sa, sb in corners:
                _, _, _, side, x = corner_plan(codes, p, sa, sb)
                high = x == 1
                hi = lo = None
                for c in PLANES:
                    v = SEND[f, p, side, c]
                    vh, vl = pltpu.roll(v, SB + 4 * c, 1), pltpu.roll(v, 120 - 4 * c, 1)
                    hi = vh if c == 0 else jnp.where(lane >= 4 * c, vh, hi)
                    lo = vl if c == 0 else jnp.where(lane < LN - 4 * c, vl, lo)
                CSEND[f, p, 2 * sa + sb] = jnp.where(high, hi, lo)

        def start_copies(codes, f, fr, p):
            for side in SIDES:
                device, slot, dside, _ = dest(codes, p, side, 0)
                here = is_here(device)

                @pl.when(here)
                def _():
                    RECV[fr, slot, dside] = SEND[f, p, side]

                @pl.when(jnp.logical_not(here))
                def _():
                    pltpu.make_async_remote_copy(
                        src_ref=SEND.at[f, p, side], dst_ref=RECV.at[fr, slot, dside], send_sem=send_sem.at[f, p, side],
                        recv_sem=recv_sem.at[fr, slot, dside], device_id=device, device_id_type=mesh_ids).start()
            for sa, sb in corners:
                cid = 2 * sa + sb

                @pl.when(has_corner(sa, sb))
                def _():
                    device, slot, dcorner, _, _ = corner_plan(codes, p, sa, sb)
                    pltpu.make_async_remote_copy(
                        src_ref=CSEND.at[f, p, cid], dst_ref=CRECV.at[fr, slot, dcorner], send_sem=csend_sem.at[f, p, cid],
                        recv_sem=crecv_sem.at[fr, slot, dcorner], device_id=device, device_id_type=mesh_ids).start()

        def wait_copies(codes, strips, blocks, sem, csem, f, p):
            for side in SIDES:
                @pl.when(jnp.logical_not(is_here(dest(codes, p, side, 0)[0])))
                def _():
                    pltpu.make_async_copy(strips.at[f, p, side], strips.at[f, p, side], sem.at[f, p, side]).wait()
            for sa, sb in corners:
                cid = 2 * sa + sb

                @pl.when(has_corner(sa, sb))
                def _():
                    pltpu.make_async_copy(blocks.at[f, p, cid], blocks.at[f, p, cid], csem.at[f, p, cid]).wait()

        def end_valid(side, e):
            if side < 2:
                return jnp.logical_not(at_edge(2 + e))
            return jnp.logical_and(jnp.logical_not(at_edge(e)), at_edge(side))

        def merged(fr, p, side, c):
            lane = lanes_of((H, LN))
            v = RECV[fr, p, side, c]
            for e in range(2):
                cid = 2 * side + e if side < 2 else 2 * e + side - 2
                msg = CRECV[fr, p, cid]
                if c:
                    msg = pltpu.roll(msg, 4 * c if e else LN - 4 * c, 1)
                inside = lane >= 124 if e else lane < 4
                v = jnp.where(jnp.logical_and(inside, end_valid(side, e)), msg, v)
            return v

        def unpack_cols(ref, dst, fr, p):
            lane = lanes_of((16, LN))
            ghost = jnp.logical_or(lane < 4, lane >= 124)
            for cp in PLANES:
                low, high = merged(fr, p, 2, cp), merged(fr, p, 3, cp)
                for c in PLANES:
                    z = ZS.at[3 * cp + c]
                    for l in SIDES:
                        m = 3 * (3 - l) + 2 - c
                        z[l:l + 1, :] = low[m:m + 1, :]
                        m = 3 * l + c
                        z[124 + l:125 + l, :] = high[m:m + 1, :]
                    t = z[...].T
                    for s in range(SB):
                        rows = pl.ds(SB * (cp + 2) + s, 16, stride=24)
                        ref[dst, c, rows, :] = jnp.where(ghost, t[16 * s:16 * s + 16, :], ref[dst, c, rows, :])

        def unpack_rows(ref, dst, fr, p):
            lane = lanes_of((H, LN))
            keep = jnp.logical_and(jnp.logical_or(lane >= 4, end_valid(0, 0)), jnp.logical_or(lane < 124, end_valid(0, 1)))
            for c in PLANES:
                v = merged(fr, p, 0, c)
                for m in range(H):
                    row = pl.ds(SB * (13 - m), 1)
                    ref[dst, c, row, :] = jnp.where(keep[m:m + 1, :], v[m:m + 1, :], ref[dst, c, row, :])
                rows = pl.ds(SB * 38 + 7, H, stride=SB)
                ref[dst, c, rows, :] = jnp.where(keep, merged(fr, p, 1, c), ref[dst, c, rows, :])

        def pad_rows(ref):
            for p in range(NPAN):
                ref[p, :, pl.ds(0, 2 * SB), :] = ref[p, :, pl.ds(SB * KR - 1, 2 * SB), :]
                ref[p, :, pl.ds(SB * (KR + 2), 2 * SB), :] = ref[p, :, pl.ds(2 * SB + 1, 2 * SB), :]

        def corner_case(fn):
            for sa, sb in corners:
                @pl.when(jnp.logical_and(at_edge(sa), at_edge(2 + sb)))
                def _():
                    fn(sa, sb)

        def quad_geom(sa, sb):
            k0, s = (0, 0) if sa == 0 else (KR - H, SB - 1)
            lane0 = 0 if sb == 0 else LN - GL
            lane, idx = lanes_of((H, LN)), rows_of((H, LN))
            col = idx if sa == sb else H - 1 - idx
            masks = [NC * (lane - lane0) + c == col for c in PLANES]
            return k0, s, lane, masks, pl.ds(SB * (k0 + 2) + s, H, stride=SB)

        def beta_column(ref, src, sa, sb, r):
            k0, s, lane, masks, rows = quad_geom(sa, sb)
            kr = H + r if sa == 0 else KR - H - 1 - r
            tot = jnp.zeros((H, LN), F32)
            for c in PLANES:
                tot = jnp.where(masks[c], ref[src, c, pl.ds(SB * (kr + 2) + s, 1), :], tot)
            l_to, c_to = (GL - 1, NC - 1 - r) if sb == 0 else (LN - GL, r)
            return jnp.sum(tot, axis=1, keepdims=True), lane == l_to, c_to, rows

        def alpha_lines(ref, src, sa, sb, r):
            _, _, lane, masks, rows = quad_geom(sa, sb)
            l_from, c_from = (GL, r) if sb == 0 else (LN - GL - 1, NC - 1 - r)
            col = jnp.sum(jnp.where(lane == l_from, ref[src, c_from, rows, :], 0.0), axis=1, keepdims=True)
            return [jnp.sum(jnp.where(mask, col, 0.0), axis=0, keepdims=True) for mask in masks]

        def fill_quadrant(src, sa, sb):
            jobs = [(p, r) for p in range(NPAN) for r in range(2)]
            columns = [beta_column(src, p, sa, sb, r) for p, r in jobs]
            lines = [alpha_lines(src, p, sa, sb, r) for p, r in jobs]
            for (p, r), (col, mask, c_to, rows), line in zip(jobs, columns, lines):
                src[p, c_to, rows, :] = jnp.where(mask, col, src[p, c_to, rows, :])
                for c in PLANES:
                    CQ[p, r, c] = jnp.broadcast_to(line[c], (SB, LN))

        def fill_winds(sa, sb):
            sign = -1.0 if sa == sb else 1.0
            for p in range(NPAN):
                col, mask, c_to, rows = beta_column(WW, WA + p, sa, sb, 0)
                line = alpha_lines(WW, WB + p, sa, sb, 0)
                WW[WB + p, c_to, rows, :] = jnp.where(mask, sign * col, WW[WB + p, c_to, rows, :])
                row_lane = lanes_of((1, LN))
                inside = row_lane < GL if sb == 0 else row_lane >= LN - GL
                row = pl.ds(SB * (H + 1), 1) if sa == 0 else pl.ds(SB * (KR - H + 3) - 1, 1)
                for c in PLANES:
                    WW[WA + p, c, row, :] = jnp.where(inside, sign * line[c], WW[WA + p, c, row, :])

        def roll_down(v):
            return pltpu.roll(v, LN - 1, 1)

        def roll_up(v):
            return pltpu.roll(v, 1, 1)

        def beta_rows(src, p, k0, scale):
            rows = pl.ds(SB * (k0 + 2), SB * BETA_ROWS)
            a0, a1, a2 = (src[p, c, rows, :] for c in PLANES)
            a2l, a0r, a1r = roll_up(a2), roll_down(a0), roll_down(a1)
            e0, e1, e2 = a2l + a1, a0 + a2, a1 + a0r
            g0, g1, g2 = 8.0 * a0 - e0, 8.0 * a1 - e1, 8.0 * a2 - e2
            g0r = 8.0 * a0r - (a2 + a1r)
            x0 = WW[WB + p, 0, rows, :] * (g0 + g1)
            x1 = WW[WB + p, 1, rows, :] * (g1 + g2)
            x2 = WW[WB + p, 2, rows, :] * (g2 + g0r)
            x2l = roll_up(x2)
            return scale * (x0 - x2l) - e0, scale * (x1 - x0) - e1, scale * (x2 - x1) - e2

        def row_group(ref, p, k):
            return ref[p, :, pl.ds(SB * (k + 2), SB), :]

        def panel_pass(src, dst, p, scale, second):
            lane, sub = lanes_of((NC, SB, LN)), rows_of((NC, SB, LN))
            ghost_lane = jnp.logical_or(jnp.logical_and(at_edge(2), lane < GL),
                                        jnp.logical_and(at_edge(3), lane >= LN - GL))
            in_low = jnp.logical_and(ghost_lane, jnp.logical_and(at_edge(0), sub == 0))
            in_high = jnp.logical_and(ghost_lane, jnp.logical_and(at_edge(1), sub == SB - 1))

            def load(k):
                v = row_group(src, p, k)
                if k in (H - 2, H - 1):
                    return jnp.where(in_low, CQ[p, H - 1 - k], v)
                if k in (KR - H, KR - H + 1):
                    return jnp.where(in_high, CQ[p, k - (KR - H)], v)
                return v

            qm, q0, q1 = load(-2), load(-1), load(0)
            q2 = load(1)
            g0 = 8.0 * q0 - (qm + q1)
            e1 = q0 + q2
            g1 = 8.0 * q1 - e1
            x_low = row_group(WW, WA + p, -1) * (g0 + g1)
            q_now, e_now, g_now, q_next = q1, e1, g1, q2
            beta = None
            for k in range(KR):
                if k % BETA_ROWS == 0:
                    beta = beta_rows(src, p, k, scale)
                at = SB * (k % BETA_ROWS)
                tb = jnp.stack([beta[c][at:at + SB] for c in PLANES])
                q_far = load(k + 2)
                e_next = q_now + q_far
                g_next = 8.0 * q_next - e_next
                x_high = row_group(WW, WA + p, k) * (g_now + g_next)
                u = scale * (x_high - x_low) - e_now + tb + 4.0 * q_now
                new = q_now - KK[:, pl.ds(SB * k, SB), :] * u
                if second:
                    new = 0.5 * (row_group(dst, p, k) + new)
                dst[p, :, pl.ds(SB * (k + 2), SB), :] = new
                x_low, q_now, e_now, g_now, q_next = x_high, q_next, e_next, g_next, q_far

        def stage(src, dst, scale, second):
            pad_rows(src)
            corner_case(lambda sa, sb: fill_quadrant(src, sa, sb))

            @pl.loop(0, NPAN)
            def _(p):
                panel_pass(src, dst, p, scale, second)

        load_field(a_in, WW, WA)
        load_field(b_in, WW, WB)
        is_cc = jnp.logical_and(jnp.logical_or(at_edge(0), at_edge(1)), jnp.logical_or(at_edge(2), at_edge(3)))
        pl.semaphore_wait(barrier, SB * NPAN - NPAN * jnp.where(is_cc, 1, 0))

        @pl.loop(0, 2 * NPAN)
        def _(n):
            f, p = lax.div(n, NPAN) + 1, lax.rem(n, NPAN)
            codes = edge_codes(p)
            pack_rows(WW, n, f, p)
            pack_cols(WW, (2 - f) * NPAN + p, f, p)
            flip_and_sign(codes, f, p, True)
            pack_corners(codes, f, p)
            start_copies(codes, f, f + 1, p)
        load_field(q_in, QA, 0)

        def finish_winds():
            metric()

            @pl.loop(0, 2 * NPAN)
            def _(n):
                f, p = lax.div(n, NPAN) + 1, lax.rem(n, NPAN)
                wait_copies(edge_codes(p), RECV, CRECV, recv_sem, crecv_sem, f + 1, p)
                unpack_cols(WW, (2 - f) * NPAN + p, f + 1, p)

            @pl.loop(0, 2 * NPAN)
            def _(n):
                f, p = lax.div(n, NPAN) + 1, lax.rem(n, NPAN)
                unpack_rows(WW, n, f + 1, p)
                wait_copies(edge_codes(p), SEND, CSEND, send_sem, csend_sem, f, p)
            corner_case(fill_winds)
            pad_rows(WW)
            face_scale = 0.5 / (12.0 * 0.5 * C_SPEED)

            @pl.loop(0, NPAN)
            def _(p):
                for c in PLANES:
                    low, high = pl.ds(SB, SB * (KR + 1)), pl.ds(2 * SB, SB * (KR + 1))
                    WW[WA + p, c, low, :] = face_scale * (WW[WA + p, c, low, :] + WW[WA + p, c, high, :])
                rows = pl.ds(2 * SB, SB * KR)
                b0, b1, b2 = (WW[WB + p, c, rows, :] for c in PLANES)
                WW[WB + p, 0, rows, :] = face_scale * (b0 + b1)
                WW[WB + p, 1, rows, :] = face_scale * (b1 + b2)
                WW[WB + p, 2, rows, :] = face_scale * (b2 + roll_down(b0))

        def metric():
            ridx = rows_of((SB * KR, LN))
            gi = tx * tile_rows + lax.rem(ridx, SB) * KR + lax.div(ridx, SB) - H
            gi = jnp.where(gi < 0, -1 - gi, jnp.where(gi >= cells, 2 * cells - 1 - gi, gi))
            tan_a = small_tan((gi.astype(F32) + 0.5) * dalpha - 0.25 * math.pi)
            for c in PLANES:
                gj = ty * tile_rows + 3 * lanes_of((SB, LN)) + c - H
                gj = jnp.where(gj < 0, -1 - gj, jnp.where(gj >= cells, 2 * cells - 1 - gj, gj))
                tan_b = small_tan((gj.astype(F32) + 0.5) * dalpha - 0.25 * math.pi)[0:1, :]
                a_sq, b_sq = tan_a * tan_a, tan_b * tan_b
                r_sq = 1.0 + a_sq + b_sq
                sqrt_g = (1.0 + a_sq) * (1.0 + b_sq) / (r_sq * jnp.sqrt(r_sq))
                KK[c] = (0.5 * C_SPEED * CFL_STEP) / sqrt_g

        @pl.loop(0, n_blocks)
        def _(b):
            fr = lax.rem(b, 2)

            @pl.loop(0, NPAN)
            def _(p):
                codes = edge_codes(p)
                pack_rows(QA, p, 0, p)
                pack_cols(QA, p, 0, p)
                flip_and_sign(codes, 0, p, False)
                pack_corners(codes, 0, p)
                start_copies(codes, 0, fr, p)

            @pl.when(b == 0)
            def _():
                finish_winds()

            @pl.loop(0, NPAN)
            def _(p):
                codes = edge_codes(p)
                wait_copies(codes, RECV, CRECV, recv_sem, crecv_sem, fr, p)
                unpack_cols(QA, p, fr, p)
                unpack_rows(QA, p, fr, p)
                wait_copies(codes, SEND, CSEND, send_sem, csend_sem, 0, p)

            @pl.loop(lax.div(b * steps, n_blocks), lax.div((b + 1) * steps, n_blocks))
            def _(t):
                scale = ws_ref[t]
                stage(QA, QB, scale, False)
                stage(QB, QA, scale, True)

        store_field(QA)

    return kernel


def solution(mesh):
    tile_count = mesh.shape['tx']
    field_spec = P(('member', 'panel'), 'tx', 'ty')
    wind_spec = P('panel', 'tx', 'ty')

    def local_run(tracer, wind_a, wind_b, wind_scale):
        steps = wind_scale.shape[0]
        n_blocks = -(-steps // STEPS_PER_BLOCK)
        ext = SB * KR
        block = pl.BlockSpec((NPAN, ext, ext), lambda n: (0, 0, 0))
        dma = pltpu.SemaphoreType.DMA
        return pl.pallas_call(
            make_kernel(tile_count, steps, n_blocks, tracer.shape[1]),
            grid=(1,),
            out_shape=jax.ShapeDtypeStruct(tracer.shape, F32),
            in_specs=[pl.BlockSpec(memory_space=pltpu.SMEM), block, block, block],
            out_specs=block,
            scratch_shapes=[
                pltpu.VMEM((NPAN, NC, ext + 32, LN), F32),
                pltpu.VMEM((NPAN, NC, ext + 32, LN), F32),
                pltpu.VMEM((2 * NPAN, NC, ext + 32, LN), F32),
                pltpu.VMEM((NPAN, 2, NC, SB, LN), F32),
                pltpu.VMEM((NC, ext, LN), F32),
                pltpu.VMEM((NC, ext + 32, LN), F32),
                pltpu.VMEM((NC, ext + 32, LN), F32),
                pltpu.VMEM((9, LN, LN), F32),
                pltpu.VMEM((3, NPAN, 4, NC, H, LN), F32),
                pltpu.VMEM((4, NPAN, 4, NC, H, LN), F32),
                pltpu.VMEM((3, NPAN, 4, H, LN), F32),
                pltpu.VMEM((4, NPAN, 4, H, LN), F32),
                *[dma((n, NPAN, 4)) for n in (3, 4, 3, 4)],
            ],
            compiler_params=pltpu.CompilerParams(collective_id=0, has_side_effects=True, vmem_limit_bytes=60 * 1024 * 1024),
            cost_estimate=pl.CostEstimate(flops=10 ** 9, bytes_accessed=10 ** 7, transcendentals=0),
        )(wind_scale, tracer, wind_a, wind_b)

    return jax.shard_map(local_run, mesh=mesh, in_specs=(field_spec, wind_spec, wind_spec, P()),
                         out_specs=field_spec, check_vma=False)
```

```python
import math
import jax
import numpy as np
import jax.numpy as jnp
from jax import lax
from jax.experimental import pallas as pl
from jax.experimental.pallas import tpu as pltpu
from jax.sharding import PartitionSpec as P

C_SPEED = 2.5
CFL_STEP = 0.12
EDGE_CODE = (
    (310, 100, 530, 420), (10, 200, 511, 410), (110, 300, 521, 431),
    (210, 0, 500, 401), (331, 130, 30, 231), (320, 121, 221, 20),
)
H = 12
KR = 48
NPAN = 3
NC = 3
SB = 8
LN = 128
GL = 4
STEPS_PER_BLOCK = 3
BETA_ROWS = 4
F32 = jnp.float32
PLANES = range(NC)
SIDES = range(4)


def turned_sign(side_id, edge_id):
    return int(side_id % 2 == edge_id % 2)


def small_tan(v):
    sq = v * v
    sin_sum, cos_sum = jnp.full_like(v, 1.0), jnp.full_like(v, 1.0)
    for n in (6, 5, 4, 3, 2, 1):
        sin_sum = 1.0 - sq * sin_sum * (1.0 / (2 * n * (2 * n + 1)))
        cos_sum = 1.0 - sq * cos_sum * (1.0 / (2 * n * (2 * n - 1)))
    return v * sin_sum / cos_sum


def sel(pred, yes, no):
    yes, no = (np.int32(v) if isinstance(v, int) else v for v in (yes, no))
    same = jnp.shape(yes) == jnp.shape(no) and jnp.shape(pred) in ((), jnp.shape(yes))
    return lax.select(pred, yes, no) if same else jnp.where(pred, yes, no)


def lanes_of(shape):
    return lax.broadcasted_iota(jnp.int32, shape, len(shape) - 1)


def rows_of(shape):
    return lax.broadcasted_iota(jnp.int32, shape, len(shape) - 2)


def make_kernel(tile_count, steps, n_blocks, tile_rows):
    last = tile_count - 1
    cells = tile_rows * tile_count
    dalpha = 0.5 * math.pi / cells

    def kernel(ws_ref, q_in, a_in, b_in, out_ref, QA, QB, WW, CQ, KK, NN, TT, ZS, SEND, RECV, CSEND, CRECV,
               send_sem, recv_sem, csend_sem, crecv_sem):
        dev = lax.axis_index('panel')
        tx = lax.axis_index('tx')
        ty = lax.axis_index('ty')
        WA, WB = 0, NPAN

        def at_edge(side):
            return (tx == 0, tx == last, ty == 0, ty == last)[side]

        def pick(v0, v1):
            return v0 if v0 == v1 else v0 + dev * (v1 - v0)

        def neighbour(p, side):
            codes = [EDGE_CODE[NPAN * dv + p][side] for dv in (0, 1)]
            panels = [code // 100 for code in codes]
            edges = [code // 10 % 10 for code in codes]
            return (pick(*[n // NPAN for n in panels]), pick(*[n % NPAN for n in panels]), pick(*edges),
                    pick(*[code % 10 for code in codes]), pick(*[turned_sign(side, e) for e in edges]))

        def dest(p, side, off):
            along = (ty if side < 2 else tx) + off
            edge = at_edge(side)
            d_dev, d_slot, dside, flip, _ = neighbour(p, side)
            al = along + flip * (last - 2 * along)
            c_tx = sel(dside == 0, 0, sel(dside == 1, last, al))
            c_ty = sel(dside == 2, 0, sel(dside == 3, last, al))
            step = 2 * (side % 2) - 1
            in_tx, in_ty = (tx + step, ty + off) if side < 2 else (tx + off, ty + step)
            device = {'tx': sel(edge, c_tx, in_tx), 'ty': sel(edge, c_ty, in_ty),
                      'panel': sel(edge, d_dev, dev)}
            return device, sel(edge, d_slot, p), sel(edge, dside, side ^ 1), sel(edge, flip, 0)

        def corner_plan(p, sa, sb):
            out_b = at_edge(2 + sb)
            plans = []
            for side, end, off in ((sa, sb, 2 * sb - 1), (2 + sb, sa, 2 * sa - 1)):
                device, slot, dside, flip = dest(p, side, off)
                x = end + flip * (1 - 2 * end)
                e = 1 - x
                plans.append((device, slot, sel(dside < 2, 2 * dside + e, 2 * e + (dside - 2)), side, x))
            (dv_a, sl_a, dc_a, s_a, x_a), (dv_b, sl_b, dc_b, s_b, x_b) = plans
            device = {key: sel(out_b, dv_b[key], dv_a[key]) for key in dv_a}
            return (device, sel(out_b, sl_b, sl_a), sel(out_b, dc_b, dc_a),
                    sel(out_b, s_b, s_a), sel(out_b, x_b, x_a))

        def has_corner(sa, sb):
            return jnp.logical_not(jnp.logical_and(at_edge(sa), at_edge(2 + sb)))

        def is_here(device):
            return jnp.logical_and(jnp.logical_and(device['tx'] == tx, device['ty'] == ty), device['panel'] == dev)

        corners = [(sa, sb) for sa in range(2) for sb in range(2)]
        slots = range(NPAN)
        strip_to = [[dest(p, side, 0)[:3] for side in SIDES] for p in slots]
        stays = [[is_here(plan[0]) for plan in row] for row in strip_to]
        corner_to = [[corner_plan(p, sa, sb) for sa, sb in corners] for p in slots]
        mesh_ids = pl.DeviceIdType.MESH

        barrier = pltpu.get_barrier_semaphore()

        for p in slots:
            for side in SIDES:
                pl.semaphore_signal(barrier, inc=1, device_id=strip_to[p][side][0], device_id_type=mesh_ids)
            for (sa, sb), plan in zip(corners, corner_to[p]):
                @pl.when(has_corner(sa, sb))
                def _():
                    pl.semaphore_signal(barrier, inc=1, device_id=plan[0], device_id_type=mesh_ids)

        def load_field(in_ref, dst, base):
            @pl.loop(0, NPAN)
            def _(p):
                for it in PLANES:
                    for jt in PLANES:
                        TT[it, pl.ds(H + LN * jt, LN), :] = in_ref[p, pl.ds(LN * it, LN), pl.ds(LN * jt, LN)].T
                    for c in PLANES:
                        NN[c, pl.ds(H + LN * it, LN), :] = TT[it, pl.ds(c, LN, stride=NC), :].T

                @pl.loop(0, KR // SB)
                def _(kb):
                    for c in PLANES:
                        for k in range(SB):
                            dst[base + p, c, pl.ds(pl.multiple_of(64 * kb + SB * (k + 2), SB), SB), :] = NN[c, pl.ds(SB * kb + k, SB, stride=KR), :]

        def store_field(src):
            @pl.loop(0, NPAN)
            def _(p):
                @pl.loop(0, KR // SB)
                def _(kb):
                    for c in PLANES:
                        for k in range(SB):
                            NN[c, pl.ds(SB * kb + k, SB, stride=KR), :] = src[p, c, pl.ds(pl.multiple_of(64 * kb + SB * (k + 2), SB), SB), :]
                for it in PLANES:
                    for c in PLANES:
                        TT[it, pl.ds(c, LN, stride=NC), :] = NN[c, pl.ds(H + LN * it, LN), :].T
                    for jt in PLANES:
                        out_ref[p, pl.ds(LN * it, LN), pl.ds(LN * jt, LN)] = TT[it, pl.ds(H + LN * jt, LN), :].T

        def quarter(n):
            return pl.ds(GL * n, GL)

        def rows_at(first, s, n):
            return pl.ds(SB * (first + 2 + n) + s, GL, stride=NC * SB)

        def pack_strips(row_ref, row_at, col_ref, col_at, f, p):
            for c in PLANES:
                for n in PLANES:
                    SEND[f, p, 0, c, quarter(n), :] = row_ref[row_at, c, rows_at(H, 0, n), :]
                    SEND[f, p, 1, c, quarter(n), :] = row_ref[row_at, c, rows_at(KR - 2 * H, SB - 1, n), :]
            lane = lanes_of((LN, LN))

            def window(first):
                return jnp.logical_and(lane >= first, lane < first + GL)
            for cp in PLANES:
                mix = None
                for c in PLANES:
                    blk = jnp.concatenate([col_ref[col_at, c, pl.ds(SB * (cp + 2) + s, 2 * SB, stride=NC * SB), :]
                                           for s in range(SB)], axis=0)
                    if c == 0:
                        mix = blk
                    else:
                        mine = jnp.logical_or(window(GL + SB * c), window(SB * (c - 1)))
                        mix = sel(mine, pltpu.roll(blk, SB * c, 1), mix)
                t = mix.T
                for c in PLANES:
                    low, high = GL + SB * c, (LN - SB + SB * c) % LN
                    SEND[f, p, 2, cp, quarter(c), :] = t[low:low + GL]
                    SEND[f, p, 3, cp, quarter(c), :] = t[high:high + GL]

        def turn_strips(f, p, winds):
            for side in SIDES:
                _, _, _, flip, turned = neighbour(p, side)
                if not isinstance(flip, int) or flip:
                    @pl.when(sel(at_edge(side), flip, 0) == 1)
                    def _():
                        inside = lanes_of((NC * H, LN))
                        inside = jnp.logical_and(inside >= GL, inside < LN - GL)
                        old = jnp.concatenate([SEND[f, p, side, NC - 1 - c] for c in PLANES], axis=0)
                        mirror = (rows_of((LN, LN)) + lanes_of((LN, LN)) == LN - 1).astype(F32)
                        new = jnp.dot(sel(inside, old, 0.0), mirror, precision=lax.Precision.HIGHEST,
                                      preferred_element_type=F32)
                        for c in PLANES:
                            SEND[f, p, side, c] = new[H * c:H * (c + 1)]
                        if winds:
                            @pl.when(f == 2)
                            def _():
                                for c in PLANES:
                                    SEND[f, p, side, c] = -SEND[f, p, side, c]
                if not isinstance(turned, int) or turned:
                    @pl.when(sel(at_edge(side), turned, 0) == 1)
                    def _():
                        for c in PLANES:
                            v = SEND[f, p, side, c]
                            if winds:
                                v = sel(f == 1, -v, v)
                            for m in range(H):
                                SEND[f, p, side, c, m:m + 1, :] = v[H - 1 - m:H - m, :]

        def pack_corners(f, p):
            lane = lanes_of((H, LN))
            for cid, (_, _, _, side, x) in enumerate(corner_to[p]):
                hi = lo = None
                for c in PLANES:
                    v = SEND[f, p, side, c]
                    vh, vl = pltpu.roll(v, SB + GL * c, 1), pltpu.roll(v, LN - SB - GL * c, 1)
                    hi = vh if c == 0 else sel(lane >= GL * c, vh, hi)
                    lo = vl if c == 0 else sel(lane < LN - GL * c, vl, lo)
                CSEND[f, p, cid] = sel(x == 1, hi, lo)

        def start_copies(f, fr, p):
            for side in SIDES:
                device, slot, dside = strip_to[p][side]
                here = stays[p][side]

                @pl.when(here)
                def _():
                    RECV[fr, slot, dside] = SEND[f, p, side]

                @pl.when(jnp.logical_not(here))
                def _():
                    pltpu.make_async_remote_copy(
                        src_ref=SEND.at[f, p, side], dst_ref=RECV.at[fr, slot, dside], send_sem=send_sem.at[f, p, side],
                        recv_sem=recv_sem.at[fr, slot, dside], device_id=device, device_id_type=mesh_ids).start()
            for cid, (sa, sb) in enumerate(corners):
                @pl.when(has_corner(sa, sb))
                def _():
                    device, slot, dcorner, _, _ = corner_to[p][cid]
                    pltpu.make_async_remote_copy(
                        src_ref=CSEND.at[f, p, cid], dst_ref=CRECV.at[fr, slot, dcorner], send_sem=csend_sem.at[f, p, cid],
                        recv_sem=crecv_sem.at[fr, slot, dcorner], device_id=device, device_id_type=mesh_ids).start()

        def wait_copies(strips, blocks, sem, csem, f, p):
            for side in SIDES:
                @pl.when(jnp.logical_not(stays[p][side]))
                def _():
                    pltpu.make_async_copy(strips.at[f, p, side], strips.at[f, p, side], sem.at[f, p, side]).wait()
            for cid, (sa, sb) in enumerate(corners):
                @pl.when(has_corner(sa, sb))
                def _():
                    pltpu.make_async_copy(blocks.at[f, p, cid], blocks.at[f, p, cid], csem.at[f, p, cid]).wait()

        def end_valid(side, e):
            if side < 2:
                return jnp.logical_not(at_edge(2 + e))
            return jnp.logical_and(jnp.logical_not(at_edge(e)), at_edge(side))

        def merged(fr, p, side, c):
            lane = lanes_of((H, LN))
            v = RECV[fr, p, side, c]
            for e in range(2):
                cid = 2 * side + e if side < 2 else 2 * e + side - 2
                msg = CRECV[fr, p, cid]
                if c:
                    msg = pltpu.roll(msg, 4 * c if e else LN - 4 * c, 1)
                inside = lane >= 124 if e else lane < 4
                v = sel(jnp.logical_and(inside, end_valid(side, e)), msg, v)
            return v

        def unpack_cols(ref, dst, fr, p):
            lane = lanes_of((2 * SB, LN))
            ghost = jnp.logical_or(lane < GL, lane >= LN - GL)
            for cp in PLANES:
                low, high = merged(fr, p, 2, cp), merged(fr, p, 3, cp)
                z = ZS.at[NC * p + cp]
                for c in PLANES:
                    z[pl.ds(SB * c, GL), :] = low[GL * c:GL * (c + 1)]
                    z[pl.ds((SB * c - GL) % LN, GL), :] = high[GL * c:GL * (c + 1)]
                t = z[...].T
                for c in PLANES:
                    tc = pltpu.roll(t, LN - SB * c, 1) if c else t
                    for s in range(SB):
                        rows = pl.ds(SB * (cp + 2) + s, 2 * SB, stride=NC * SB)
                        ref[dst, c, rows, :] = sel(ghost, tc[2 * SB * s:2 * SB * (s + 1)], ref[dst, c, rows, :])

        def unpack_rows(ref, dst, fr, p):
            lane = lanes_of((GL, LN))
            keep = jnp.logical_and(jnp.logical_or(lane >= GL, end_valid(0, 0)),
                                   jnp.logical_or(lane < LN - GL, end_valid(0, 1)))
            for c in PLANES:
                for side, first, s in ((0, 0, 0), (1, KR - H, SB - 1)):
                    v = merged(fr, p, side, c)
                    for n in PLANES:
                        rows = rows_at(first, s, n)
                        ref[dst, c, rows, :] = sel(keep, v[GL * n:GL * (n + 1)], ref[dst, c, rows, :])

        def pad_rows(ref):
            at = pl.ds(0, NPAN)
            ref[at, :, pl.ds(0, 2 * SB), :] = ref[at, :, pl.ds(SB * KR - 1, 2 * SB), :]
            ref[at, :, pl.ds(SB * (KR + 2), 2 * SB), :] = ref[at, :, pl.ds(2 * SB + 1, 2 * SB), :]

        def corner_case(fn):
            for sa, sb in corners:
                @pl.when(jnp.logical_and(at_edge(sa), at_edge(2 + sb)))
                def _():
                    fn(sa, sb)

        def quad_geom(sa, sb):
            k0, s = (0, 0) if sa == 0 else (KR - H, SB - 1)
            lane0 = 0 if sb == 0 else LN - GL
            lane, idx = lanes_of((H, LN)), rows_of((H, LN))
            col = idx if sa == sb else H - 1 - idx
            masks = [NC * (lane - lane0) + c == col for c in PLANES]
            return k0, s, lane, masks, pl.ds(SB * (k0 + 2) + s, H, stride=SB)

        def beta_column(ref, first, sa, sb, r):
            k0, s, lane, masks, rows = quad_geom(sa, sb)
            kr = H + r if sa == 0 else KR - H - 1 - r
            tot = jnp.zeros((NPAN, H, LN), F32)
            for c in PLANES:
                line = ref[pl.ds(first, NPAN), c, pl.ds(SB * (kr + 2) + s, 1), :]
                tot = sel(wide(masks[c]), jnp.broadcast_to(line, tot.shape), tot)
            l_to, c_to = (GL - 1, NC - 1 - r) if sb == 0 else (LN - GL, r)
            return jnp.broadcast_to(jnp.sum(tot, axis=2, keepdims=True), tot.shape), wide(lane == l_to), c_to, rows

        def alpha_lines(ref, first, sa, sb, r):
            _, _, lane, masks, rows = quad_geom(sa, sb)
            l_from, c_from = (GL, r) if sb == 0 else (LN - GL - 1, NC - 1 - r)
            zero = jnp.zeros((NPAN, H, LN), F32)
            col = jnp.sum(sel(wide(lane == l_from), ref[pl.ds(first, NPAN), c_from, rows, :], zero), axis=2, keepdims=True)
            col = jnp.broadcast_to(col, zero.shape)
            return [jnp.sum(sel(wide(mask), col, zero), axis=1, keepdims=True) for mask in masks]

        def wide(mask):
            return jnp.broadcast_to(mask[None], (NPAN, *mask.shape))

        def fill_quadrant(src, sa, sb):
            columns = [beta_column(src, 0, sa, sb, r) for r in range(2)]
            lines = [alpha_lines(src, 0, sa, sb, r) for r in range(2)]
            for r in range(2):
                col, mask, c_to, rows = columns[r]
                src[:, c_to, rows, :] = sel(mask, col, src[:, c_to, rows, :])
                for c in PLANES:
                    CQ[:, r, c] = jnp.broadcast_to(lines[r][c], (NPAN, SB, LN))

        def fill_winds(sa, sb):
            sign = -1.0 if sa == sb else 1.0
            col, mask, c_to, rows = beta_column(WW, WA, sa, sb, 0)
            line = alpha_lines(WW, WB, sa, sb, 0)
            to_b, to_a = pl.ds(WB, NPAN), pl.ds(WA, NPAN)
            WW[to_b, c_to, rows, :] = sel(mask, sign * col, WW[to_b, c_to, rows, :])
            row_lane = lanes_of((NPAN, 1, LN))
            inside = row_lane < GL if sb == 0 else row_lane >= LN - GL
            row = pl.ds(SB * (H + 1), 1) if sa == 0 else pl.ds(SB * (KR - H + 3) - 1, 1)
            for c in PLANES:
                WW[to_a, c, row, :] = sel(inside, sign * line[c], WW[to_a, c, row, :])

        def roll_down(v):
            return pltpu.roll(v, LN - 1, 1)

        def roll_up(v):
            return pltpu.roll(v, 1, 1)

        def beta_rows(src, p, k0, scale):
            rows = pl.ds(SB * (k0 + 2), SB * BETA_ROWS)
            a0, a1, a2 = (src[p, c, rows, :] for c in PLANES)
            a2l, a0r, a1r = roll_up(a2), roll_down(a0), roll_down(a1)
            e0, e1, e2 = a2l + a1, a0 + a2, a1 + a0r
            g0, g1, g2 = 8.0 * a0 - e0, 8.0 * a1 - e1, 8.0 * a2 - e2
            g0r = 8.0 * a0r - (a2 + a1r)
            x0 = WW[WB + p, 0, rows, :] * (g0 + g1)
            x1 = WW[WB + p, 1, rows, :] * (g1 + g2)
            x2 = WW[WB + p, 2, rows, :] * (g2 + g0r)
            x2l = roll_up(x2)
            return jnp.stack([x0 - x2l, x1 - x0, x2 - x1]), jnp.stack([e0, e1, e2])

        def row_group(ref, p, k):
            return ref[p, :, pl.ds(SB * (k + 2), SB), :]

        def panel_pass(src, dst, p, scale, second):
            lane, sub = lanes_of((NC, SB, LN)), rows_of((NC, SB, LN))
            ghost_lane = jnp.logical_or(jnp.logical_and(at_edge(2), lane < GL),
                                        jnp.logical_and(at_edge(3), lane >= LN - GL))
            in_low = jnp.logical_and(ghost_lane, jnp.logical_and(at_edge(0), sub == 0))
            in_high = jnp.logical_and(ghost_lane, jnp.logical_and(at_edge(1), sub == SB - 1))

            def load(k):
                v = row_group(src, p, k)
                if k in (H - 2, H - 1):
                    return sel(in_low, CQ[p, H - 1 - k], v)
                if k in (KR - H, KR - H + 1):
                    return sel(in_high, CQ[p, k - (KR - H)], v)
                return v

            qm, q0, q1 = load(-2), load(-1), load(0)
            q2 = load(1)
            g0 = 8.0 * q0 - (qm + q1)
            e1 = q0 + q2
            g1 = 8.0 * q1 - e1
            x_low = row_group(WW, WA + p, -1) * (g0 + g1)
            q_now, e_now, g_now, q_next = q1, e1, g1, q2
            beta = None
            for k in range(KR):
                if k % BETA_ROWS == 0:
                    beta = beta_rows(src, p, k, scale)
                at = SB * (k % BETA_ROWS)
                tb, eb = (v[:, at:at + SB] for v in beta)
                q_far = load(k + 2)
                e_next = q_now + q_far
                g_next = 8.0 * q_next - e_next
                x_high = row_group(WW, WA + p, k) * (g_now + g_next)
                u = scale * (x_high - x_low + tb) - (e_now + eb)
                new = KK[1, :, pl.ds(SB * k, SB), :] * q_now - KK[0, :, pl.ds(SB * k, SB), :] * u
                if second:
                    new = 0.5 * (row_group(dst, p, k) + new)
                dst[p, :, pl.ds(SB * (k + 2), SB), :] = new
                x_low, q_now, e_now, g_now, q_next = x_high, q_next, e_next, g_next, q_far

        def stage(src, dst, scale, second, more):
            pad_rows(src)

            @pl.when(more)
            def _():
                corner_case(lambda sa, sb: fill_quadrant(src, sa, sb))

            @pl.loop(0, NPAN)
            def _(p):
                panel_pass(src, dst, p, scale, second)

        load_field(a_in, WW, WA)
        load_field(b_in, WW, WB)
        is_cc = jnp.logical_and(jnp.logical_or(at_edge(0), at_edge(1)), jnp.logical_or(at_edge(2), at_edge(3)))
        pl.semaphore_wait(barrier, SB * NPAN - NPAN * sel(is_cc, 1, 0))

        @pl.loop(1, 3)
        def _(f):
            @pl.loop(0, NPAN)
            def _(p):
                pack_strips(WW, (f - 1) * NPAN + p, WW, (2 - f) * NPAN + p, f, p)
            for p in slots:
                turn_strips(f, p, True)
            for p in slots:
                pack_corners(f, p)
            for p in slots:
                start_copies(f, f + 1, p)
        load_field(q_in, QA, 0)

        def finish_winds():
            metric()

            @pl.loop(1, 3)
            def _(f):
                for p in slots:
                    wait_copies(RECV, CRECV, recv_sem, crecv_sem, f + 1, p)

                @pl.loop(0, NPAN)
                def _(p):
                    unpack_cols(WW, (2 - f) * NPAN + p, f + 1, p)

            @pl.loop(1, 3)
            def _(f):
                @pl.loop(0, NPAN)
                def _(p):
                    unpack_rows(WW, (f - 1) * NPAN + p, f + 1, p)
                for p in slots:
                    wait_copies(SEND, CSEND, send_sem, csend_sem, f, p)
            corner_case(fill_winds)
            pad_rows(WW)
            face_scale = 0.5 / (12.0 * 0.5 * C_SPEED)

            @pl.loop(0, NPAN)
            def _(p):
                for c in PLANES:
                    low, high = pl.ds(SB, SB * (KR + 1)), pl.ds(2 * SB, SB * (KR + 1))
                    WW[WA + p, c, low, :] = face_scale * (WW[WA + p, c, low, :] + WW[WA + p, c, high, :])
                rows = pl.ds(2 * SB, SB * KR)
                b0, b1, b2 = (WW[WB + p, c, rows, :] for c in PLANES)
                WW[WB + p, 0, rows, :] = face_scale * (b0 + b1)
                WW[WB + p, 1, rows, :] = face_scale * (b1 + b2)
                WW[WB + p, 2, rows, :] = face_scale * (b2 + roll_down(b0))

        def metric():
            ridx = rows_of((SB * KR, LN))
            gi = tx * tile_rows + lax.rem(ridx, SB) * KR + lax.div(ridx, SB) - H
            gi = sel(gi < 0, -1 - gi, sel(gi >= cells, 2 * cells - 1 - gi, gi))
            tan_a = small_tan((gi.astype(F32) + 0.5) * dalpha - 0.25 * math.pi)
            for c in PLANES:
                gj = ty * tile_rows + 3 * lanes_of((SB, LN)) + c - H
                gj = sel(gj < 0, -1 - gj, sel(gj >= cells, 2 * cells - 1 - gj, gj))
                tan_b = small_tan((gj.astype(F32) + 0.5) * dalpha - 0.25 * math.pi)[0:1, :]
                a_sq, b_sq = tan_a * tan_a, tan_b * tan_b
                r_sq = 1.0 + a_sq + b_sq
                sqrt_g = (1.0 + a_sq) * (1.0 + b_sq) / (r_sq * jnp.sqrt(r_sq))
                KK[0, c] = (0.5 * C_SPEED * CFL_STEP) / sqrt_g
                KK[1, c] = 1.0 - 4.0 * KK[0, c]

        @pl.loop(0, n_blocks)
        def _(b):
            fr = lax.rem(b, 2)

            for p in slots:
                pack_strips(QA, p, QA, p, 0, p)
            for p in slots:
                turn_strips(0, p, False)
            for p in slots:
                pack_corners(0, p)
            for p in slots:
                start_copies(0, fr, p)

            @pl.when(b == 0)
            def _():
                finish_winds()

            for p in slots:
                wait_copies(RECV, CRECV, recv_sem, crecv_sem, fr, p)
            for p in slots:
                unpack_cols(QA, p, fr, p)
            for p in slots:
                unpack_rows(QA, p, fr, p)
            for p in slots:
                wait_copies(SEND, CSEND, send_sem, csend_sem, 0, p)
            end = lax.div((b + 1) * steps, n_blocks)

            @pl.loop(lax.div(b * steps, n_blocks), end)
            def _(t):
                scale = ws_ref[t]
                stage(QA, QB, scale, False, True)
                stage(QB, QA, scale, True, t + 1 < end)

        store_field(QA)

    return kernel


def solution(mesh):
    tile_count = mesh.shape['tx']
    field_spec = P(('member', 'panel'), 'tx', 'ty')
    wind_spec = P('panel', 'tx', 'ty')

    def local_run(tracer, wind_a, wind_b, wind_scale):
        steps = wind_scale.shape[0]
        n_blocks = -(-steps // STEPS_PER_BLOCK)
        ext = SB * KR
        block = pl.BlockSpec((NPAN, ext, ext), lambda n: (0, 0, 0))
        dma = pltpu.SemaphoreType.DMA
        return pl.pallas_call(
            make_kernel(tile_count, steps, n_blocks, tracer.shape[1]),
            grid=(1,),
            out_shape=jax.ShapeDtypeStruct(tracer.shape, F32),
            in_specs=[pl.BlockSpec(memory_space=pltpu.SMEM), block, block, block],
            out_specs=block,
            scratch_shapes=[
                pltpu.VMEM((NPAN, NC, ext + 32, LN), F32),
                pltpu.VMEM((NPAN, NC, ext + 32, LN), F32),
                pltpu.VMEM((2 * NPAN, NC, ext + 32, LN), F32),
                pltpu.VMEM((NPAN, 2, NC, SB, LN), F32),
                pltpu.VMEM((2, NC, ext, LN), F32),
                pltpu.VMEM((NC, ext + 32, LN), F32),
                pltpu.VMEM((NC, ext + 32, LN), F32),
                pltpu.VMEM((9, LN, LN), F32),
                pltpu.VMEM((3, NPAN, 4, NC, H, LN), F32),
                pltpu.VMEM((4, NPAN, 4, NC, H, LN), F32),
                pltpu.VMEM((3, NPAN, 4, H, LN), F32),
                pltpu.VMEM((4, NPAN, 4, H, LN), F32),
                *[dma((n, NPAN, 4)) for n in (3, 4, 3, 4)],
            ],
            compiler_params=pltpu.CompilerParams(collective_id=0, has_side_effects=True, vmem_limit_bytes=60 * 1024 * 1024),
            cost_estimate=pl.CostEstimate(flops=10 ** 9, bytes_accessed=10 ** 7, transcendentals=0),
        )(wind_scale, tracer, wind_a, wind_b)

    return jax.shard_map(local_run, mesh=mesh, in_specs=(field_spec, wind_spec, wind_spec, P()),
                         out_specs=field_spec, check_vma=False)
```

```python
import math
import jax
import numpy as np
import jax.numpy as jnp
from jax import lax
from jax.experimental import pallas as pl
from jax.experimental.pallas import tpu as pltpu
from jax.sharding import PartitionSpec as P

C_SPEED = 2.5
CFL_STEP = 0.12
EDGE_CODE = (
    (310, 100, 530, 420), (10, 200, 511, 410), (110, 300, 521, 431),
    (210, 0, 500, 401), (331, 130, 30, 231), (320, 121, 221, 20),
)
H = 12
KR = 48
NPAN = 3
NC = 3
SB = 8
LN = 128
GL = 4
STEPS_PER_BLOCK = 3
BETA_ROWS = 4
F32 = jnp.float32
PLANES = range(NC)
SIDES = range(4)


def turned_sign(side_id, edge_id):
    return int(side_id % 2 == edge_id % 2)


def small_tan(v):
    sq = v * v
    sin_sum, cos_sum = jnp.full_like(v, 1.0), jnp.full_like(v, 1.0)
    for n in (6, 5, 4, 3, 2, 1):
        sin_sum = 1.0 - sq * sin_sum * (1.0 / (2 * n * (2 * n + 1)))
        cos_sum = 1.0 - sq * cos_sum * (1.0 / (2 * n * (2 * n - 1)))
    return v * sin_sum / cos_sum


def sel(pred, yes, no):
    yes, no = (np.int32(v) if isinstance(v, int) else v for v in (yes, no))
    same = jnp.shape(yes) == jnp.shape(no) and jnp.shape(pred) in ((), jnp.shape(yes))
    return lax.select(pred, yes, no) if same else jnp.where(pred, yes, no)


def lanes_of(shape):
    return lax.broadcasted_iota(jnp.int32, shape, len(shape) - 1)


def rows_of(shape):
    return lax.broadcasted_iota(jnp.int32, shape, len(shape) - 2)


def make_kernel(tile_count, steps, n_blocks, tile_rows):
    last = tile_count - 1
    cells = tile_rows * tile_count
    dalpha = 0.5 * math.pi / cells

    def kernel(ws_ref, q_in, a_in, b_in, out_ref, QA, QB, WW, CQ, KK, NN, TT, ZS, SEND, RECV, CSEND, CRECV,
               send_sem, recv_sem, csend_sem, crecv_sem):
        dev = lax.axis_index('panel')
        tx = lax.axis_index('tx')
        ty = lax.axis_index('ty')
        WA, WB = 0, NPAN

        def at_edge(side):
            return (tx == 0, tx == last, ty == 0, ty == last)[side]

        def pick(v0, v1):
            return v0 if v0 == v1 else v0 + dev * (v1 - v0)

        def neighbour(p, side):
            codes = [EDGE_CODE[NPAN * dv + p][side] for dv in (0, 1)]
            panels = [code // 100 for code in codes]
            edges = [code // 10 % 10 for code in codes]
            return (pick(*[n // NPAN for n in panels]), pick(*[n % NPAN for n in panels]), pick(*edges),
                    pick(*[code % 10 for code in codes]), pick(*[turned_sign(side, e) for e in edges]))

        def dest(p, side, off):
            along = (ty if side < 2 else tx) + off
            edge = at_edge(side)
            d_dev, d_slot, dside, flip, _ = neighbour(p, side)
            al = along + flip * (last - 2 * along)
            c_tx = sel(dside == 0, 0, sel(dside == 1, last, al))
            c_ty = sel(dside == 2, 0, sel(dside == 3, last, al))
            step = 2 * (side % 2) - 1
            in_tx, in_ty = (tx + step, ty + off) if side < 2 else (tx + off, ty + step)
            device = {'tx': sel(edge, c_tx, in_tx), 'ty': sel(edge, c_ty, in_ty),
                      'panel': sel(edge, d_dev, dev)}
            return device, sel(edge, d_slot, p), sel(edge, dside, side ^ 1), sel(edge, flip, 0)

        def corner_plan(p, sa, sb):
            out_b = at_edge(2 + sb)
            plans = []
            for side, end, off in ((sa, sb, 2 * sb - 1), (2 + sb, sa, 2 * sa - 1)):
                device, slot, dside, flip = dest(p, side, off)
                x = end + flip * (1 - 2 * end)
                e = 1 - x
                plans.append((device, slot, sel(dside < 2, 2 * dside + e, 2 * e + (dside - 2)), side, x))
            (dv_a, sl_a, dc_a, s_a, x_a), (dv_b, sl_b, dc_b, s_b, x_b) = plans
            device = {key: sel(out_b, dv_b[key], dv_a[key]) for key in dv_a}
            return (device, sel(out_b, sl_b, sl_a), sel(out_b, dc_b, dc_a),
                    sel(out_b, s_b, s_a), sel(out_b, x_b, x_a))

        def has_corner(sa, sb):
            return jnp.logical_not(jnp.logical_and(at_edge(sa), at_edge(2 + sb)))

        def is_here(device):
            return jnp.logical_and(jnp.logical_and(device['tx'] == tx, device['ty'] == ty), device['panel'] == dev)

        corners = [(sa, sb) for sa in range(2) for sb in range(2)]
        slots = range(NPAN)
        strip_to = [[dest(p, side, 0)[:3] for side in SIDES] for p in slots]
        stays = [[sel(is_here(plan[0]), 1, 0) for plan in row] for row in strip_to]
        corner_to = [[corner_plan(p, sa, sb) for sa, sb in corners] for p in slots]
        flips = [[sel(at_edge(side), neighbour(p, side)[3], 0) for side in SIDES] for p in slots]
        turns = [[sel(at_edge(side), neighbour(p, side)[4], 0) for side in SIDES] for p in slots]

        def at_slot(p, table):
            first = table[0]
            if isinstance(first, dict):
                return {key: at_slot(p, [row[key] for row in table]) for key in first}
            if isinstance(first, (tuple, list)):
                return [at_slot(p, [row[n] for row in table]) for n in range(len(first))]
            return sel(p == 0, first, sel(p == 1, table[1], table[2]))
        mesh_ids = pl.DeviceIdType.MESH

        barrier = pltpu.get_barrier_semaphore()

        for p in slots:
            for side in SIDES:
                pl.semaphore_signal(barrier, inc=1, device_id=strip_to[p][side][0], device_id_type=mesh_ids)
            for (sa, sb), plan in zip(corners, corner_to[p]):
                @pl.when(has_corner(sa, sb))
                def _():
                    pl.semaphore_signal(barrier, inc=1, device_id=plan[0], device_id_type=mesh_ids)

        def load_field(in_ref, dst, base):
            @pl.loop(0, NPAN)
            def _(p):
                for it in PLANES:
                    for jt in PLANES:
                        TT[it, pl.ds(H + LN * jt, LN), :] = in_ref[p, pl.ds(LN * it, LN), pl.ds(LN * jt, LN)].T
                    for c in PLANES:
                        NN[c, pl.ds(H + LN * it, LN), :] = TT[it, pl.ds(c, LN, stride=NC), :].T

                @pl.loop(0, KR // SB)
                def _(kb):
                    for c in PLANES:
                        for k in range(SB):
                            dst[base + p, c, pl.ds(pl.multiple_of(64 * kb + SB * (k + 2), SB), SB), :] = NN[c, pl.ds(SB * kb + k, SB, stride=KR), :]

        def store_field(src):
            @pl.loop(0, NPAN)
            def _(p):
                @pl.loop(0, KR // SB)
                def _(kb):
                    for c in PLANES:
                        for k in range(SB):
                            NN[c, pl.ds(SB * kb + k, SB, stride=KR), :] = src[p, c, pl.ds(pl.multiple_of(64 * kb + SB * (k + 2), SB), SB), :]
                for it in PLANES:
                    for c in PLANES:
                        TT[it, pl.ds(c, LN, stride=NC), :] = NN[c, pl.ds(H + LN * it, LN), :].T
                    for jt in PLANES:
                        out_ref[p, pl.ds(LN * it, LN), pl.ds(LN * jt, LN)] = TT[it, pl.ds(H + LN * jt, LN), :].T

        def quarter(n):
            return pl.ds(GL * n, GL)

        def rows_at(first, s, n):
            return pl.ds(SB * (first + 2 + n) + s, GL, stride=NC * SB)

        def pack_strips(row_ref, row_at, col_ref, col_at, f, p):
            for c in PLANES:
                for n in PLANES:
                    SEND[f, p, 0, c, quarter(n), :] = row_ref[row_at, c, rows_at(H, 0, n), :]
                    SEND[f, p, 1, c, quarter(n), :] = row_ref[row_at, c, rows_at(KR - 2 * H, SB - 1, n), :]
            lane = lanes_of((LN, LN))

            def window(first):
                return jnp.logical_and(lane >= first, lane < first + GL)
            for cp in PLANES:
                mix = None
                for c in PLANES:
                    blk = jnp.concatenate([col_ref[col_at, c, pl.ds(SB * (cp + 2) + s, 2 * SB, stride=NC * SB), :]
                                           for s in range(SB)], axis=0)
                    if c == 0:
                        mix = blk
                    else:
                        mine = jnp.logical_or(window(GL + SB * c), window(SB * (c - 1)))
                        mix = sel(mine, pltpu.roll(blk, SB * c, 1), mix)
                t = mix.T
                for c in PLANES:
                    low, high = GL + SB * c, (LN - SB + SB * c) % LN
                    SEND[f, p, 2, cp, quarter(c), :] = t[low:low + GL]
                    SEND[f, p, 3, cp, quarter(c), :] = t[high:high + GL]

        def turn_strips(f, p, winds):
            flip_at, turn_at = at_slot(p, flips), at_slot(p, turns)
            for side in SIDES:
                @pl.when(flip_at[side] == 1)
                def _():
                    inside = lanes_of((NC * H, LN))
                    inside = jnp.logical_and(inside >= GL, inside < LN - GL)
                    old = jnp.concatenate([SEND[f, p, side, NC - 1 - c] for c in PLANES], axis=0)
                    mirror = (rows_of((LN, LN)) + lanes_of((LN, LN)) == LN - 1).astype(F32)
                    new = jnp.dot(jnp.where(inside, old, 0.0), mirror, precision=lax.Precision.HIGHEST,
                                  preferred_element_type=F32)
                    for c in PLANES:
                        SEND[f, p, side, c] = new[H * c:H * (c + 1)]
                    if winds:
                        @pl.when(f == 2)
                        def _():
                            for c in PLANES:
                                SEND[f, p, side, c] = -SEND[f, p, side, c]

                @pl.when(turn_at[side] == 1)
                def _():
                    for c in PLANES:
                        v = SEND[f, p, side, c]
                        if winds:
                            v = sel(f == 1, -v, v)
                        for m in range(H):
                            SEND[f, p, side, c, m:m + 1, :] = v[H - 1 - m:H - m, :]

        def pack_corners(f, p, plan):
            lane = lanes_of((H, LN))
            for cid, (_, _, _, side, x) in enumerate(plan):
                hi = lo = None
                for c in PLANES:
                    v = SEND[f, p, side, c]
                    vh, vl = pltpu.roll(v, SB + GL * c, 1), pltpu.roll(v, LN - SB - GL * c, 1)
                    hi = vh if c == 0 else sel(lane >= GL * c, vh, hi)
                    lo = vl if c == 0 else sel(lane < LN - GL * c, vl, lo)
                CSEND[f, p, cid] = sel(x == 1, hi, lo)

        def send_panel(row_ref, row_at, col_ref, col_at, f, fr, p, winds):
            pack_strips(row_ref, row_at, col_ref, col_at, f, p)
            turn_strips(f, p, winds)
            plan = at_slot(p, corner_to)
            pack_corners(f, p, plan)
            to, here_at = at_slot(p, strip_to), at_slot(p, stays)
            for side in SIDES:
                device, slot, dside = to[side]

                @pl.when(here_at[side] == 1)
                def _():
                    RECV[fr, slot, dside] = SEND[f, p, side]

                @pl.when(here_at[side] == 0)
                def _():
                    pltpu.make_async_remote_copy(
                        src_ref=SEND.at[f, p, side], dst_ref=RECV.at[fr, slot, dside], send_sem=send_sem.at[f, p, side],
                        recv_sem=recv_sem.at[fr, slot, dside], device_id=device, device_id_type=mesh_ids).start()
            for cid, (sa, sb) in enumerate(corners):
                @pl.when(has_corner(sa, sb))
                def _():
                    device, slot, dcorner, _, _ = plan[cid]
                    pltpu.make_async_remote_copy(
                        src_ref=CSEND.at[f, p, cid], dst_ref=CRECV.at[fr, slot, dcorner], send_sem=csend_sem.at[f, p, cid],
                        recv_sem=crecv_sem.at[fr, slot, dcorner], device_id=device, device_id_type=mesh_ids).start()

        def wait_copies(strips, blocks, sem, csem, f, p):
            for side in SIDES:
                @pl.when(stays[p][side] == 0)
                def _():
                    pltpu.make_async_copy(strips.at[f, p, side], strips.at[f, p, side], sem.at[f, p, side]).wait()
            for cid, (sa, sb) in enumerate(corners):
                @pl.when(has_corner(sa, sb))
                def _():
                    pltpu.make_async_copy(blocks.at[f, p, cid], blocks.at[f, p, cid], csem.at[f, p, cid]).wait()

        def end_valid(side, e):
            if side < 2:
                return jnp.logical_not(at_edge(2 + e))
            return jnp.logical_and(jnp.logical_not(at_edge(e)), at_edge(side))

        def merged(fr, p, side, c):
            lane = lanes_of((H, LN))
            v = RECV[fr, p, side, c]
            for e in range(2):
                cid = 2 * side + e if side < 2 else 2 * e + side - 2
                msg = CRECV[fr, p, cid]
                if c:
                    msg = pltpu.roll(msg, 4 * c if e else LN - 4 * c, 1)
                inside = lane >= 124 if e else lane < 4
                v = sel(jnp.logical_and(inside, end_valid(side, e)), msg, v)
            return v

        def unpack_cols(ref, dst, fr, p):
            lane = lanes_of((2 * SB, LN))
            ghost = jnp.logical_or(lane < GL, lane >= LN - GL)
            for cp in PLANES:
                low, high = merged(fr, p, 2, cp), merged(fr, p, 3, cp)
                z = ZS.at[NC * p + cp]
                for c in PLANES:
                    z[pl.ds(SB * c, GL), :] = low[GL * c:GL * (c + 1)]
                    z[pl.ds((SB * c - GL) % LN, GL), :] = high[GL * c:GL * (c + 1)]
                t = z[...].T
                for c in PLANES:
                    tc = pltpu.roll(t, LN - SB * c, 1) if c else t
                    for s in range(SB):
                        rows = pl.ds(SB * (cp + 2) + s, 2 * SB, stride=NC * SB)
                        ref[dst, c, rows, :] = sel(ghost, tc[2 * SB * s:2 * SB * (s + 1)], ref[dst, c, rows, :])

        def unpack_rows(ref, dst, fr, p):
            lane = lanes_of((GL, LN))
            keep = jnp.logical_and(jnp.logical_or(lane >= GL, end_valid(0, 0)),
                                   jnp.logical_or(lane < LN - GL, end_valid(0, 1)))
            for c in PLANES:
                for side, first, s in ((0, 0, 0), (1, KR - H, SB - 1)):
                    v = merged(fr, p, side, c)
                    for n in PLANES:
                        rows = rows_at(first, s, n)
                        ref[dst, c, rows, :] = sel(keep, v[GL * n:GL * (n + 1)], ref[dst, c, rows, :])

        def pad_rows(ref):
            at = pl.ds(0, NPAN)
            ref[at, :, pl.ds(0, 2 * SB), :] = ref[at, :, pl.ds(SB * KR - 1, 2 * SB), :]
            ref[at, :, pl.ds(SB * (KR + 2), 2 * SB), :] = ref[at, :, pl.ds(2 * SB + 1, 2 * SB), :]

        def corner_case(fn):
            for sa, sb in corners:
                @pl.when(jnp.logical_and(at_edge(sa), at_edge(2 + sb)))
                def _():
                    fn(sa, sb)

        def quad_geom(sa, sb):
            k0, s = (0, 0) if sa == 0 else (KR - H, SB - 1)
            lane0 = 0 if sb == 0 else LN - GL
            lane, idx = lanes_of((H, LN)), rows_of((H, LN))
            col = idx if sa == sb else H - 1 - idx
            masks = [NC * (lane - lane0) + c == col for c in PLANES]
            return k0, s, lane, masks, pl.ds(SB * (k0 + 2) + s, H, stride=SB)

        def beta_column(ref, first, sa, sb, r):
            k0, s, lane, masks, rows = quad_geom(sa, sb)
            kr = H + r if sa == 0 else KR - H - 1 - r
            tot = jnp.zeros((NPAN, H, LN), F32)
            for c in PLANES:
                line = ref[pl.ds(first, NPAN), c, pl.ds(SB * (kr + 2) + s, 1), :]
                tot = sel(wide(masks[c]), jnp.broadcast_to(line, tot.shape), tot)
            l_to, c_to = (GL - 1, NC - 1 - r) if sb == 0 else (LN - GL, r)
            return jnp.broadcast_to(jnp.sum(tot, axis=2, keepdims=True), tot.shape), wide(lane == l_to), c_to, rows

        def alpha_lines(ref, first, sa, sb, r):
            _, _, lane, masks, rows = quad_geom(sa, sb)
            l_from, c_from = (GL, r) if sb == 0 else (LN - GL - 1, NC - 1 - r)
            zero = jnp.zeros((NPAN, H, LN), F32)
            col = jnp.sum(sel(wide(lane == l_from), ref[pl.ds(first, NPAN), c_from, rows, :], zero), axis=2, keepdims=True)
            col = jnp.broadcast_to(col, zero.shape)
            return [jnp.sum(sel(wide(mask), col, zero), axis=1, keepdims=True) for mask in masks]

        def wide(mask):
            return jnp.broadcast_to(mask[None], (NPAN, *mask.shape))

        def fill_quadrant(src, sa, sb):
            columns = [beta_column(src, 0, sa, sb, r) for r in range(2)]
            lines = [alpha_lines(src, 0, sa, sb, r) for r in range(2)]
            for r in range(2):
                col, mask, c_to, rows = columns[r]
                src[:, c_to, rows, :] = sel(mask, col, src[:, c_to, rows, :])
                for c in PLANES:
                    CQ[:, r, c] = jnp.broadcast_to(lines[r][c], (NPAN, SB, LN))

        def fill_winds(sa, sb):
            sign = -1.0 if sa == sb else 1.0
            col, mask, c_to, rows = beta_column(WW, WA, sa, sb, 0)
            line = alpha_lines(WW, WB, sa, sb, 0)
            to_b, to_a = pl.ds(WB, NPAN), pl.ds(WA, NPAN)
            WW[to_b, c_to, rows, :] = sel(mask, sign * col, WW[to_b, c_to, rows, :])
            row_lane = lanes_of((NPAN, 1, LN))
            inside = row_lane < GL if sb == 0 else row_lane >= LN - GL
            row = pl.ds(SB * (H + 1), 1) if sa == 0 else pl.ds(SB * (KR - H + 3) - 1, 1)
            for c in PLANES:
                WW[to_a, c, row, :] = sel(inside, sign * line[c], WW[to_a, c, row, :])

        def roll_down(v):
            return pltpu.roll(v, LN - 1, 1)

        def roll_up(v):
            return pltpu.roll(v, 1, 1)

        def beta_rows(src, p, k0, scale):
            rows = pl.ds(SB * (k0 + 2), SB * BETA_ROWS)
            a0, a1, a2 = (src[p, c, rows, :] for c in PLANES)
            a2l, a0r, a1r = roll_up(a2), roll_down(a0), roll_down(a1)
            e0, e1, e2 = a2l + a1, a0 + a2, a1 + a0r
            g0, g1, g2 = 8.0 * a0 - e0, 8.0 * a1 - e1, 8.0 * a2 - e2
            g0r = 8.0 * a0r - (a2 + a1r)
            x0 = WW[WB + p, 0, rows, :] * (g0 + g1)
            x1 = WW[WB + p, 1, rows, :] * (g1 + g2)
            x2 = WW[WB + p, 2, rows, :] * (g2 + g0r)
            x2l = roll_up(x2)
            return jnp.stack([x0 - x2l, x1 - x0, x2 - x1]), jnp.stack([e0, e1, e2])

        def row_group(ref, p, k):
            return ref[p, :, pl.ds(SB * (k + 2), SB), :]

        def panel_pass(src, dst, p, scale, second):
            lane, sub = lanes_of((NC, SB, LN)), rows_of((NC, SB, LN))
            ghost_lane = jnp.logical_or(jnp.logical_and(at_edge(2), lane < GL),
                                        jnp.logical_and(at_edge(3), lane >= LN - GL))
            in_low = jnp.logical_and(ghost_lane, jnp.logical_and(at_edge(0), sub == 0))
            in_high = jnp.logical_and(ghost_lane, jnp.logical_and(at_edge(1), sub == SB - 1))

            def load(k):
                v = row_group(src, p, k)
                if k in (H - 2, H - 1):
                    return sel(in_low, CQ[p, H - 1 - k], v)
                if k in (KR - H, KR - H + 1):
                    return sel(in_high, CQ[p, k - (KR - H)], v)
                return v

            qm, q0, q1 = load(-2), load(-1), load(0)
            q2 = load(1)
            g0 = 8.0 * q0 - (qm + q1)
            e1 = q0 + q2
            g1 = 8.0 * q1 - e1
            x_low = row_group(WW, WA + p, -1) * (g0 + g1)
            q_now, e_now, g_now, q_next = q1, e1, g1, q2
            beta = None
            for k in range(KR):
                if k % BETA_ROWS == 0:
                    beta = beta_rows(src, p, k, scale)
                at = SB * (k % BETA_ROWS)
                tb, eb = (v[:, at:at + SB] for v in beta)
                q_far = load(k + 2)
                e_next = q_now + q_far
                g_next = 8.0 * q_next - e_next
                x_high = row_group(WW, WA + p, k) * (g_now + g_next)
                u = scale * (x_high - x_low + tb) - (e_now + eb)
                new = KK[1, :, pl.ds(SB * k, SB), :] * q_now - KK[0, :, pl.ds(SB * k, SB), :] * u
                if second:
                    new = 0.5 * (row_group(dst, p, k) + new)
                dst[p, :, pl.ds(SB * (k + 2), SB), :] = new
                x_low, q_now, e_now, g_now, q_next = x_high, q_next, e_next, g_next, q_far

        def stage(src, dst, scale, second, more, after=None):
            pad_rows(src)

            @pl.when(more)
            def _():
                corner_case(lambda sa, sb: fill_quadrant(src, sa, sb))

            @pl.loop(0, NPAN)
            def _(p):
                panel_pass(src, dst, p, scale, second)
                if after is not None:
                    after(p)

        load_field(a_in, WW, WA)
        load_field(b_in, WW, WB)
        is_cc = jnp.logical_and(jnp.logical_or(at_edge(0), at_edge(1)), jnp.logical_or(at_edge(2), at_edge(3)))
        pl.semaphore_wait(barrier, SB * NPAN - NPAN * sel(is_cc, 1, 0))

        @pl.loop(1, 3)
        def _(f):
            @pl.loop(0, NPAN)
            def _(p):
                send_panel(WW, (f - 1) * NPAN + p, WW, (2 - f) * NPAN + p, f, f + 1, p, True)
        load_field(q_in, QA, 0)

        def finish_winds():
            metric()

            @pl.loop(1, 3)
            def _(f):
                for p in slots:
                    wait_copies(RECV, CRECV, recv_sem, crecv_sem, f + 1, p)

                @pl.loop(0, NPAN)
                def _(p):
                    unpack_cols(WW, (2 - f) * NPAN + p, f + 1, p)

            @pl.loop(1, 3)
            def _(f):
                @pl.loop(0, NPAN)
                def _(p):
                    unpack_rows(WW, (f - 1) * NPAN + p, f + 1, p)
                for p in slots:
                    wait_copies(SEND, CSEND, send_sem, csend_sem, f, p)
            corner_case(fill_winds)
            pad_rows(WW)
            face_scale = 0.5 / (12.0 * 0.5 * C_SPEED)

            @pl.loop(0, NPAN)
            def _(p):
                for c in PLANES:
                    low, high = pl.ds(SB, SB * (KR + 1)), pl.ds(2 * SB, SB * (KR + 1))
                    WW[WA + p, c, low, :] = face_scale * (WW[WA + p, c, low, :] + WW[WA + p, c, high, :])
                rows = pl.ds(2 * SB, SB * KR)
                b0, b1, b2 = (WW[WB + p, c, rows, :] for c in PLANES)
                WW[WB + p, 0, rows, :] = face_scale * (b0 + b1)
                WW[WB + p, 1, rows, :] = face_scale * (b1 + b2)
                WW[WB + p, 2, rows, :] = face_scale * (b2 + roll_down(b0))

        def metric():
            ridx = rows_of((SB * KR, LN))
            gi = tx * tile_rows + lax.rem(ridx, SB) * KR + lax.div(ridx, SB) - H
            gi = sel(gi < 0, -1 - gi, sel(gi >= cells, 2 * cells - 1 - gi, gi))
            tan_a = small_tan((gi.astype(F32) + 0.5) * dalpha - 0.25 * math.pi)
            for c in PLANES:
                gj = ty * tile_rows + 3 * lanes_of((SB, LN)) + c - H
                gj = sel(gj < 0, -1 - gj, sel(gj >= cells, 2 * cells - 1 - gj, gj))
                tan_b = small_tan((gj.astype(F32) + 0.5) * dalpha - 0.25 * math.pi)[0:1, :]
                a_sq, b_sq = tan_a * tan_a, tan_b * tan_b
                r_sq = 1.0 + a_sq + b_sq
                sqrt_g = (1.0 + a_sq) * (1.0 + b_sq) / (r_sq * jnp.sqrt(r_sq))
                KK[0, c] = (0.5 * C_SPEED * CFL_STEP) / sqrt_g
                KK[1, c] = 1.0 - 4.0 * KK[0, c]

        @pl.loop(0, n_blocks)
        def _(b):
            fr = lax.rem(b, 2)

            @pl.when(b == 0)
            def _():
                @pl.loop(0, NPAN)
                def _(p):
                    send_panel(QA, p, QA, p, 0, 0, p, False)

            @pl.when(b == 0)
            def _():
                finish_winds()

            for p in slots:
                wait_copies(RECV, CRECV, recv_sem, crecv_sem, fr, p)
            for p in slots:
                unpack_cols(QA, p, fr, p)
            for p in slots:
                unpack_rows(QA, p, fr, p)
            for p in slots:
                wait_copies(SEND, CSEND, send_sem, csend_sem, 0, p)
            end = lax.div((b + 1) * steps, n_blocks)

            @pl.loop(lax.div(b * steps, n_blocks), end)
            def _(t):
                scale = ws_ref[t]
                stage(QA, QB, scale, False, True)

                def after(p):
                    @pl.when(jnp.logical_and(t + 1 == end, b + 1 < n_blocks))
                    def _():
                        send_panel(QA, p, QA, p, 0, 1 - fr, p, False)
                stage(QB, QA, scale, True, t + 1 < end, after)

        store_field(QA)

    return kernel


def solution(mesh):
    tile_count = mesh.shape['tx']
    field_spec = P(('member', 'panel'), 'tx', 'ty')
    wind_spec = P('panel', 'tx', 'ty')

    def local_run(tracer, wind_a, wind_b, wind_scale):
        steps = wind_scale.shape[0]
        n_blocks = -(-steps // STEPS_PER_BLOCK)
        ext = SB * KR
        block = pl.BlockSpec((NPAN, ext, ext), lambda n: (0, 0, 0))
        dma = pltpu.SemaphoreType.DMA
        return pl.pallas_call(
            make_kernel(tile_count, steps, n_blocks, tracer.shape[1]),
            grid=(1,),
            out_shape=jax.ShapeDtypeStruct(tracer.shape, F32),
            in_specs=[pl.BlockSpec(memory_space=pltpu.SMEM), block, block, block],
            out_specs=block,
            scratch_shapes=[
                pltpu.VMEM((NPAN, NC, ext + 32, LN), F32),
                pltpu.VMEM((NPAN, NC, ext + 32, LN), F32),
                pltpu.VMEM((2 * NPAN, NC, ext + 32, LN), F32),
                pltpu.VMEM((NPAN, 2, NC, SB, LN), F32),
                pltpu.VMEM((2, NC, ext, LN), F32),
                pltpu.VMEM((NC, ext + 32, LN), F32),
                pltpu.VMEM((NC, ext + 32, LN), F32),
                pltpu.VMEM((9, LN, LN), F32),
                pltpu.VMEM((3, NPAN, 4, NC, H, LN), F32),
                pltpu.VMEM((4, NPAN, 4, NC, H, LN), F32),
                pltpu.VMEM((3, NPAN, 4, H, LN), F32),
                pltpu.VMEM((4, NPAN, 4, H, LN), F32),
                *[dma((n, NPAN, 4)) for n in (3, 4, 3, 4)],
            ],
            compiler_params=pltpu.CompilerParams(collective_id=0, has_side_effects=True, vmem_limit_bytes=60 * 1024 * 1024),
            cost_estimate=pl.CostEstimate(flops=10 ** 9, bytes_accessed=10 ** 7, transcendentals=0),
        )(wind_scale, tracer, wind_a, wind_b)

    return jax.shard_map(local_run, mesh=mesh, in_specs=(field_spec, wind_spec, wind_spec, P()),
                         out_specs=field_spec, check_vma=False)
```

```python
import math
import jax
import numpy as np
import jax.numpy as jnp
from jax import lax
from jax.experimental import pallas as pl
from jax.experimental.pallas import tpu as pltpu
from jax.sharding import PartitionSpec as P

C_SPEED = 2.5
CFL_STEP = 0.12
EDGE_CODE = (
    (310, 100, 530, 420), (10, 200, 511, 410), (110, 300, 521, 431),
    (210, 0, 500, 401), (331, 130, 30, 231), (320, 121, 221, 20),
)
H = 12
KR = 48
NPAN = 3
NC = 3
SB = 8
LN = 128
GL = 4
BETA_SHIFT = 71
STEPS_PER_BLOCK = 3
BETA_ROWS = 4
F32 = jnp.float32
PLANES = range(NC)
SIDES = range(4)


def turned_sign(side_id, edge_id):
    return int(side_id % 2 == edge_id % 2)


def small_tan(v):
    sq = v * v
    sin_sum, cos_sum = jnp.full_like(v, 1.0), jnp.full_like(v, 1.0)
    for n in (6, 5, 4, 3, 2, 1):
        sin_sum = 1.0 - sq * sin_sum * (1.0 / (2 * n * (2 * n + 1)))
        cos_sum = 1.0 - sq * cos_sum * (1.0 / (2 * n * (2 * n - 1)))
    return v * sin_sum / cos_sum


def sel(pred, yes, no):
    yes, no = (np.int32(v) if isinstance(v, int) else v for v in (yes, no))
    same = jnp.shape(yes) == jnp.shape(no) and jnp.shape(pred) in ((), jnp.shape(yes))
    return lax.select(pred, yes, no) if same else jnp.where(pred, yes, no)


def lanes_of(shape):
    return lax.broadcasted_iota(jnp.int32, shape, len(shape) - 1)


def rows_of(shape):
    return lax.broadcasted_iota(jnp.int32, shape, len(shape) - 2)


def make_kernel(tile_count, steps, n_blocks, tile_rows):
    last = tile_count - 1
    cells = tile_rows * tile_count
    dalpha = 0.5 * math.pi / cells

    def kernel(ws_ref, q_in, a_in, b_in, out_ref, QA, QB, WW, CQ, KK, NN, TT, ZS, SEND, RECV, CSEND, CRECV,
               send_sem, recv_sem, csend_sem, crecv_sem):
        dev = lax.axis_index('panel')
        tx = lax.axis_index('tx')
        ty = lax.axis_index('ty')
        WA, WB = 0, NPAN

        def at_edge(side):
            return (tx == 0, tx == last, ty == 0, ty == last)[side]

        def pick(v0, v1):
            return v0 if v0 == v1 else v0 + dev * (v1 - v0)

        def neighbour(p, side):
            codes = [EDGE_CODE[NPAN * dv + p][side] for dv in (0, 1)]
            panels = [code // 100 for code in codes]
            edges = [code // 10 % 10 for code in codes]
            return (pick(*[n // NPAN for n in panels]), pick(*[n % NPAN for n in panels]), pick(*edges),
                    pick(*[code % 10 for code in codes]), pick(*[turned_sign(side, e) for e in edges]))

        def dest(p, side, off):
            along = (ty if side < 2 else tx) + off
            edge = at_edge(side)
            d_dev, d_slot, dside, flip, _ = neighbour(p, side)
            al = along + flip * (last - 2 * along)
            c_tx = sel(dside == 0, 0, sel(dside == 1, last, al))
            c_ty = sel(dside == 2, 0, sel(dside == 3, last, al))
            step = 2 * (side % 2) - 1
            in_tx, in_ty = (tx + step, ty + off) if side < 2 else (tx + off, ty + step)
            device = {'tx': sel(edge, c_tx, in_tx), 'ty': sel(edge, c_ty, in_ty),
                      'panel': sel(edge, d_dev, dev)}
            return device, sel(edge, d_slot, p), sel(edge, dside, side ^ 1), sel(edge, flip, 0)

        def corner_plan(p, sa, sb):
            out_b = at_edge(2 + sb)
            plans = []
            for side, end, off in ((sa, sb, 2 * sb - 1), (2 + sb, sa, 2 * sa - 1)):
                device, slot, dside, flip = dest(p, side, off)
                x = end + flip * (1 - 2 * end)
                e = 1 - x
                plans.append((device, slot, sel(dside < 2, 2 * dside + e, 2 * e + (dside - 2)), side, x,
                              sel(dside < 2, 0, 1)))
            device = {key: sel(out_b, plans[1][0][key], plans[0][0][key]) for key in plans[0][0]}
            return (device, *[sel(out_b, second, first) for first, second in zip(plans[0][1:], plans[1][1:])])

        def has_corner(sa, sb):
            return jnp.logical_not(jnp.logical_and(at_edge(sa), at_edge(2 + sb)))

        def is_here(device):
            return jnp.logical_and(jnp.logical_and(device['tx'] == tx, device['ty'] == ty), device['panel'] == dev)

        corners = [(sa, sb) for sa in range(2) for sb in range(2)]
        slots = range(NPAN)
        strip_to = [[dest(p, side, 0)[:3] for side in SIDES] for p in slots]
        stays = [[sel(is_here(plan[0]), 1, 0) for plan in row] for row in strip_to]
        corner_to = [[corner_plan(p, sa, sb) for sa, sb in corners] for p in slots]
        flips = [[sel(at_edge(side), neighbour(p, side)[3], 0) for side in SIDES] for p in slots]
        turns = [[sel(at_edge(side), neighbour(p, side)[4], 0) for side in SIDES] for p in slots]

        def at_slot(p, table):
            first = table[0]
            if isinstance(first, dict):
                return {key: at_slot(p, [row[key] for row in table]) for key in first}
            if isinstance(first, (tuple, list)):
                return [at_slot(p, [row[n] for row in table]) for n in range(len(first))]
            return sel(p == 0, first, sel(p == 1, table[1], table[2]))
        mesh_ids = pl.DeviceIdType.MESH

        barrier = pltpu.get_barrier_semaphore()

        for p in slots:
            for side in SIDES:
                pl.semaphore_signal(barrier, inc=1, device_id=strip_to[p][side][0], device_id_type=mesh_ids)
            for (sa, sb), plan in zip(corners, corner_to[p]):
                @pl.when(has_corner(sa, sb))
                def _():
                    pl.semaphore_signal(barrier, inc=1, device_id=plan[0], device_id_type=mesh_ids)

        def load_field(in_ref, dst, base):
            @pl.loop(0, NPAN)
            def _(p):
                for it in PLANES:
                    for jt in PLANES:
                        TT[it, pl.ds(H + LN * jt, LN), :] = in_ref[p, pl.ds(LN * it, LN), pl.ds(LN * jt, LN)].T
                    for c in PLANES:
                        NN[c, pl.ds(H + LN * it, LN), :] = TT[it, pl.ds(c, LN, stride=NC), :].T

                @pl.loop(0, KR // SB)
                def _(kb):
                    for c in PLANES:
                        for k in range(SB):
                            dst[base + p, c, pl.ds(pl.multiple_of(64 * kb + SB * (k + 2), SB), SB), :] = NN[c, pl.ds(SB * kb + k, SB, stride=KR), :]

        def store_field(src):
            @pl.loop(0, NPAN)
            def _(p):
                @pl.loop(0, KR // SB)
                def _(kb):
                    for c in PLANES:
                        for k in range(SB):
                            NN[c, pl.ds(SB * kb + k, SB, stride=KR), :] = src[p, c, pl.ds(pl.multiple_of(64 * kb + SB * (k + 2), SB), SB), :]
                for it in PLANES:
                    for c in PLANES:
                        TT[it, pl.ds(c, LN, stride=NC), :] = NN[c, pl.ds(H + LN * it, LN), :].T
                    for jt in PLANES:
                        out_ref[p, pl.ds(LN * it, LN), pl.ds(LN * jt, LN)] = TT[it, pl.ds(H + LN * jt, LN), :].T

        def quarter(n):
            return pl.ds(GL * n, GL)

        def rows_at(first, s, n):
            return pl.ds(SB * (first + 2 + n) + s, GL, stride=NC * SB)

        def pack_strips(row_ref, row_at, col_ref, col_at, f, p):
            for c in PLANES:
                for n in PLANES:
                    SEND[f, p, 0, c, quarter(n), :] = row_ref[row_at, c, rows_at(H, 0, n), :]
                    SEND[f, p, 1, c, quarter(n), :] = row_ref[row_at, c, rows_at(KR - 2 * H, SB - 1, n), :]
            lane = lanes_of((LN, LN))

            def window(first):
                return jnp.logical_and(lane >= first, lane < first + GL)
            planes = [col_ref[col_at, c, pl.ds(2 * SB, SB * KR), :].reshape(2 * SB, NC * SB, LN) for c in PLANES]
            for cp in PLANES:
                mix = None
                for c in PLANES:
                    blk = planes[c][:, SB * cp:SB * (cp + 1)].reshape(LN, LN)
                    if c == 0:
                        mix = blk
                    else:
                        mine = jnp.logical_or(window(GL + SB * c), window(SB * (c - 1)))
                        mix = sel(mine, pltpu.roll(blk, SB * c, 1), mix)
                t = mix.T
                for c in PLANES:
                    low, high = GL + SB * c, (LN - SB + SB * c) % LN
                    SEND[f, p, 2, cp, quarter(c), :] = t[low:low + GL]
                    SEND[f, p, 3, cp, quarter(c), :] = t[high:high + GL]

        def beta_order(lane):
            return 2 * SB * lax.rem(lane, SB) + lax.div(lane, SB)

        def beta_lane(n):
            return SB * lax.rem(n, 2 * SB) + lax.div(n, 2 * SB)

        def turn_strips(f, p, winds):
            flip_at, turn_at, to = at_slot(p, flips), at_slot(p, turns), at_slot(p, strip_to)
            for side in SIDES:
                to_beta = to[side][2] >= 2
                moved = jnp.logical_not(to_beta) if side >= 2 else to_beta

                @pl.when(jnp.logical_or(flip_at[side] == 1, moved))
                def _():
                    back = flip_at[side] == 1
                    at = lanes_of((NC * H, LN))
                    at = beta_order(at) if side >= 2 else at
                    inside = jnp.logical_and(at >= GL, at < LN - GL)
                    now = [SEND[f, p, side, c] for c in PLANES]
                    old = jnp.concatenate([sel(back, now[NC - 1 - c], now[c]) for c in PLANES], axis=0)
                    come = lanes_of((LN, LN))
                    come = sel(to_beta, beta_order(come), come)
                    come = sel(back, LN - 1 - come, come)
                    come = beta_lane(come) if side >= 2 else come
                    place = (rows_of((LN, LN)) == come).astype(F32)
                    new = jnp.dot(sel(inside, old, jnp.zeros_like(old)), place, precision=lax.Precision.HIGHEST,
                                  preferred_element_type=F32)
                    for c in PLANES:
                        SEND[f, p, side, c] = new[H * c:H * (c + 1)]
                    if winds:
                        @pl.when(jnp.logical_and(f == 2, back))
                        def _():
                            for c in PLANES:
                                SEND[f, p, side, c] = -SEND[f, p, side, c]

                @pl.when(turn_at[side] == 1)
                def _():
                    for c in PLANES:
                        v = SEND[f, p, side, c]
                        if winds:
                            v = sel(f == 1, -v, v)
                        for m in range(H):
                            SEND[f, p, side, c, m:m + 1, :] = v[H - 1 - m:H - m, :]

        def pack_corners(f, p, plan):
            lane = lanes_of((H, LN))
            for cid, (_, _, _, side, x, to_beta) in enumerate(plan):
                beta, high = to_beta == 1, x == 1
                key = sel(beta, lax.rem(lane, SB), lane)
                key = sel(high, key, sel(beta, SB - 1, LN - 1) - key)
                step = sel(beta, 1, GL)
                first = sel(beta, LN - BETA_SHIFT, SB)
                msg = None
                for c in PLANES:
                    shift = sel(high, first + step * c, LN - first - step * c)
                    v = pltpu.roll(SEND[f, p, side, c], shift, 1)
                    msg = v if c == 0 else sel(key >= step * c, v, msg)
                CSEND[f, p, cid] = msg

        def send_panel(row_ref, row_at, col_ref, col_at, f, fr, p, winds):
            pack_strips(row_ref, row_at, col_ref, col_at, f, p)
            turn_strips(f, p, winds)
            plan = at_slot(p, corner_to)
            pack_corners(f, p, plan)
            to, here_at = at_slot(p, strip_to), at_slot(p, stays)
            for side in SIDES:
                device, slot, dside = to[side]

                @pl.when(here_at[side] == 1)
                def _():
                    RECV[fr, slot, dside] = SEND[f, p, side]

                @pl.when(here_at[side] == 0)
                def _():
                    pltpu.make_async_remote_copy(
                        src_ref=SEND.at[f, p, side], dst_ref=RECV.at[fr, slot, dside], send_sem=send_sem.at[f, p, side],
                        recv_sem=recv_sem.at[fr, slot, dside], device_id=device, device_id_type=mesh_ids).start()
            for cid, (sa, sb) in enumerate(corners):
                @pl.when(has_corner(sa, sb))
                def _():
                    device, slot, dcorner = plan[cid][:3]
                    pltpu.make_async_remote_copy(
                        src_ref=CSEND.at[f, p, cid], dst_ref=CRECV.at[fr, slot, dcorner], send_sem=csend_sem.at[f, p, cid],
                        recv_sem=crecv_sem.at[fr, slot, dcorner], device_id=device, device_id_type=mesh_ids).start()

        def wait_copies(strips, blocks, sem, csem, f, p):
            for side in SIDES:
                @pl.when(stays[p][side] == 0)
                def _():
                    pltpu.make_async_copy(strips.at[f, p, side], strips.at[f, p, side], sem.at[f, p, side]).wait()
            for cid, (sa, sb) in enumerate(corners):
                @pl.when(has_corner(sa, sb))
                def _():
                    pltpu.make_async_copy(blocks.at[f, p, cid], blocks.at[f, p, cid], csem.at[f, p, cid]).wait()

        def end_valid(side, e):
            if side < 2:
                return jnp.logical_not(at_edge(2 + e))
            return jnp.logical_and(jnp.logical_not(at_edge(e)), at_edge(side))

        def merged(fr, p, side, c):
            lane = lanes_of((H, LN))
            v = RECV[fr, p, side, c]
            for e in range(2):
                cid = 2 * side + e if side < 2 else 2 * e + side - 2
                msg = CRECV[fr, p, cid]
                step = c if side >= 2 else GL * c
                if c:
                    msg = pltpu.roll(msg, step if e else LN - step, 1)
                at = beta_order(lane) if side >= 2 else lane
                inside = at >= LN - GL if e else at < GL
                v = sel(jnp.logical_and(inside, end_valid(side, e)), msg, v)
            return v

        def unpack_cols(ref, dst, fr, p):
            parts = []
            for cp in PLANES:
                low, high = merged(fr, p, 2, cp), merged(fr, p, 3, cp)
                z = ZS.at[NC * p + cp]
                for c in PLANES:
                    z[pl.ds(SB * c, GL), :] = low[GL * c:GL * (c + 1)]
                    z[pl.ds((SB * c - GL) % LN, GL), :] = high[GL * c:GL * (c + 1)]
                t = z[...].T
                parts.append([(pltpu.roll(t, LN - SB * c, 1) if c else t).reshape(2 * SB, SB, LN) for c in PLANES])
            lane = lanes_of((SB * KR, LN))
            ghost = jnp.logical_or(lane < GL, lane >= LN - GL)
            rows = pl.ds(2 * SB, SB * KR)
            for c in PLANES:
                new = jnp.concatenate([part[c] for part in parts], axis=1).reshape(SB * KR, LN)
                ref[dst, c, rows, :] = sel(ghost, new, ref[dst, c, rows, :])

        def unpack_rows(ref, dst, fr, p):
            lane = lanes_of((GL, LN))
            keep = jnp.logical_and(jnp.logical_or(lane >= GL, end_valid(0, 0)),
                                   jnp.logical_or(lane < LN - GL, end_valid(0, 1)))
            for c in PLANES:
                for side, first, s in ((0, 0, 0), (1, KR - H, SB - 1)):
                    v = merged(fr, p, side, c)
                    for n in PLANES:
                        rows = rows_at(first, s, n)
                        ref[dst, c, rows, :] = sel(keep, v[GL * n:GL * (n + 1)], ref[dst, c, rows, :])

        def pad_rows(ref):
            at = pl.ds(0, NPAN)
            ref[at, :, pl.ds(0, 2 * SB), :] = ref[at, :, pl.ds(SB * KR - 1, 2 * SB), :]
            ref[at, :, pl.ds(SB * (KR + 2), 2 * SB), :] = ref[at, :, pl.ds(2 * SB + 1, 2 * SB), :]

        def corner_case(fn):
            for sa, sb in corners:
                @pl.when(jnp.logical_and(at_edge(sa), at_edge(2 + sb)))
                def _():
                    fn(sa, sb)

        def quad_geom(sa, sb):
            k0, s = (0, 0) if sa == 0 else (KR - H, SB - 1)
            lane0 = 0 if sb == 0 else LN - GL
            lane, idx = lanes_of((H, LN)), rows_of((H, LN))
            col = idx if sa == sb else H - 1 - idx
            masks = [NC * (lane - lane0) + c == col for c in PLANES]
            return k0, s, lane, masks, pl.ds(SB * (k0 + 2) + s, H, stride=SB)

        def beta_column(ref, first, sa, sb, r):
            k0, s, lane, masks, rows = quad_geom(sa, sb)
            kr = H + r if sa == 0 else KR - H - 1 - r
            tot = jnp.zeros((NPAN, H, LN), F32)
            for c in PLANES:
                line = ref[pl.ds(first, NPAN), c, pl.ds(SB * (kr + 2) + s, 1), :]
                tot = sel(wide(masks[c]), jnp.broadcast_to(line, tot.shape), tot)
            l_to, c_to = (GL - 1, NC - 1 - r) if sb == 0 else (LN - GL, r)
            return jnp.broadcast_to(jnp.sum(tot, axis=2, keepdims=True), tot.shape), wide(lane == l_to), c_to, rows

        def alpha_lines(ref, first, sa, sb, r):
            _, _, lane, masks, rows = quad_geom(sa, sb)
            l_from, c_from = (GL, r) if sb == 0 else (LN - GL - 1, NC - 1 - r)
            zero = jnp.zeros((NPAN, H, LN), F32)
            col = jnp.sum(sel(wide(lane == l_from), ref[pl.ds(first, NPAN), c_from, rows, :], zero), axis=2, keepdims=True)
            col = jnp.broadcast_to(col, zero.shape)
            return [jnp.sum(sel(wide(mask), col, zero), axis=1, keepdims=True) for mask in masks]

        def wide(mask):
            return jnp.broadcast_to(mask[None], (NPAN, *mask.shape))

        def fill_quadrant(src, sa, sb):
            columns = [beta_column(src, 0, sa, sb, r) for r in range(2)]
            lines = [alpha_lines(src, 0, sa, sb, r) for r in range(2)]
            for r in range(2):
                col, mask, c_to, rows = columns[r]
                src[:, c_to, rows, :] = sel(mask, col, src[:, c_to, rows, :])
                for c in PLANES:
                    CQ[:, r, c] = jnp.broadcast_to(lines[r][c], (NPAN, SB, LN))

        def fill_winds(sa, sb):
            sign = -1.0 if sa == sb else 1.0
            col, mask, c_to, rows = beta_column(WW, WA, sa, sb, 0)
            line = alpha_lines(WW, WB, sa, sb, 0)
            to_b, to_a = pl.ds(WB, NPAN), pl.ds(WA, NPAN)
            WW[to_b, c_to, rows, :] = sel(mask, sign * col, WW[to_b, c_to, rows, :])
            row_lane = lanes_of((NPAN, 1, LN))
            inside = row_lane < GL if sb == 0 else row_lane >= LN - GL
            row = pl.ds(SB * (H + 1), 1) if sa == 0 else pl.ds(SB * (KR - H + 3) - 1, 1)
            for c in PLANES:
                WW[to_a, c, row, :] = sel(inside, sign * line[c], WW[to_a, c, row, :])

        def roll_down(v):
            return pltpu.roll(v, LN - 1, 1)

        def roll_up(v):
            return pltpu.roll(v, 1, 1)

        def beta_rows(src, p, k0, scale):
            rows = pl.ds(SB * (k0 + 2), SB * BETA_ROWS)
            a0, a1, a2 = (src[p, c, rows, :] for c in PLANES)
            a2l, a0r, a1r = roll_up(a2), roll_down(a0), roll_down(a1)
            e0, e1, e2 = a2l + a1, a0 + a2, a1 + a0r
            g0, g1, g2 = 8.0 * a0 - e0, 8.0 * a1 - e1, 8.0 * a2 - e2
            g0r = 8.0 * a0r - (a2 + a1r)
            x0 = WW[WB + p, 0, rows, :] * (g0 + g1)
            x1 = WW[WB + p, 1, rows, :] * (g1 + g2)
            x2 = WW[WB + p, 2, rows, :] * (g2 + g0r)
            x2l = roll_up(x2)
            return jnp.stack([x0 - x2l, x1 - x0, x2 - x1]), jnp.stack([e0, e1, e2])

        def row_group(ref, p, k):
            return ref[p, :, pl.ds(SB * (k + 2), SB), :]

        def panel_pass(src, dst, p, scale, second):
            lane, sub = lanes_of((NC, SB, LN)), rows_of((NC, SB, LN))
            ghost_lane = jnp.logical_or(jnp.logical_and(at_edge(2), lane < GL),
                                        jnp.logical_and(at_edge(3), lane >= LN - GL))
            in_low = jnp.logical_and(ghost_lane, jnp.logical_and(at_edge(0), sub == 0))
            in_high = jnp.logical_and(ghost_lane, jnp.logical_and(at_edge(1), sub == SB - 1))

            def load(k):
                v = row_group(src, p, k)
                if k in (H - 2, H - 1):
                    return sel(in_low, CQ[p, H - 1 - k], v)
                if k in (KR - H, KR - H + 1):
                    return sel(in_high, CQ[p, k - (KR - H)], v)
                return v

            qm, q0, q1 = load(-2), load(-1), load(0)
            q2 = load(1)
            g0 = 8.0 * q0 - (qm + q1)
            e1 = q0 + q2
            g1 = 8.0 * q1 - e1
            x_low = row_group(WW, WA + p, -1) * (g0 + g1)
            q_now, e_now, g_now, q_next = q1, e1, g1, q2
            beta = None
            for k in range(KR):
                if k % BETA_ROWS == 0:
                    beta = beta_rows(src, p, k, scale)
                at = SB * (k % BETA_ROWS)
                tb, eb = (v[:, at:at + SB] for v in beta)
                q_far = load(k + 2)
                e_next = q_now + q_far
                g_next = 8.0 * q_next - e_next
                x_high = row_group(WW, WA + p, k) * (g_now + g_next)
                u = scale * (x_high - x_low + tb) - (e_now + eb)
                new = KK[1, :, pl.ds(SB * k, SB), :] * q_now - KK[0, :, pl.ds(SB * k, SB), :] * u
                if second:
                    new = 0.5 * (row_group(dst, p, k) + new)
                dst[p, :, pl.ds(SB * (k + 2), SB), :] = new
                x_low, q_now, e_now, g_now, q_next = x_high, q_next, e_next, g_next, q_far

        def stage(src, dst, scale, second, more, after=None):
            pad_rows(src)

            @pl.when(more)
            def _():
                corner_case(lambda sa, sb: fill_quadrant(src, sa, sb))

            @pl.loop(0, NPAN)
            def _(p):
                panel_pass(src, dst, p, scale, second)
                if after is not None:
                    after(p)

        load_field(a_in, WW, WA)
        load_field(b_in, WW, WB)
        is_cc = jnp.logical_and(jnp.logical_or(at_edge(0), at_edge(1)), jnp.logical_or(at_edge(2), at_edge(3)))
        pl.semaphore_wait(barrier, SB * NPAN - NPAN * sel(is_cc, 1, 0))

        @pl.loop(1, 3)
        def _(f):
            @pl.loop(0, NPAN)
            def _(p):
                send_panel(WW, (f - 1) * NPAN + p, WW, (2 - f) * NPAN + p, f, f + 1, p, True)
        load_field(q_in, QA, 0)

        def finish_winds():
            metric()

            @pl.loop(1, 3)
            def _(f):
                for p in slots:
                    wait_copies(RECV, CRECV, recv_sem, crecv_sem, f + 1, p)

                @pl.loop(0, NPAN)
                def _(p):
                    unpack_cols(WW, (2 - f) * NPAN + p, f + 1, p)

            @pl.loop(1, 3)
            def _(f):
                @pl.loop(0, NPAN)
                def _(p):
                    unpack_rows(WW, (f - 1) * NPAN + p, f + 1, p)
                for p in slots:
                    wait_copies(SEND, CSEND, send_sem, csend_sem, f, p)
            corner_case(fill_winds)
            pad_rows(WW)
            face_scale = 0.5 / (12.0 * 0.5 * C_SPEED)

            @pl.loop(0, NPAN)
            def _(p):
                for c in PLANES:
                    low, high = pl.ds(SB, SB * (KR + 1)), pl.ds(2 * SB, SB * (KR + 1))
                    WW[WA + p, c, low, :] = face_scale * (WW[WA + p, c, low, :] + WW[WA + p, c, high, :])
                rows = pl.ds(2 * SB, SB * KR)
                b0, b1, b2 = (WW[WB + p, c, rows, :] for c in PLANES)
                WW[WB + p, 0, rows, :] = face_scale * (b0 + b1)
                WW[WB + p, 1, rows, :] = face_scale * (b1 + b2)
                WW[WB + p, 2, rows, :] = face_scale * (b2 + roll_down(b0))

        def metric():
            ridx = rows_of((SB * KR, LN))
            gi = tx * tile_rows + lax.rem(ridx, SB) * KR + lax.div(ridx, SB) - H
            gi = sel(gi < 0, -1 - gi, sel(gi >= cells, 2 * cells - 1 - gi, gi))
            tan_a = small_tan((gi.astype(F32) + 0.5) * dalpha - 0.25 * math.pi)
            for c in PLANES:
                gj = ty * tile_rows + 3 * lanes_of((SB, LN)) + c - H
                gj = sel(gj < 0, -1 - gj, sel(gj >= cells, 2 * cells - 1 - gj, gj))
                tan_b = small_tan((gj.astype(F32) + 0.5) * dalpha - 0.25 * math.pi)[0:1, :]
                a_sq, b_sq = tan_a * tan_a, tan_b * tan_b
                r_sq = 1.0 + a_sq + b_sq
                sqrt_g = (1.0 + a_sq) * (1.0 + b_sq) / (r_sq * jnp.sqrt(r_sq))
                KK[0, c] = (0.5 * C_SPEED * CFL_STEP) / sqrt_g
                KK[1, c] = 1.0 - 4.0 * KK[0, c]

        @pl.loop(0, n_blocks)
        def _(b):
            fr = lax.rem(b, 2)

            @pl.when(b == 0)
            def _():
                @pl.loop(0, NPAN)
                def _(p):
                    send_panel(QA, p, QA, p, 0, 0, p, False)

            @pl.when(b == 0)
            def _():
                finish_winds()

            for p in slots:
                wait_copies(RECV, CRECV, recv_sem, crecv_sem, fr, p)
            for p in slots:
                unpack_cols(QA, p, fr, p)
            for p in slots:
                unpack_rows(QA, p, fr, p)
            for p in slots:
                wait_copies(SEND, CSEND, send_sem, csend_sem, 0, p)
            end = lax.div((b + 1) * steps, n_blocks)

            @pl.loop(lax.div(b * steps, n_blocks), end)
            def _(t):
                scale = ws_ref[t]
                stage(QA, QB, scale, False, True)

                def after(p):
                    @pl.when(jnp.logical_and(t + 1 == end, b + 1 < n_blocks))
                    def _():
                        send_panel(QA, p, QA, p, 0, 1 - fr, p, False)
                stage(QB, QA, scale, True, t + 1 < end, after)

        store_field(QA)

    return kernel


def solution(mesh):
    tile_count = mesh.shape['tx']
    field_spec = P(('member', 'panel'), 'tx', 'ty')
    wind_spec = P('panel', 'tx', 'ty')

    def local_run(tracer, wind_a, wind_b, wind_scale):
        steps = wind_scale.shape[0]
        n_blocks = -(-steps // STEPS_PER_BLOCK)
        ext = SB * KR
        block = pl.BlockSpec((NPAN, ext, ext), lambda n: (0, 0, 0))
        dma = pltpu.SemaphoreType.DMA
        return pl.pallas_call(
            make_kernel(tile_count, steps, n_blocks, tracer.shape[1]),
            grid=(1,),
            out_shape=jax.ShapeDtypeStruct(tracer.shape, F32),
            in_specs=[pl.BlockSpec(memory_space=pltpu.SMEM), block, block, block],
            out_specs=block,
            scratch_shapes=[
                pltpu.VMEM((NPAN, NC, ext + 32, LN), F32),
                pltpu.VMEM((NPAN, NC, ext + 32, LN), F32),
                pltpu.VMEM((2 * NPAN, NC, ext + 32, LN), F32),
                pltpu.VMEM((NPAN, 2, NC, SB, LN), F32),
                pltpu.VMEM((2, NC, ext, LN), F32),
                pltpu.VMEM((NC, ext + 32, LN), F32),
                pltpu.VMEM((NC, ext + 32, LN), F32),
                pltpu.VMEM((9, LN, LN), F32),
                pltpu.VMEM((3, NPAN, 4, NC, H, LN), F32),
                pltpu.VMEM((4, NPAN, 4, NC, H, LN), F32),
                pltpu.VMEM((3, NPAN, 4, H, LN), F32),
                pltpu.VMEM((4, NPAN, 4, H, LN), F32),
                *[dma((n, NPAN, 4)) for n in (3, 4, 3, 4)],
            ],
            compiler_params=pltpu.CompilerParams(collective_id=0, has_side_effects=True, vmem_limit_bytes=60 * 1024 * 1024),
            cost_estimate=pl.CostEstimate(flops=10 ** 9, bytes_accessed=10 ** 7, transcendentals=0),
        )(wind_scale, tracer, wind_a, wind_b)

    return jax.shard_map(local_run, mesh=mesh, in_specs=(field_spec, wind_spec, wind_spec, P()),
                         out_specs=field_spec, check_vma=False)
```

```python
import math
import jax
import numpy as np
import jax.numpy as jnp
from jax import lax
from jax.experimental import pallas as pl
from jax.experimental.pallas import tpu as pltpu
from jax.sharding import PartitionSpec as P

C_SPEED = 2.5
CFL_STEP = 0.12
EDGE_CODE = (
    (310, 100, 530, 420), (10, 200, 511, 410), (110, 300, 521, 431),
    (210, 0, 500, 401), (331, 130, 30, 231), (320, 121, 221, 20),
)
H = 12
KR = 48
NPAN = 3
NC = 3
SB = 8
LN = 128
GL = 4
BETA_SHIFT = 71
STEPS_PER_BLOCK = 3
BETA_ROWS = 4
F32 = jnp.float32
PLANES = range(NC)
SIDES = range(4)


def turned_sign(side_id, edge_id):
    return int(side_id % 2 == edge_id % 2)


def small_tan(v):
    sq = v * v
    sin_sum, cos_sum = jnp.full_like(v, 1.0), jnp.full_like(v, 1.0)
    for n in (6, 5, 4, 3, 2, 1):
        sin_sum = 1.0 - sq * sin_sum * (1.0 / (2 * n * (2 * n + 1)))
        cos_sum = 1.0 - sq * cos_sum * (1.0 / (2 * n * (2 * n - 1)))
    return v * sin_sum / cos_sum


def sel(pred, yes, no):
    yes, no = (np.int32(v) if isinstance(v, int) else v for v in (yes, no))
    same = jnp.shape(yes) == jnp.shape(no) and jnp.shape(pred) in ((), jnp.shape(yes))
    return lax.select(pred, yes, no) if same else jnp.where(pred, yes, no)


def lanes_of(shape):
    return lax.broadcasted_iota(jnp.int32, shape, len(shape) - 1)


def rows_of(shape):
    return lax.broadcasted_iota(jnp.int32, shape, len(shape) - 2)


def make_kernel(tile_count, steps, n_blocks, tile_rows):
    last = tile_count - 1
    cells = tile_rows * tile_count
    dalpha = 0.5 * math.pi / cells

    def kernel(ws_ref, q_in, a_in, b_in, out_ref, QA, QB, WW, CQ, KK, NN, TT, ZS, SEND, RECV, CSEND, CRECV,
               send_sem, recv_sem, csend_sem, crecv_sem):
        dev = lax.axis_index('panel')
        tx = lax.axis_index('tx')
        ty = lax.axis_index('ty')
        WA, WB = 0, NPAN

        def at_edge(side):
            return (tx == 0, tx == last, ty == 0, ty == last)[side]

        def pick(v0, v1):
            return v0 if v0 == v1 else v0 + dev * (v1 - v0)

        def neighbour(p, side):
            codes = [EDGE_CODE[NPAN * dv + p][side] for dv in (0, 1)]
            panels = [code // 100 for code in codes]
            edges = [code // 10 % 10 for code in codes]
            return (pick(*[n // NPAN for n in panels]), pick(*[n % NPAN for n in panels]), pick(*edges),
                    pick(*[code % 10 for code in codes]), pick(*[turned_sign(side, e) for e in edges]))

        def dest(p, side, off):
            along = (ty if side < 2 else tx) + off
            edge = at_edge(side)
            d_dev, d_slot, dside, flip, _ = neighbour(p, side)
            al = along + flip * (last - 2 * along)
            c_tx = sel(dside == 0, 0, sel(dside == 1, last, al))
            c_ty = sel(dside == 2, 0, sel(dside == 3, last, al))
            step = 2 * (side % 2) - 1
            in_tx, in_ty = (tx + step, ty + off) if side < 2 else (tx + off, ty + step)
            device = {'tx': sel(edge, c_tx, in_tx), 'ty': sel(edge, c_ty, in_ty),
                      'panel': sel(edge, d_dev, dev)}
            return device, sel(edge, d_slot, p), sel(edge, dside, side ^ 1), sel(edge, flip, 0)

        def corner_plan(p, sa, sb):
            out_b = at_edge(2 + sb)
            plans = []
            for side, end, off in ((sa, sb, 2 * sb - 1), (2 + sb, sa, 2 * sa - 1)):
                device, slot, dside, flip = dest(p, side, off)
                x = end + flip * (1 - 2 * end)
                e = 1 - x
                plans.append((device, slot, sel(dside < 2, 2 * dside + e, 2 * e + (dside - 2)), side, x,
                              sel(dside < 2, 0, 1)))
            device = {key: sel(out_b, plans[1][0][key], plans[0][0][key]) for key in plans[0][0]}
            return (device, *[sel(out_b, second, first) for first, second in zip(plans[0][1:], plans[1][1:])])

        def has_corner(sa, sb):
            return jnp.logical_not(jnp.logical_and(at_edge(sa), at_edge(2 + sb)))

        def is_here(device):
            return jnp.logical_and(jnp.logical_and(device['tx'] == tx, device['ty'] == ty), device['panel'] == dev)

        corners = [(sa, sb) for sa in range(2) for sb in range(2)]
        slots = range(NPAN)
        strip_to = [[dest(p, side, 0)[:3] for side in SIDES] for p in slots]
        stays = [[sel(is_here(plan[0]), 1, 0) for plan in row] for row in strip_to]
        corner_to = [[corner_plan(p, sa, sb) for sa, sb in corners] for p in slots]
        flips = [[sel(at_edge(side), neighbour(p, side)[3], 0) for side in SIDES] for p in slots]
        turns = [[sel(at_edge(side), neighbour(p, side)[4], 0) for side in SIDES] for p in slots]

        def at_slot(p, table):
            first = table[0]
            if isinstance(first, dict):
                return {key: at_slot(p, [row[key] for row in table]) for key in first}
            if isinstance(first, (tuple, list)):
                return [at_slot(p, [row[n] for row in table]) for n in range(len(first))]
            return sel(p == 0, first, sel(p == 1, table[1], table[2]))
        mesh_ids = pl.DeviceIdType.MESH

        barrier = pltpu.get_barrier_semaphore()

        for p in slots:
            for side in SIDES:
                pl.semaphore_signal(barrier, inc=1, device_id=strip_to[p][side][0], device_id_type=mesh_ids)
            for (sa, sb), plan in zip(corners, corner_to[p]):
                @pl.when(has_corner(sa, sb))
                def _():
                    pl.semaphore_signal(barrier, inc=1, device_id=plan[0], device_id_type=mesh_ids)

        def load_field(in_ref, dst, base):
            @pl.loop(0, NPAN)
            def _(p):
                for it in PLANES:
                    for jt in PLANES:
                        TT[it, pl.ds(H + LN * jt, LN), :] = in_ref[p, pl.ds(LN * it, LN), pl.ds(LN * jt, LN)].T
                    for c in PLANES:
                        NN[c, pl.ds(H + LN * it, LN), :] = TT[it, pl.ds(c, LN, stride=NC), :].T

                @pl.loop(0, KR // SB)
                def _(kb):
                    for c in PLANES:
                        for k in range(SB):
                            dst[base + p, c, pl.ds(pl.multiple_of(64 * kb + SB * (k + 2), SB), SB), :] = NN[c, pl.ds(SB * kb + k, SB, stride=KR), :]

        def store_field(src):
            @pl.loop(0, NPAN)
            def _(p):
                @pl.loop(0, KR // SB)
                def _(kb):
                    for c in PLANES:
                        for k in range(SB):
                            NN[c, pl.ds(SB * kb + k, SB, stride=KR), :] = src[p, c, pl.ds(pl.multiple_of(64 * kb + SB * (k + 2), SB), SB), :]
                for it in PLANES:
                    for c in PLANES:
                        TT[it, pl.ds(c, LN, stride=NC), :] = NN[c, pl.ds(H + LN * it, LN), :].T
                    for jt in PLANES:
                        out_ref[p, pl.ds(LN * it, LN), pl.ds(LN * jt, LN)] = TT[it, pl.ds(H + LN * jt, LN), :].T

        def quarter(n):
            return pl.ds(GL * n, GL)

        def rows_at(first, s, n):
            return pl.ds(SB * (first + 2 + n) + s, GL, stride=NC * SB)

        def pack_strips(row_ref, row_at, col_ref, col_at, f, p):
            for c in PLANES:
                for n in PLANES:
                    SEND[f, p, 0, c, quarter(n), :] = row_ref[row_at, c, rows_at(H, 0, n), :]
                    SEND[f, p, 1, c, quarter(n), :] = row_ref[row_at, c, rows_at(KR - 2 * H, SB - 1, n), :]
            lane = lanes_of((LN, LN))

            def window(first):
                return jnp.logical_and(lane >= first, lane < first + GL)
            planes = [col_ref[col_at, c, pl.ds(2 * SB, SB * KR), :].reshape(2 * SB, NC * SB, LN) for c in PLANES]
            for cp in PLANES:
                mix = None
                for c in PLANES:
                    blk = planes[c][:, SB * cp:SB * (cp + 1)].reshape(LN, LN)
                    if c == 0:
                        mix = blk
                    else:
                        mine = jnp.logical_or(window(GL + SB * c), window(SB * (c - 1)))
                        mix = sel(mine, pltpu.roll(blk, SB * c, 1), mix)
                t = mix.T
                for c in PLANES:
                    low, high = GL + SB * c, (LN - SB + SB * c) % LN
                    SEND[f, p, 2, cp, quarter(c), :] = t[low:low + GL]
                    SEND[f, p, 3, cp, quarter(c), :] = t[high:high + GL]

        def beta_order(lane):
            return 2 * SB * lax.rem(lane, SB) + lax.div(lane, SB)

        def beta_lane(n):
            return SB * lax.rem(n, 2 * SB) + lax.div(n, 2 * SB)

        def turn_strips(f, p, winds):
            flip_at, turn_at, to = at_slot(p, flips), at_slot(p, turns), at_slot(p, strip_to)
            for side in SIDES:
                to_beta = to[side][2] >= 2
                moved = jnp.logical_not(to_beta) if side >= 2 else to_beta

                @pl.when(jnp.logical_or(flip_at[side] == 1, moved))
                def _():
                    back = flip_at[side] == 1
                    at = lanes_of((NC * H, LN))
                    at = beta_order(at) if side >= 2 else at
                    inside = jnp.logical_and(at >= GL, at < LN - GL)
                    now = [SEND[f, p, side, c] for c in PLANES]
                    old = jnp.concatenate([sel(back, now[NC - 1 - c], now[c]) for c in PLANES], axis=0)
                    come = lanes_of((LN, LN))
                    come = sel(to_beta, beta_order(come), come)
                    come = sel(back, LN - 1 - come, come)
                    come = beta_lane(come) if side >= 2 else come
                    place = (rows_of((LN, LN)) == come).astype(F32)
                    new = jnp.dot(sel(inside, old, jnp.zeros_like(old)), place, precision=lax.Precision.HIGHEST,
                                  preferred_element_type=F32)
                    for c in PLANES:
                        SEND[f, p, side, c] = new[H * c:H * (c + 1)]
                    if winds:
                        @pl.when(jnp.logical_and(f == 2, back))
                        def _():
                            for c in PLANES:
                                SEND[f, p, side, c] = -SEND[f, p, side, c]

                @pl.when(turn_at[side] == 1)
                def _():
                    for c in PLANES:
                        v = SEND[f, p, side, c]
                        if winds:
                            v = sel(f == 1, -v, v)
                        for m in range(H):
                            SEND[f, p, side, c, m:m + 1, :] = v[H - 1 - m:H - m, :]

        def pack_corners(f, p, plan):
            lane = lanes_of((H, LN))
            for cid, (_, _, _, side, x, to_beta) in enumerate(plan):
                beta, high = to_beta == 1, x == 1
                key = sel(beta, lax.rem(lane, SB), lane)
                key = sel(high, key, sel(beta, SB - 1, LN - 1) - key)
                step = sel(beta, 1, GL)
                first = sel(beta, LN - BETA_SHIFT, SB)
                msg = None
                for c in PLANES:
                    shift = sel(high, first + step * c, LN - first - step * c)
                    v = pltpu.roll(SEND[f, p, side, c], shift, 1)
                    msg = v if c == 0 else sel(key >= step * c, v, msg)
                CSEND[f, p, cid] = msg

        def send_panel(row_ref, row_at, col_ref, col_at, f, fr, p, winds):
            pack_strips(row_ref, row_at, col_ref, col_at, f, p)
            turn_strips(f, p, winds)
            plan = at_slot(p, corner_to)
            pack_corners(f, p, plan)
            to, here_at = at_slot(p, strip_to), at_slot(p, stays)
            for side in SIDES:
                device, slot, dside = to[side]

                @pl.when(here_at[side] == 1)
                def _():
                    RECV[fr, slot, dside] = SEND[f, p, side]

                @pl.when(here_at[side] == 0)
                def _():
                    pltpu.make_async_remote_copy(
                        src_ref=SEND.at[f, p, side], dst_ref=RECV.at[fr, slot, dside], send_sem=send_sem.at[f, p, side],
                        recv_sem=recv_sem.at[fr, slot, dside], device_id=device, device_id_type=mesh_ids).start()
            for cid, (sa, sb) in enumerate(corners):
                @pl.when(has_corner(sa, sb))
                def _():
                    device, slot, dcorner = plan[cid][:3]
                    pltpu.make_async_remote_copy(
                        src_ref=CSEND.at[f, p, cid], dst_ref=CRECV.at[fr, slot, dcorner], send_sem=csend_sem.at[f, p, cid],
                        recv_sem=crecv_sem.at[fr, slot, dcorner], device_id=device, device_id_type=mesh_ids).start()

        def wait_copies(strips, blocks, sem, csem, f, p):
            for side in SIDES:
                @pl.when(stays[p][side] == 0)
                def _():
                    pltpu.make_async_copy(strips.at[f, p, side], strips.at[f, p, side], sem.at[f, p, side]).wait()
            for cid, (sa, sb) in enumerate(corners):
                @pl.when(has_corner(sa, sb))
                def _():
                    pltpu.make_async_copy(blocks.at[f, p, cid], blocks.at[f, p, cid], csem.at[f, p, cid]).wait()

        def end_valid(side, e):
            if side < 2:
                return jnp.logical_not(at_edge(2 + e))
            return jnp.logical_and(jnp.logical_not(at_edge(e)), at_edge(side))

        def merged(fr, p, side, c):
            lane = lanes_of((H, LN))
            v = RECV[fr, p, side, c]
            for e in range(2):
                cid = 2 * side + e if side < 2 else 2 * e + side - 2
                msg = CRECV[fr, p, cid]
                step = c if side >= 2 else GL * c
                if c:
                    msg = pltpu.roll(msg, step if e else LN - step, 1)
                at = beta_order(lane) if side >= 2 else lane
                inside = at >= LN - GL if e else at < GL
                v = sel(jnp.logical_and(inside, end_valid(side, e)), msg, v)
            return v

        def unpack_cols(ref, dst, fr, p):
            parts = []
            for cp in PLANES:
                low, high = merged(fr, p, 2, cp), merged(fr, p, 3, cp)
                z = ZS.at[NC * p + cp]
                for c in PLANES:
                    z[pl.ds(SB * c, GL), :] = low[GL * c:GL * (c + 1)]
                    z[pl.ds((SB * c - GL) % LN, GL), :] = high[GL * c:GL * (c + 1)]
                t = z[...].T
                parts.append([(pltpu.roll(t, LN - SB * c, 1) if c else t).reshape(2 * SB, SB, LN) for c in PLANES])
            lane = lanes_of((SB * KR, LN))
            ghost = jnp.logical_or(lane < GL, lane >= LN - GL)
            rows = pl.ds(2 * SB, SB * KR)
            for c in PLANES:
                new = jnp.concatenate([part[c] for part in parts], axis=1).reshape(SB * KR, LN)
                ref[dst, c, rows, :] = sel(ghost, new, ref[dst, c, rows, :])

        def unpack_rows(ref, dst, fr, p):
            lane = lanes_of((GL, LN))
            keep = jnp.logical_and(jnp.logical_or(lane >= GL, end_valid(0, 0)),
                                   jnp.logical_or(lane < LN - GL, end_valid(0, 1)))
            for c in PLANES:
                for side, first, s in ((0, 0, 0), (1, KR - H, SB - 1)):
                    v = merged(fr, p, side, c)
                    for n in PLANES:
                        rows = rows_at(first, s, n)
                        ref[dst, c, rows, :] = sel(keep, v[GL * n:GL * (n + 1)], ref[dst, c, rows, :])

        def pad_rows(ref):
            at = pl.ds(0, NPAN)
            ref[at, :, pl.ds(0, 2 * SB), :] = ref[at, :, pl.ds(SB * KR - 1, 2 * SB), :]
            ref[at, :, pl.ds(SB * (KR + 2), 2 * SB), :] = ref[at, :, pl.ds(2 * SB + 1, 2 * SB), :]

        def corner_case(fn):
            for sa, sb in corners:
                @pl.when(jnp.logical_and(at_edge(sa), at_edge(2 + sb)))
                def _():
                    fn(sa, sb)

        def quad_geom(sa, sb):
            k0, s = (0, 0) if sa == 0 else (KR - H, SB - 1)
            lane0 = 0 if sb == 0 else LN - GL
            lane, idx = lanes_of((H, LN)), rows_of((H, LN))
            col = idx if sa == sb else H - 1 - idx
            masks = [NC * (lane - lane0) + c == col for c in PLANES]
            return k0, s, lane, masks, pl.ds(SB * (k0 + 2) + s, H, stride=SB)

        def beta_column(ref, first, sa, sb, r):
            k0, s, lane, masks, rows = quad_geom(sa, sb)
            kr = H + r if sa == 0 else KR - H - 1 - r
            tot = jnp.zeros((NPAN, H, LN), F32)
            for c in PLANES:
                line = ref[pl.ds(first, NPAN), c, pl.ds(SB * (kr + 2) + s, 1), :]
                tot = sel(wide(masks[c]), jnp.broadcast_to(line, tot.shape), tot)
            l_to, c_to = (GL - 1, NC - 1 - r) if sb == 0 else (LN - GL, r)
            return jnp.broadcast_to(jnp.sum(tot, axis=2, keepdims=True), tot.shape), wide(lane == l_to), c_to, rows

        def alpha_lines(ref, first, sa, sb, r):
            _, _, lane, masks, rows = quad_geom(sa, sb)
            l_from, c_from = (GL, r) if sb == 0 else (LN - GL - 1, NC - 1 - r)
            zero = jnp.zeros((NPAN, H, LN), F32)
            col = jnp.sum(sel(wide(lane == l_from), ref[pl.ds(first, NPAN), c_from, rows, :], zero), axis=2, keepdims=True)
            col = jnp.broadcast_to(col, zero.shape)
            return [jnp.sum(sel(wide(mask), col, zero), axis=1, keepdims=True) for mask in masks]

        def wide(mask):
            return jnp.broadcast_to(mask[None], (NPAN, *mask.shape))

        def fill_quadrant(src, sa, sb):
            columns = [beta_column(src, 0, sa, sb, r) for r in range(2)]
            lines = [alpha_lines(src, 0, sa, sb, r) for r in range(2)]
            for r in range(2):
                col, mask, c_to, rows = columns[r]
                src[:, c_to, rows, :] = sel(mask, col, src[:, c_to, rows, :])
                for c in PLANES:
                    CQ[:, r, c] = jnp.broadcast_to(lines[r][c], (NPAN, SB, LN))

        def fill_winds(sa, sb):
            sign = -1.0 if sa == sb else 1.0
            col, mask, c_to, rows = beta_column(WW, WA, sa, sb, 0)
            line = alpha_lines(WW, WB, sa, sb, 0)
            to_b, to_a = pl.ds(WB, NPAN), pl.ds(WA, NPAN)
            WW[to_b, c_to, rows, :] = sel(mask, sign * col, WW[to_b, c_to, rows, :])
            row_lane = lanes_of((NPAN, 1, LN))
            inside = row_lane < GL if sb == 0 else row_lane >= LN - GL
            row = pl.ds(SB * (H + 1), 1) if sa == 0 else pl.ds(SB * (KR - H + 3) - 1, 1)
            for c in PLANES:
                WW[to_a, c, row, :] = sel(inside, sign * line[c], WW[to_a, c, row, :])

        def roll_down(v):
            return pltpu.roll(v, LN - 1, 1)

        def roll_up(v):
            return pltpu.roll(v, 1, 1)

        def beta_rows(src, p, k0, scale):
            rows = pl.ds(SB * (k0 + 2), SB * BETA_ROWS)
            a0, a1, a2 = (src[p, c, rows, :] for c in PLANES)
            a2l, a0r, a1r = roll_up(a2), roll_down(a0), roll_down(a1)
            e0, e1, e2 = a2l + a1, a0 + a2, a1 + a0r
            g0, g1, g2 = 8.0 * a0 - e0, 8.0 * a1 - e1, 8.0 * a2 - e2
            g0r = 8.0 * a0r - (a2 + a1r)
            x0 = WW[WB + p, 0, rows, :] * (g0 + g1)
            x1 = WW[WB + p, 1, rows, :] * (g1 + g2)
            x2 = WW[WB + p, 2, rows, :] * (g2 + g0r)
            x2l = roll_up(x2)
            return jnp.stack([scale * (x0 - x2l) - e0, scale * (x1 - x0) - e1, scale * (x2 - x1) - e2])

        def row_group(ref, p, k):
            return ref[p, :, pl.ds(SB * (k + 2), SB), :]

        def panel_pass(src, dst, p, scale, second):
            lane, sub = lanes_of((NC, SB, LN)), rows_of((NC, SB, LN))
            ghost_lane = jnp.logical_or(jnp.logical_and(at_edge(2), lane < GL),
                                        jnp.logical_and(at_edge(3), lane >= LN - GL))
            in_low = jnp.logical_and(ghost_lane, jnp.logical_and(at_edge(0), sub == 0))
            in_high = jnp.logical_and(ghost_lane, jnp.logical_and(at_edge(1), sub == SB - 1))

            def load(k):
                v = row_group(src, p, k)
                if k in (H - 2, H - 1):
                    return sel(in_low, CQ[p, H - 1 - k], v)
                if k in (KR - H, KR - H + 1):
                    return sel(in_high, CQ[p, k - (KR - H)], v)
                return v

            qm, q0, q1 = load(-2), load(-1), load(0)
            q2 = load(1)
            g0 = 8.0 * q0 - (qm + q1)
            e1 = q0 + q2
            g1 = 8.0 * q1 - e1
            x_low = row_group(WW, WA + p, -1) * (g0 + g1)
            q_now, e_now, g_now, q_next = q1, e1, g1, q2
            beta = None
            for k in range(KR):
                if k % BETA_ROWS == 0:
                    beta = beta_rows(src, p, k, scale)
                at = SB * (k % BETA_ROWS)
                tb = beta[:, at:at + SB]
                q_far = load(k + 2)
                e_next = q_now + q_far
                g_next = 8.0 * q_next - e_next
                x_high = row_group(WW, WA + p, k) * (g_now + g_next)
                u = scale * (x_high - x_low) - e_now + tb + 4.0 * q_now
                new = q_now - KK[:, pl.ds(SB * k, SB), :] * u
                if second:
                    new = 0.5 * (row_group(dst, p, k) + new)
                dst[p, :, pl.ds(SB * (k + 2), SB), :] = new
                x_low, q_now, e_now, g_now, q_next = x_high, q_next, e_next, g_next, q_far

        def stage(src, dst, scale, second, more, after=None):
            pad_rows(src)

            @pl.when(more)
            def _():
                corner_case(lambda sa, sb: fill_quadrant(src, sa, sb))

            @pl.loop(0, NPAN)
            def _(p):
                panel_pass(src, dst, p, scale, second)
                if after is not None:
                    after(p)

        load_field(a_in, WW, WA)
        load_field(b_in, WW, WB)
        is_cc = jnp.logical_and(jnp.logical_or(at_edge(0), at_edge(1)), jnp.logical_or(at_edge(2), at_edge(3)))
        pl.semaphore_wait(barrier, SB * NPAN - NPAN * sel(is_cc, 1, 0))

        @pl.loop(1, 3)
        def _(f):
            @pl.loop(0, NPAN)
            def _(p):
                send_panel(WW, (f - 1) * NPAN + p, WW, (2 - f) * NPAN + p, f, f + 1, p, True)
        load_field(q_in, QA, 0)

        def finish_winds():
            metric()

            @pl.loop(1, 3)
            def _(f):
                for p in slots:
                    wait_copies(RECV, CRECV, recv_sem, crecv_sem, f + 1, p)

                @pl.loop(0, NPAN)
                def _(p):
                    unpack_cols(WW, (2 - f) * NPAN + p, f + 1, p)

            @pl.loop(1, 3)
            def _(f):
                @pl.loop(0, NPAN)
                def _(p):
                    unpack_rows(WW, (f - 1) * NPAN + p, f + 1, p)
                for p in slots:
                    wait_copies(SEND, CSEND, send_sem, csend_sem, f, p)
            corner_case(fill_winds)
            pad_rows(WW)
            face_scale = 0.5 / (12.0 * 0.5 * C_SPEED)

            @pl.loop(0, NPAN)
            def _(p):
                for c in PLANES:
                    low, high = pl.ds(SB, SB * (KR + 1)), pl.ds(2 * SB, SB * (KR + 1))
                    WW[WA + p, c, low, :] = face_scale * (WW[WA + p, c, low, :] + WW[WA + p, c, high, :])
                rows = pl.ds(2 * SB, SB * KR)
                b0, b1, b2 = (WW[WB + p, c, rows, :] for c in PLANES)
                WW[WB + p, 0, rows, :] = face_scale * (b0 + b1)
                WW[WB + p, 1, rows, :] = face_scale * (b1 + b2)
                WW[WB + p, 2, rows, :] = face_scale * (b2 + roll_down(b0))

        def metric():
            ridx = rows_of((SB * KR, LN))
            gi = tx * tile_rows + lax.rem(ridx, SB) * KR + lax.div(ridx, SB) - H
            gi = sel(gi < 0, -1 - gi, sel(gi >= cells, 2 * cells - 1 - gi, gi))
            tan_a = small_tan((gi.astype(F32) + 0.5) * dalpha - 0.25 * math.pi)
            for c in PLANES:
                gj = ty * tile_rows + 3 * lanes_of((SB, LN)) + c - H
                gj = sel(gj < 0, -1 - gj, sel(gj >= cells, 2 * cells - 1 - gj, gj))
                tan_b = small_tan((gj.astype(F32) + 0.5) * dalpha - 0.25 * math.pi)[0:1, :]
                a_sq, b_sq = tan_a * tan_a, tan_b * tan_b
                r_sq = 1.0 + a_sq + b_sq
                sqrt_g = (1.0 + a_sq) * (1.0 + b_sq) / (r_sq * jnp.sqrt(r_sq))
                KK[c] = (0.5 * C_SPEED * CFL_STEP) / sqrt_g

        @pl.loop(0, n_blocks)
        def _(b):
            fr = lax.rem(b, 2)

            @pl.when(b == 0)
            def _():
                @pl.loop(0, NPAN)
                def _(p):
                    send_panel(QA, p, QA, p, 0, 0, p, False)

            @pl.when(b == 0)
            def _():
                finish_winds()

            for p in slots:
                wait_copies(RECV, CRECV, recv_sem, crecv_sem, fr, p)
            for p in slots:
                unpack_cols(QA, p, fr, p)
            for p in slots:
                unpack_rows(QA, p, fr, p)
            for p in slots:
                wait_copies(SEND, CSEND, send_sem, csend_sem, 0, p)
            end = lax.div((b + 1) * steps, n_blocks)

            @pl.loop(lax.div(b * steps, n_blocks), end)
            def _(t):
                scale = ws_ref[t]
                stage(QA, QB, scale, False, True)

                def after(p):
                    @pl.when(jnp.logical_and(t + 1 == end, b + 1 < n_blocks))
                    def _():
                        send_panel(QA, p, QA, p, 0, 1 - fr, p, False)
                stage(QB, QA, scale, True, t + 1 < end, after)

        store_field(QA)

    return kernel


def solution(mesh):
    tile_count = mesh.shape['tx']
    field_spec = P(('member', 'panel'), 'tx', 'ty')
    wind_spec = P('panel', 'tx', 'ty')

    def local_run(tracer, wind_a, wind_b, wind_scale):
        steps = wind_scale.shape[0]
        n_blocks = -(-steps // STEPS_PER_BLOCK)
        ext = SB * KR
        block = pl.BlockSpec((NPAN, ext, ext), lambda n: (0, 0, 0))
        dma = pltpu.SemaphoreType.DMA
        return pl.pallas_call(
            make_kernel(tile_count, steps, n_blocks, tracer.shape[1]),
            grid=(1,),
            out_shape=jax.ShapeDtypeStruct(tracer.shape, F32),
            in_specs=[pl.BlockSpec(memory_space=pltpu.SMEM), block, block, block],
            out_specs=block,
            scratch_shapes=[
                pltpu.VMEM((NPAN, NC, ext + 32, LN), F32),
                pltpu.VMEM((NPAN, NC, ext + 32, LN), F32),
                pltpu.VMEM((2 * NPAN, NC, ext + 32, LN), F32),
                pltpu.VMEM((NPAN, 2, NC, SB, LN), F32),
                pltpu.VMEM((NC, ext, LN), F32),
                pltpu.VMEM((NC, ext + 32, LN), F32),
                pltpu.VMEM((NC, ext + 32, LN), F32),
                pltpu.VMEM((9, LN, LN), F32),
                pltpu.VMEM((3, NPAN, 4, NC, H, LN), F32),
                pltpu.VMEM((4, NPAN, 4, NC, H, LN), F32),
                pltpu.VMEM((3, NPAN, 4, H, LN), F32),
                pltpu.VMEM((4, NPAN, 4, H, LN), F32),
                *[dma((n, NPAN, 4)) for n in (3, 4, 3, 4)],
            ],
            compiler_params=pltpu.CompilerParams(collective_id=0, has_side_effects=True, vmem_limit_bytes=60 * 1024 * 1024),
            cost_estimate=pl.CostEstimate(flops=10 ** 9, bytes_accessed=10 ** 7, transcendentals=0),
        )(wind_scale, tracer, wind_a, wind_b)

    return jax.shard_map(local_run, mesh=mesh, in_specs=(field_spec, wind_spec, wind_spec, P()),
                         out_specs=field_spec, check_vma=False)
```

```python
import math
import jax
import numpy as np
import jax.numpy as jnp
from jax import lax
from jax.experimental import pallas as pl
from jax.experimental.pallas import tpu as pltpu
from jax.sharding import PartitionSpec as P

C_SPEED = 2.5
CFL_STEP = 0.12
EDGE_CODE = (
    (310, 100, 530, 420), (10, 200, 511, 410), (110, 300, 521, 431),
    (210, 0, 500, 401), (331, 130, 30, 231), (320, 121, 221, 20),
)
H = 12
KR = 48
NPAN = 3
NC = 3
SB = 8
LN = 128
GL = 4
BETA_SHIFT = 71
STEPS_PER_BLOCK = 3
BETA_ROWS = 4
F32 = jnp.float32
PLANES = range(NC)
SIDES = range(4)


def turned_sign(side_id, edge_id):
    return int(side_id % 2 == edge_id % 2)


def small_tan(v):
    sq = v * v
    sin_sum, cos_sum = jnp.full_like(v, 1.0), jnp.full_like(v, 1.0)
    for n in (6, 5, 4, 3, 2, 1):
        sin_sum = 1.0 - sq * sin_sum * (1.0 / (2 * n * (2 * n + 1)))
        cos_sum = 1.0 - sq * cos_sum * (1.0 / (2 * n * (2 * n - 1)))
    return v * sin_sum / cos_sum


def sel(pred, yes, no):
    yes, no = (np.int32(v) if isinstance(v, int) else v for v in (yes, no))
    same = jnp.shape(yes) == jnp.shape(no) and jnp.shape(pred) in ((), jnp.shape(yes))
    return lax.select(pred, yes, no) if same else jnp.where(pred, yes, no)


def lanes_of(shape):
    return lax.broadcasted_iota(jnp.int32, shape, len(shape) - 1)


def rows_of(shape):
    return lax.broadcasted_iota(jnp.int32, shape, len(shape) - 2)


def make_kernel(tile_count, steps, n_blocks, tile_rows):
    last = tile_count - 1
    cells = tile_rows * tile_count
    dalpha = 0.5 * math.pi / cells

    def kernel(ws_ref, q_in, a_in, b_in, out_ref, QA, QB, WW, CQ, KK, NN, TT, ZS, SEND, RECV, CSEND, CRECV,
               send_sem, recv_sem, csend_sem, crecv_sem):
        dev = lax.axis_index('panel')
        tx = lax.axis_index('tx')
        ty = lax.axis_index('ty')
        WA, WB = 0, NPAN

        def at_edge(side):
            return (tx == 0, tx == last, ty == 0, ty == last)[side]

        def pick(v0, v1):
            return v0 if v0 == v1 else v0 + dev * (v1 - v0)

        def neighbour(p, side):
            codes = [EDGE_CODE[NPAN * dv + p][side] for dv in (0, 1)]
            panels = [code // 100 for code in codes]
            edges = [code // 10 % 10 for code in codes]
            return (pick(*[n // NPAN for n in panels]), pick(*[n % NPAN for n in panels]), pick(*edges),
                    pick(*[code % 10 for code in codes]), pick(*[turned_sign(side, e) for e in edges]))

        def dest(p, side, off):
            along = (ty if side < 2 else tx) + off
            edge = at_edge(side)
            d_dev, d_slot, dside, flip, _ = neighbour(p, side)
            al = along + flip * (last - 2 * along)
            c_tx = sel(dside == 0, 0, sel(dside == 1, last, al))
            c_ty = sel(dside == 2, 0, sel(dside == 3, last, al))
            step = 2 * (side % 2) - 1
            in_tx, in_ty = (tx + step, ty + off) if side < 2 else (tx + off, ty + step)
            device = {'tx': sel(edge, c_tx, in_tx), 'ty': sel(edge, c_ty, in_ty),
                      'panel': sel(edge, d_dev, dev)}
            return device, sel(edge, d_slot, p), sel(edge, dside, side ^ 1), sel(edge, flip, 0)

        def corner_plan(p, sa, sb):
            out_b = at_edge(2 + sb)
            plans = []
            for side, end, off in ((sa, sb, 2 * sb - 1), (2 + sb, sa, 2 * sa - 1)):
                device, slot, dside, flip = dest(p, side, off)
                x = end + flip * (1 - 2 * end)
                e = 1 - x
                plans.append((device, slot, sel(dside < 2, 2 * dside + e, 2 * e + (dside - 2)), side, x,
                              sel(dside < 2, 0, 1)))
            device = {key: sel(out_b, plans[1][0][key], plans[0][0][key]) for key in plans[0][0]}
            return (device, *[sel(out_b, second, first) for first, second in zip(plans[0][1:], plans[1][1:])])

        def has_corner(sa, sb):
            return jnp.logical_not(jnp.logical_and(at_edge(sa), at_edge(2 + sb)))

        def is_here(device):
            return jnp.logical_and(jnp.logical_and(device['tx'] == tx, device['ty'] == ty), device['panel'] == dev)

        corners = [(sa, sb) for sa in range(2) for sb in range(2)]
        slots = range(NPAN)
        strip_to = [[dest(p, side, 0)[:3] for side in SIDES] for p in slots]
        stays = [[sel(is_here(plan[0]), 1, 0) for plan in row] for row in strip_to]
        corner_to = [[corner_plan(p, sa, sb) for sa, sb in corners] for p in slots]
        flips = [[sel(at_edge(side), neighbour(p, side)[3], 0) for side in SIDES] for p in slots]
        turns = [[sel(at_edge(side), neighbour(p, side)[4], 0) for side in SIDES] for p in slots]

        def at_slot(p, table):
            first = table[0]
            if isinstance(first, dict):
                return {key: at_slot(p, [row[key] for row in table]) for key in first}
            if isinstance(first, (tuple, list)):
                return [at_slot(p, [row[n] for row in table]) for n in range(len(first))]
            return sel(p == 0, first, sel(p == 1, table[1], table[2]))
        mesh_ids = pl.DeviceIdType.MESH

        barrier = pltpu.get_barrier_semaphore()

        for p in slots:
            for side in SIDES:
                pl.semaphore_signal(barrier, inc=1, device_id=strip_to[p][side][0], device_id_type=mesh_ids)
            for (sa, sb), plan in zip(corners, corner_to[p]):
                @pl.when(has_corner(sa, sb))
                def _():
                    pl.semaphore_signal(barrier, inc=1, device_id=plan[0], device_id_type=mesh_ids)

        def load_field(in_ref, dst, base):
            @pl.loop(0, NPAN)
            def _(p):
                for it in PLANES:
                    for jt in PLANES:
                        TT[it, pl.ds(H + LN * jt, LN), :] = in_ref[p, pl.ds(LN * it, LN), pl.ds(LN * jt, LN)].T
                    for c in PLANES:
                        NN[c, pl.ds(H + LN * it, LN), :] = TT[it, pl.ds(c, LN, stride=NC), :].T

                @pl.loop(0, KR // SB)
                def _(kb):
                    for c in PLANES:
                        for k in range(SB):
                            dst[base + p, c, pl.ds(pl.multiple_of(64 * kb + SB * (k + 2), SB), SB), :] = NN[c, pl.ds(SB * kb + k, SB, stride=KR), :]

        def store_field(src):
            @pl.loop(0, NPAN)
            def _(p):
                @pl.loop(0, KR // SB)
                def _(kb):
                    for c in PLANES:
                        for k in range(SB):
                            NN[c, pl.ds(SB * kb + k, SB, stride=KR), :] = src[p, c, pl.ds(pl.multiple_of(64 * kb + SB * (k + 2), SB), SB), :]
                for it in PLANES:
                    for c in PLANES:
                        TT[it, pl.ds(c, LN, stride=NC), :] = NN[c, pl.ds(H + LN * it, LN), :].T
                    for jt in PLANES:
                        out_ref[p, pl.ds(LN * it, LN), pl.ds(LN * jt, LN)] = TT[it, pl.ds(H + LN * jt, LN), :].T

        def quarter(n):
            return pl.ds(GL * n, GL)

        def rows_at(first, s, n):
            return pl.ds(SB * (first + 2 + n) + s, GL, stride=NC * SB)

        def pack_strips(row_ref, row_at, col_ref, col_at, f, p):
            for c in PLANES:
                for n in PLANES:
                    SEND[f, p, 0, c, quarter(n), :] = row_ref[row_at, c, rows_at(H, 0, n), :]
                    SEND[f, p, 1, c, quarter(n), :] = row_ref[row_at, c, rows_at(KR - 2 * H, SB - 1, n), :]
            lane = lanes_of((LN, LN))

            def window(first):
                return jnp.logical_and(lane >= first, lane < first + GL)
            planes = [col_ref[col_at, c, pl.ds(2 * SB, SB * KR), :].reshape(2 * SB, NC * SB, LN) for c in PLANES]
            for cp in PLANES:
                mix = None
                for c in PLANES:
                    blk = planes[c][:, SB * cp:SB * (cp + 1)].reshape(LN, LN)
                    if c == 0:
                        mix = blk
                    else:
                        mine = jnp.logical_or(window(GL + SB * c), window(SB * (c - 1)))
                        mix = sel(mine, pltpu.roll(blk, SB * c, 1), mix)
                t = mix.T
                for c in PLANES:
                    low, high = GL + SB * c, (LN - SB + SB * c) % LN
                    SEND[f, p, 2, cp, quarter(c), :] = t[low:low + GL]
                    SEND[f, p, 3, cp, quarter(c), :] = t[high:high + GL]

        def beta_order(lane):
            return 2 * SB * lax.rem(lane, SB) + lax.div(lane, SB)

        def beta_lane(n):
            return SB * lax.rem(n, 2 * SB) + lax.div(n, 2 * SB)

        def turn_strips(f, p, winds):
            flip_at, turn_at, to = at_slot(p, flips), at_slot(p, turns), at_slot(p, strip_to)
            for side in SIDES:
                to_beta = to[side][2] >= 2
                moved = jnp.logical_not(to_beta) if side >= 2 else to_beta

                @pl.when(jnp.logical_or(flip_at[side] == 1, moved))
                def _():
                    back = flip_at[side] == 1
                    at = lanes_of((NC * H, LN))
                    at = beta_order(at) if side >= 2 else at
                    inside = jnp.logical_and(at >= GL, at < LN - GL)
                    now = [SEND[f, p, side, c] for c in PLANES]
                    old = jnp.concatenate([sel(back, now[NC - 1 - c], now[c]) for c in PLANES], axis=0)
                    come = lanes_of((LN, LN))
                    come = sel(to_beta, beta_order(come), come)
                    come = sel(back, LN - 1 - come, come)
                    come = beta_lane(come) if side >= 2 else come
                    place = (rows_of((LN, LN)) == come).astype(F32)
                    new = jnp.dot(sel(inside, old, jnp.zeros_like(old)), place, precision=lax.Precision.HIGHEST,
                                  preferred_element_type=F32)
                    for c in PLANES:
                        SEND[f, p, side, c] = new[H * c:H * (c + 1)]
                    if winds:
                        @pl.when(jnp.logical_and(f == 2, back))
                        def _():
                            for c in PLANES:
                                SEND[f, p, side, c] = -SEND[f, p, side, c]

                @pl.when(turn_at[side] == 1)
                def _():
                    for c in PLANES:
                        v = SEND[f, p, side, c]
                        if winds:
                            v = sel(f == 1, -v, v)
                        for m in range(H):
                            SEND[f, p, side, c, m:m + 1, :] = v[H - 1 - m:H - m, :]

        def pack_corners(f, p, plan):
            lane = lanes_of((H, LN))
            for cid, (_, _, _, side, x, to_beta) in enumerate(plan):
                beta, high = to_beta == 1, x == 1
                key = sel(beta, lax.rem(lane, SB), lane)
                key = sel(high, key, sel(beta, SB - 1, LN - 1) - key)
                step = sel(beta, 1, GL)
                first = sel(beta, LN - BETA_SHIFT, SB)
                msg = None
                for c in PLANES:
                    shift = sel(high, first + step * c, LN - first - step * c)
                    v = pltpu.roll(SEND[f, p, side, c], shift, 1)
                    msg = v if c == 0 else sel(key >= step * c, v, msg)
                CSEND[f, p, cid] = msg

        def send_panel(row_ref, row_at, col_ref, col_at, f, fr, p, winds):
            pack_strips(row_ref, row_at, col_ref, col_at, f, p)
            turn_strips(f, p, winds)
            plan = at_slot(p, corner_to)
            pack_corners(f, p, plan)
            to, here_at = at_slot(p, strip_to), at_slot(p, stays)
            for side in SIDES:
                device, slot, dside = to[side]

                @pl.when(here_at[side] == 1)
                def _():
                    RECV[fr, slot, dside] = SEND[f, p, side]

                @pl.when(here_at[side] == 0)
                def _():
                    pltpu.make_async_remote_copy(
                        src_ref=SEND.at[f, p, side], dst_ref=RECV.at[fr, slot, dside], send_sem=send_sem.at[f, p, side],
                        recv_sem=recv_sem.at[fr, slot, dside], device_id=device, device_id_type=mesh_ids).start()
            for cid, (sa, sb) in enumerate(corners):
                @pl.when(has_corner(sa, sb))
                def _():
                    device, slot, dcorner = plan[cid][:3]
                    pltpu.make_async_remote_copy(
                        src_ref=CSEND.at[f, p, cid], dst_ref=CRECV.at[fr, slot, dcorner], send_sem=csend_sem.at[f, p, cid],
                        recv_sem=crecv_sem.at[fr, slot, dcorner], device_id=device, device_id_type=mesh_ids).start()

        def wait_copies(strips, blocks, sem, csem, f, p):
            for side in SIDES:
                @pl.when(stays[p][side] == 0)
                def _():
                    pltpu.make_async_copy(strips.at[f, p, side], strips.at[f, p, side], sem.at[f, p, side]).wait()
            for cid, (sa, sb) in enumerate(corners):
                @pl.when(has_corner(sa, sb))
                def _():
                    pltpu.make_async_copy(blocks.at[f, p, cid], blocks.at[f, p, cid], csem.at[f, p, cid]).wait()

        def end_valid(side, e):
            if side < 2:
                return jnp.logical_not(at_edge(2 + e))
            return jnp.logical_and(jnp.logical_not(at_edge(e)), at_edge(side))

        def merged(fr, p, side, c):
            lane = lanes_of((H, LN))
            v = RECV[fr, p, side, c]
            for e in range(2):
                cid = 2 * side + e if side < 2 else 2 * e + side - 2
                msg = CRECV[fr, p, cid]
                step = c if side >= 2 else GL * c
                if c:
                    msg = pltpu.roll(msg, step if e else LN - step, 1)
                at = beta_order(lane) if side >= 2 else lane
                inside = at >= LN - GL if e else at < GL
                v = sel(jnp.logical_and(inside, end_valid(side, e)), msg, v)
            return v

        def unpack_cols(ref, dst, fr, p):
            parts = []
            for cp in PLANES:
                low, high = merged(fr, p, 2, cp), merged(fr, p, 3, cp)
                z = ZS.at[NC * p + cp]
                for c in PLANES:
                    z[pl.ds(SB * c, GL), :] = low[GL * c:GL * (c + 1)]
                    z[pl.ds((SB * c - GL) % LN, GL), :] = high[GL * c:GL * (c + 1)]
                t = z[...].T
                parts.append([(pltpu.roll(t, LN - SB * c, 1) if c else t).reshape(2 * SB, SB, LN) for c in PLANES])
            lane = lanes_of((SB * KR, LN))
            ghost = jnp.logical_or(lane < GL, lane >= LN - GL)
            rows = pl.ds(2 * SB, SB * KR)
            for c in PLANES:
                new = jnp.concatenate([part[c] for part in parts], axis=1).reshape(SB * KR, LN)
                ref[dst, c, rows, :] = sel(ghost, new, ref[dst, c, rows, :])

        def unpack_rows(ref, dst, fr, p):
            lane = lanes_of((GL, LN))
            keep = jnp.logical_and(jnp.logical_or(lane >= GL, end_valid(0, 0)),
                                   jnp.logical_or(lane < LN - GL, end_valid(0, 1)))
            for c in PLANES:
                for side, first, s in ((0, 0, 0), (1, KR - H, SB - 1)):
                    v = merged(fr, p, side, c)
                    for n in PLANES:
                        rows = rows_at(first, s, n)
                        ref[dst, c, rows, :] = sel(keep, v[GL * n:GL * (n + 1)], ref[dst, c, rows, :])

        def pad_rows(ref):
            at = pl.ds(0, NPAN)
            ref[at, :, pl.ds(0, 2 * SB), :] = ref[at, :, pl.ds(SB * KR - 1, 2 * SB), :]
            ref[at, :, pl.ds(SB * (KR + 2), 2 * SB), :] = ref[at, :, pl.ds(2 * SB + 1, 2 * SB), :]

        def corner_case(fn):
            for sa, sb in corners:
                @pl.when(jnp.logical_and(at_edge(sa), at_edge(2 + sb)))
                def _():
                    fn(sa, sb)

        def quad_geom(sa, sb):
            k0, s = (0, 0) if sa == 0 else (KR - H, SB - 1)
            lane0 = 0 if sb == 0 else LN - GL
            lane, idx = lanes_of((H, LN)), rows_of((H, LN))
            col = idx if sa == sb else H - 1 - idx
            masks = [NC * (lane - lane0) + c == col for c in PLANES]
            return k0, s, lane, masks, pl.ds(SB * (k0 + 2) + s, H, stride=SB)

        def beta_column(ref, first, sa, sb, r):
            k0, s, lane, masks, rows = quad_geom(sa, sb)
            kr = H + r if sa == 0 else KR - H - 1 - r
            tot = jnp.zeros((NPAN, H, LN), F32)
            for c in PLANES:
                line = ref[pl.ds(first, NPAN), c, pl.ds(SB * (kr + 2) + s, 1), :]
                tot = sel(wide(masks[c]), jnp.broadcast_to(line, tot.shape), tot)
            l_to, c_to = (GL - 1, NC - 1 - r) if sb == 0 else (LN - GL, r)
            return jnp.broadcast_to(jnp.sum(tot, axis=2, keepdims=True), tot.shape), wide(lane == l_to), c_to, rows

        def alpha_lines(ref, first, sa, sb, r):
            _, _, lane, masks, rows = quad_geom(sa, sb)
            l_from, c_from = (GL, r) if sb == 0 else (LN - GL - 1, NC - 1 - r)
            zero = jnp.zeros((NPAN, H, LN), F32)
            col = jnp.sum(sel(wide(lane == l_from), ref[pl.ds(first, NPAN), c_from, rows, :], zero), axis=2, keepdims=True)
            col = jnp.broadcast_to(col, zero.shape)
            return [jnp.sum(sel(wide(mask), col, zero), axis=1, keepdims=True) for mask in masks]

        def wide(mask):
            return jnp.broadcast_to(mask[None], (NPAN, *mask.shape))

        def fill_quadrant(src, sa, sb):
            columns = [beta_column(src, 0, sa, sb, r) for r in range(2)]
            lines = [alpha_lines(src, 0, sa, sb, r) for r in range(2)]
            for r in range(2):
                col, mask, c_to, rows = columns[r]
                src[:, c_to, rows, :] = sel(mask, col, src[:, c_to, rows, :])
                for c in PLANES:
                    CQ[:, r, c] = jnp.broadcast_to(lines[r][c], (NPAN, SB, LN))

        def fill_winds(sa, sb):
            sign = -1.0 if sa == sb else 1.0
            col, mask, c_to, rows = beta_column(WW, WA, sa, sb, 0)
            line = alpha_lines(WW, WB, sa, sb, 0)
            to_b, to_a = pl.ds(WB, NPAN), pl.ds(WA, NPAN)
            WW[to_b, c_to, rows, :] = sel(mask, sign * col, WW[to_b, c_to, rows, :])
            row_lane = lanes_of((NPAN, 1, LN))
            inside = row_lane < GL if sb == 0 else row_lane >= LN - GL
            row = pl.ds(SB * (H + 1), 1) if sa == 0 else pl.ds(SB * (KR - H + 3) - 1, 1)
            for c in PLANES:
                WW[to_a, c, row, :] = sel(inside, sign * line[c], WW[to_a, c, row, :])

        def roll_down(v):
            return pltpu.roll(v, LN - 1, 1)

        def roll_up(v):
            return pltpu.roll(v, 1, 1)

        def beta_rows(src, p, k0, scale):
            rows = pl.ds(SB * (k0 + 2), SB * BETA_ROWS)
            a0, a1, a2 = (src[p, c, rows, :] for c in PLANES)
            a2l, a0r, a1r = roll_up(a2), roll_down(a0), roll_down(a1)
            e0, e1, e2 = a2l + a1, a0 + a2, a1 + a0r
            g0, g1, g2 = 8.0 * a0 - e0, 8.0 * a1 - e1, 8.0 * a2 - e2
            g0r = 8.0 * a0r - (a2 + a1r)
            x0 = WW[WB + p, 0, rows, :] * (g0 + g1)
            x1 = WW[WB + p, 1, rows, :] * (g1 + g2)
            x2 = WW[WB + p, 2, rows, :] * (g2 + g0r)
            x2l = roll_up(x2)
            return jnp.stack([x0 - x2l, x1 - x0, x2 - x1]), jnp.stack([e0, e1, e2])

        def row_group(ref, p, k):
            return ref[p, :, pl.ds(SB * (k + 2), SB), :]

        def panel_pass(src, dst, p, scale, second):
            lane, sub = lanes_of((NC, SB, LN)), rows_of((NC, SB, LN))
            ghost_lane = jnp.logical_or(jnp.logical_and(at_edge(2), lane < GL),
                                        jnp.logical_and(at_edge(3), lane >= LN - GL))
            in_low = jnp.logical_and(ghost_lane, jnp.logical_and(at_edge(0), sub == 0))
            in_high = jnp.logical_and(ghost_lane, jnp.logical_and(at_edge(1), sub == SB - 1))

            def load(k):
                v = row_group(src, p, k)
                if k in (H - 2, H - 1):
                    return sel(in_low, CQ[p, H - 1 - k], v)
                if k in (KR - H, KR - H + 1):
                    return sel(in_high, CQ[p, k - (KR - H)], v)
                return v

            qm, q0, q1 = load(-2), load(-1), load(0)
            q2 = load(1)
            g0 = 8.0 * q0 - (qm + q1)
            e1 = q0 + q2
            g1 = 8.0 * q1 - e1
            x_low = row_group(WW, WA + p, -1) * (g0 + g1)
            q_now, e_now, g_now, q_next = q1, e1, g1, q2
            beta = None
            for k in range(KR):
                if k % BETA_ROWS == 0:
                    beta = beta_rows(src, p, k, scale)
                at = SB * (k % BETA_ROWS)
                tb, eb = (v[:, at:at + SB] for v in beta)
                q_far = load(k + 2)
                e_next = q_now + q_far
                g_next = 8.0 * q_next - e_next
                x_high = row_group(WW, WA + p, k) * (g_now + g_next)
                u = scale * (x_high - x_low + tb) - (e_now + eb)
                new = KK[1, :, pl.ds(SB * k, SB), :] * q_now - KK[0, :, pl.ds(SB * k, SB), :] * u
                if second:
                    new = 0.5 * (row_group(dst, p, k) + new)
                dst[p, :, pl.ds(SB * (k + 2), SB), :] = new
                x_low, q_now, e_now, g_now, q_next = x_high, q_next, e_next, g_next, q_far

        def stage(src, dst, scale, second, more, after=None):
            pad_rows(src)

            @pl.when(more)
            def _():
                corner_case(lambda sa, sb: fill_quadrant(src, sa, sb))

            @pl.loop(0, NPAN)
            def _(p):
                panel_pass(src, dst, p, scale, second)
                if after is not None:
                    after(p)

        load_field(a_in, WW, WA)
        load_field(b_in, WW, WB)
        is_cc = jnp.logical_and(jnp.logical_or(at_edge(0), at_edge(1)), jnp.logical_or(at_edge(2), at_edge(3)))
        pl.semaphore_wait(barrier, SB * NPAN - NPAN * sel(is_cc, 1, 0))

        @pl.loop(1, 3)
        def _(f):
            @pl.loop(0, NPAN)
            def _(p):
                send_panel(WW, (f - 1) * NPAN + p, WW, (2 - f) * NPAN + p, f, f + 1, p, True)
        load_field(q_in, QA, 0)

        def finish_winds():
            metric()

            @pl.loop(1, 3)
            def _(f):
                for p in slots:
                    wait_copies(RECV, CRECV, recv_sem, crecv_sem, f + 1, p)

                @pl.loop(0, NPAN)
                def _(p):
                    unpack_cols(WW, (2 - f) * NPAN + p, f + 1, p)

            @pl.loop(1, 3)
            def _(f):
                @pl.loop(0, NPAN)
                def _(p):
                    unpack_rows(WW, (f - 1) * NPAN + p, f + 1, p)
                for p in slots:
                    wait_copies(SEND, CSEND, send_sem, csend_sem, f, p)
            corner_case(fill_winds)
            pad_rows(WW)
            face_scale = 0.5 / (12.0 * 0.5 * C_SPEED)

            @pl.loop(0, NPAN)
            def _(p):
                for c in PLANES:
                    low, high = pl.ds(SB, SB * (KR + 1)), pl.ds(2 * SB, SB * (KR + 1))
                    WW[WA + p, c, low, :] = face_scale * (WW[WA + p, c, low, :] + WW[WA + p, c, high, :])
                rows = pl.ds(2 * SB, SB * KR)
                b0, b1, b2 = (WW[WB + p, c, rows, :] for c in PLANES)
                WW[WB + p, 0, rows, :] = face_scale * (b0 + b1)
                WW[WB + p, 1, rows, :] = face_scale * (b1 + b2)
                WW[WB + p, 2, rows, :] = face_scale * (b2 + roll_down(b0))

        def metric():
            ridx = rows_of((SB * KR, LN))
            gi = tx * tile_rows + lax.rem(ridx, SB) * KR + lax.div(ridx, SB) - H
            gi = sel(gi < 0, -1 - gi, sel(gi >= cells, 2 * cells - 1 - gi, gi))
            tan_a = small_tan((gi.astype(F32) + 0.5) * dalpha - 0.25 * math.pi)
            for c in PLANES:
                gj = ty * tile_rows + 3 * lanes_of((SB, LN)) + c - H
                gj = sel(gj < 0, -1 - gj, sel(gj >= cells, 2 * cells - 1 - gj, gj))
                tan_b = small_tan((gj.astype(F32) + 0.5) * dalpha - 0.25 * math.pi)[0:1, :]
                a_sq, b_sq = tan_a * tan_a, tan_b * tan_b
                r_sq = 1.0 + a_sq + b_sq
                sqrt_g = (1.0 + a_sq) * (1.0 + b_sq) / (r_sq * jnp.sqrt(r_sq))
                KK[0, c] = (0.5 * C_SPEED * CFL_STEP) / sqrt_g
                KK[1, c] = 1.0 - 4.0 * KK[0, c]

        @pl.loop(0, n_blocks)
        def _(b):
            fr = lax.rem(b, 2)

            @pl.when(b == 0)
            def _():
                @pl.loop(0, NPAN)
                def _(p):
                    send_panel(QA, p, QA, p, 0, 0, p, False)

            @pl.when(b == 0)
            def _():
                finish_winds()

            for p in slots:
                wait_copies(RECV, CRECV, recv_sem, crecv_sem, fr, p)
                unpack_cols(QA, p, fr, p)
                unpack_rows(QA, p, fr, p)
            for p in slots:
                wait_copies(SEND, CSEND, send_sem, csend_sem, 0, p)
            end = lax.div((b + 1) * steps, n_blocks)

            @pl.loop(lax.div(b * steps, n_blocks), end)
            def _(t):
                scale = ws_ref[t]
                stage(QA, QB, scale, False, True)

                def after(p):
                    @pl.when(jnp.logical_and(t + 1 == end, b + 1 < n_blocks))
                    def _():
                        send_panel(QA, p, QA, p, 0, 1 - fr, p, False)
                stage(QB, QA, scale, True, t + 1 < end, after)

        store_field(QA)

    return kernel


def solution(mesh):
    tile_count = mesh.shape['tx']
    field_spec = P(('member', 'panel'), 'tx', 'ty')
    wind_spec = P('panel', 'tx', 'ty')

    def local_run(tracer, wind_a, wind_b, wind_scale):
        steps = wind_scale.shape[0]
        n_blocks = -(-steps // STEPS_PER_BLOCK)
        ext = SB * KR
        block = pl.BlockSpec((NPAN, ext, ext), lambda n: (0, 0, 0))
        dma = pltpu.SemaphoreType.DMA
        return pl.pallas_call(
            make_kernel(tile_count, steps, n_blocks, tracer.shape[1]),
            grid=(1,),
            out_shape=jax.ShapeDtypeStruct(tracer.shape, F32),
            in_specs=[pl.BlockSpec(memory_space=pltpu.SMEM), block, block, block],
            out_specs=block,
            scratch_shapes=[
                pltpu.VMEM((NPAN, NC, ext + 32, LN), F32),
                pltpu.VMEM((NPAN, NC, ext + 32, LN), F32),
                pltpu.VMEM((2 * NPAN, NC, ext + 32, LN), F32),
                pltpu.VMEM((NPAN, 2, NC, SB, LN), F32),
                pltpu.VMEM((2, NC, ext, LN), F32),
                pltpu.VMEM((NC, ext + 32, LN), F32),
                pltpu.VMEM((NC, ext + 32, LN), F32),
                pltpu.VMEM((9, LN, LN), F32),
                pltpu.VMEM((3, NPAN, 4, NC, H, LN), F32),
                pltpu.VMEM((4, NPAN, 4, NC, H, LN), F32),
                pltpu.VMEM((3, NPAN, 4, H, LN), F32),
                pltpu.VMEM((4, NPAN, 4, H, LN), F32),
                *[dma((n, NPAN, 4)) for n in (3, 4, 3, 4)],
            ],
            compiler_params=pltpu.CompilerParams(collective_id=0, has_side_effects=True, vmem_limit_bytes=60 * 1024 * 1024),
            cost_estimate=pl.CostEstimate(flops=10 ** 9, bytes_accessed=10 ** 7, transcendentals=0),
        )(wind_scale, tracer, wind_a, wind_b)

    return jax.shard_map(local_run, mesh=mesh, in_specs=(field_spec, wind_spec, wind_spec, P()),
                         out_specs=field_spec, check_vma=False)
```

```python
import math
import jax
import numpy as np
import jax.numpy as jnp
from jax import lax
from jax.experimental import pallas as pl
from jax.experimental.pallas import tpu as pltpu
from jax.sharding import PartitionSpec as P

C_SPEED = 2.5
CFL_STEP = 0.12
EDGE_CODE = (
    (310, 100, 530, 420), (10, 200, 511, 410), (110, 300, 521, 431),
    (210, 0, 500, 401), (331, 130, 30, 231), (320, 121, 221, 20),
)
H = 12
KR = 48
NPAN = 3
NC = 3
SB = 8
LN = 128
GL = 4
BETA_SHIFT = 71
STEPS_PER_BLOCK = 3
BETA_ROWS = 4
F32 = jnp.float32
PLANES = range(NC)
SIDES = range(4)


def turned_sign(side_id, edge_id):
    return int(side_id % 2 == edge_id % 2)


def small_tan(v):
    sq = v * v
    sin_sum, cos_sum = jnp.full_like(v, 1.0), jnp.full_like(v, 1.0)
    for n in (6, 5, 4, 3, 2, 1):
        sin_sum = 1.0 - sq * sin_sum * (1.0 / (2 * n * (2 * n + 1)))
        cos_sum = 1.0 - sq * cos_sum * (1.0 / (2 * n * (2 * n - 1)))
    return v * sin_sum / cos_sum


def sel(pred, yes, no):
    yes, no = (np.int32(v) if isinstance(v, int) else v for v in (yes, no))
    same = jnp.shape(yes) == jnp.shape(no) and jnp.shape(pred) in ((), jnp.shape(yes))
    return lax.select(pred, yes, no) if same else jnp.where(pred, yes, no)


def lanes_of(shape):
    return lax.broadcasted_iota(jnp.int32, shape, len(shape) - 1)


def rows_of(shape):
    return lax.broadcasted_iota(jnp.int32, shape, len(shape) - 2)


def make_kernel(tile_count, steps, n_blocks, tile_rows):
    last = tile_count - 1
    cells = tile_rows * tile_count
    dalpha = 0.5 * math.pi / cells

    def kernel(ws_ref, q_in, a_in, b_in, out_ref, QA, QB, WW, CQ, KK, NN, TT, ZS, SEND, RECV, CSEND, CRECV,
               send_sem, recv_sem, csend_sem, crecv_sem):
        dev = lax.axis_index('panel')
        tx = lax.axis_index('tx')
        ty = lax.axis_index('ty')
        WA, WB = 0, NPAN

        def at_edge(side):
            return (tx == 0, tx == last, ty == 0, ty == last)[side]

        def pick(v0, v1):
            return v0 if v0 == v1 else v0 + dev * (v1 - v0)

        def neighbour(p, side):
            codes = [EDGE_CODE[NPAN * dv + p][side] for dv in (0, 1)]
            panels = [code // 100 for code in codes]
            edges = [code // 10 % 10 for code in codes]
            return (pick(*[n // NPAN for n in panels]), pick(*[n % NPAN for n in panels]), pick(*edges),
                    pick(*[code % 10 for code in codes]), pick(*[turned_sign(side, e) for e in edges]))

        def dest(p, side, off):
            along = (ty if side < 2 else tx) + off
            edge = at_edge(side)
            d_dev, d_slot, dside, flip, _ = neighbour(p, side)
            al = along + flip * (last - 2 * along)
            c_tx = sel(dside == 0, 0, sel(dside == 1, last, al))
            c_ty = sel(dside == 2, 0, sel(dside == 3, last, al))
            step = 2 * (side % 2) - 1
            in_tx, in_ty = (tx + step, ty + off) if side < 2 else (tx + off, ty + step)
            device = {'tx': sel(edge, c_tx, in_tx), 'ty': sel(edge, c_ty, in_ty),
                      'panel': sel(edge, d_dev, dev)}
            return device, sel(edge, d_slot, p), sel(edge, dside, side ^ 1), sel(edge, flip, 0)

        def corner_plan(p, sa, sb):
            out_b = at_edge(2 + sb)
            plans = []
            for side, end, off in ((sa, sb, 2 * sb - 1), (2 + sb, sa, 2 * sa - 1)):
                device, slot, dside, flip = dest(p, side, off)
                x = end + flip * (1 - 2 * end)
                e = 1 - x
                plans.append((device, slot, sel(dside < 2, 2 * dside + e, 2 * e + (dside - 2)), side, x,
                              sel(dside < 2, 0, 1)))
            device = {key: sel(out_b, plans[1][0][key], plans[0][0][key]) for key in plans[0][0]}
            return (device, *[sel(out_b, second, first) for first, second in zip(plans[0][1:], plans[1][1:])])

        def has_corner(sa, sb):
            return jnp.logical_not(jnp.logical_and(at_edge(sa), at_edge(2 + sb)))

        def is_here(device):
            return jnp.logical_and(jnp.logical_and(device['tx'] == tx, device['ty'] == ty), device['panel'] == dev)

        corners = [(sa, sb) for sa in range(2) for sb in range(2)]
        slots = range(NPAN)
        strip_to = [[dest(p, side, 0)[:3] for side in SIDES] for p in slots]
        stays = [[sel(is_here(plan[0]), 1, 0) for plan in row] for row in strip_to]
        corner_to = [[corner_plan(p, sa, sb) for sa, sb in corners] for p in slots]
        flips = [[sel(at_edge(side), neighbour(p, side)[3], 0) for side in SIDES] for p in slots]
        turns = [[sel(at_edge(side), neighbour(p, side)[4], 0) for side in SIDES] for p in slots]

        def at_slot(p, table):
            first = table[0]
            if isinstance(first, dict):
                return {key: at_slot(p, [row[key] for row in table]) for key in first}
            if isinstance(first, (tuple, list)):
                return [at_slot(p, [row[n] for row in table]) for n in range(len(first))]
            return sel(p == 0, first, sel(p == 1, table[1], table[2]))
        mesh_ids = pl.DeviceIdType.MESH

        barrier = pltpu.get_barrier_semaphore()

        for p in slots:
            for side in SIDES:
                pl.semaphore_signal(barrier, inc=1, device_id=strip_to[p][side][0], device_id_type=mesh_ids)
            for (sa, sb), plan in zip(corners, corner_to[p]):
                @pl.when(has_corner(sa, sb))
                def _():
                    pl.semaphore_signal(barrier, inc=1, device_id=plan[0], device_id_type=mesh_ids)

        def load_fields(jobs):
            @pl.loop(0, NPAN)
            def _(p):
                for f, (in_ref, _, _) in enumerate(jobs):
                    for it in PLANES:
                        for jt in PLANES:
                            TT[NC * f + it, pl.ds(H + LN * jt, LN), :] = in_ref[p, pl.ds(LN * it, LN), pl.ds(LN * jt, LN)].T
                        for c in PLANES:
                            NN[NC * f + c, pl.ds(H + LN * it, LN), :] = TT[NC * f + it, pl.ds(c, LN, stride=NC), :].T
                for f, (_, dst, base) in enumerate(jobs):
                    for c in PLANES:
                        for k in range(KR):
                            dst[base + p, c, pl.ds(SB * (k + 2), SB), :] = NN[NC * f + c, pl.ds(k, SB, stride=KR), :]

        def store_field(src):
            @pl.loop(0, NPAN)
            def _(p):
                @pl.loop(0, KR // SB)
                def _(kb):
                    for c in PLANES:
                        for k in range(SB):
                            NN[c, pl.ds(SB * kb + k, SB, stride=KR), :] = src[p, c, pl.ds(pl.multiple_of(64 * kb + SB * (k + 2), SB), SB), :]
                for it in PLANES:
                    for c in PLANES:
                        TT[it, pl.ds(c, LN, stride=NC), :] = NN[c, pl.ds(H + LN * it, LN), :].T
                    for jt in PLANES:
                        out_ref[p, pl.ds(LN * it, LN), pl.ds(LN * jt, LN)] = TT[it, pl.ds(H + LN * jt, LN), :].T

        def quarter(n):
            return pl.ds(GL * n, GL)

        def rows_at(first, s, n):
            return pl.ds(SB * (first + 2 + n) + s, GL, stride=NC * SB)

        def pack_strips(row_ref, row_at, col_ref, col_at, f, p):
            for c in PLANES:
                for n in PLANES:
                    SEND[f, p, 0, c, quarter(n), :] = row_ref[row_at, c, rows_at(H, 0, n), :]
                    SEND[f, p, 1, c, quarter(n), :] = row_ref[row_at, c, rows_at(KR - 2 * H, SB - 1, n), :]
            lane = lanes_of((LN, LN))

            def window(first):
                return jnp.logical_and(lane >= first, lane < first + GL)
            planes = [col_ref[col_at, c, pl.ds(2 * SB, SB * KR), :].reshape(2 * SB, NC * SB, LN) for c in PLANES]
            for cp in PLANES:
                mix = None
                for c in PLANES:
                    blk = planes[c][:, SB * cp:SB * (cp + 1)].reshape(LN, LN)
                    if c == 0:
                        mix = blk
                    else:
                        mine = jnp.logical_or(window(GL + SB * c), window(SB * (c - 1)))
                        mix = sel(mine, pltpu.roll(blk, SB * c, 1), mix)
                t = mix.T
                for c in PLANES:
                    low, high = GL + SB * c, (LN - SB + SB * c) % LN
                    SEND[f, p, 2, cp, quarter(c), :] = t[low:low + GL]
                    SEND[f, p, 3, cp, quarter(c), :] = t[high:high + GL]

        def beta_order(lane):
            return 2 * SB * lax.rem(lane, SB) + lax.div(lane, SB)

        def beta_lane(n):
            return SB * lax.rem(n, 2 * SB) + lax.div(n, 2 * SB)

        def turn_strips(f, p, winds):
            flip_at, turn_at, to = at_slot(p, flips), at_slot(p, turns), at_slot(p, strip_to)
            for side in SIDES:
                to_beta = to[side][2] >= 2
                moved = jnp.logical_not(to_beta) if side >= 2 else to_beta

                @pl.when(jnp.logical_or(flip_at[side] == 1, moved))
                def _():
                    back = flip_at[side] == 1
                    at = lanes_of((NC * H, LN))
                    at = beta_order(at) if side >= 2 else at
                    inside = jnp.logical_and(at >= GL, at < LN - GL)
                    now = [SEND[f, p, side, c] for c in PLANES]
                    old = jnp.concatenate([sel(back, now[NC - 1 - c], now[c]) for c in PLANES], axis=0)
                    come = lanes_of((LN, LN))
                    come = sel(to_beta, beta_order(come), come)
                    come = sel(back, LN - 1 - come, come)
                    come = beta_lane(come) if side >= 2 else come
                    place = (rows_of((LN, LN)) == come).astype(F32)
                    new = jnp.dot(sel(inside, old, jnp.zeros_like(old)), place, precision=lax.Precision.HIGHEST,
                                  preferred_element_type=F32)
                    for c in PLANES:
                        SEND[f, p, side, c] = new[H * c:H * (c + 1)]
                    if winds:
                        @pl.when(jnp.logical_and(f == 2, back))
                        def _():
                            for c in PLANES:
                                SEND[f, p, side, c] = -SEND[f, p, side, c]

                @pl.when(turn_at[side] == 1)
                def _():
                    for c in PLANES:
                        v = SEND[f, p, side, c]
                        if winds:
                            v = sel(f == 1, -v, v)
                        for m in range(H):
                            SEND[f, p, side, c, m:m + 1, :] = v[H - 1 - m:H - m, :]

        def pack_corners(f, p, plan):
            lane = lanes_of((H, LN))
            for cid, (_, _, _, side, x, to_beta) in enumerate(plan):
                beta, high = to_beta == 1, x == 1
                key = sel(beta, lax.rem(lane, SB), lane)
                key = sel(high, key, sel(beta, SB - 1, LN - 1) - key)
                step = sel(beta, 1, GL)
                first = sel(beta, LN - BETA_SHIFT, SB)
                msg = None
                for c in PLANES:
                    shift = sel(high, first + step * c, LN - first - step * c)
                    v = pltpu.roll(SEND[f, p, side, c], shift, 1)
                    msg = v if c == 0 else sel(key >= step * c, v, msg)
                CSEND[f, p, cid] = msg

        def send_panel(row_ref, row_at, col_ref, col_at, f, fr, p, winds):
            pack_strips(row_ref, row_at, col_ref, col_at, f, p)
            turn_strips(f, p, winds)
            plan = at_slot(p, corner_to)
            pack_corners(f, p, plan)
            to, here_at = at_slot(p, strip_to), at_slot(p, stays)
            for side in SIDES:
                device, slot, dside = to[side]

                @pl.when(here_at[side] == 1)
                def _():
                    RECV[fr, slot, dside] = SEND[f, p, side]

                @pl.when(here_at[side] == 0)
                def _():
                    pltpu.make_async_remote_copy(
                        src_ref=SEND.at[f, p, side], dst_ref=RECV.at[fr, slot, dside], send_sem=send_sem.at[f, p, side],
                        recv_sem=recv_sem.at[fr, slot, dside], device_id=device, device_id_type=mesh_ids).start()
            for cid, (sa, sb) in enumerate(corners):
                @pl.when(has_corner(sa, sb))
                def _():
                    device, slot, dcorner = plan[cid][:3]
                    pltpu.make_async_remote_copy(
                        src_ref=CSEND.at[f, p, cid], dst_ref=CRECV.at[fr, slot, dcorner], send_sem=csend_sem.at[f, p, cid],
                        recv_sem=crecv_sem.at[fr, slot, dcorner], device_id=device, device_id_type=mesh_ids).start()

        def wait_copies(strips, blocks, sem, csem, f, p):
            for side in SIDES:
                @pl.when(stays[p][side] == 0)
                def _():
                    pltpu.make_async_copy(strips.at[f, p, side], strips.at[f, p, side], sem.at[f, p, side]).wait()
            for cid, (sa, sb) in enumerate(corners):
                @pl.when(has_corner(sa, sb))
                def _():
                    pltpu.make_async_copy(blocks.at[f, p, cid], blocks.at[f, p, cid], csem.at[f, p, cid]).wait()

        def end_valid(side, e):
            if side < 2:
                return jnp.logical_not(at_edge(2 + e))
            return jnp.logical_and(jnp.logical_not(at_edge(e)), at_edge(side))

        def merged(fr, p, side, c):
            lane = lanes_of((H, LN))
            v = RECV[fr, p, side, c]
            for e in range(2):
                cid = 2 * side + e if side < 2 else 2 * e + side - 2
                msg = CRECV[fr, p, cid]
                step = c if side >= 2 else GL * c
                if c:
                    msg = pltpu.roll(msg, step if e else LN - step, 1)
                at = beta_order(lane) if side >= 2 else lane
                inside = at >= LN - GL if e else at < GL
                v = sel(jnp.logical_and(inside, end_valid(side, e)), msg, v)
            return v

        def unpack_cols(ref, dst, fr, p):
            parts = []
            for cp in PLANES:
                low, high = merged(fr, p, 2, cp), merged(fr, p, 3, cp)
                z = ZS.at[NC * p + cp]
                for c in PLANES:
                    z[pl.ds(SB * c, GL), :] = low[GL * c:GL * (c + 1)]
                    z[pl.ds((SB * c - GL) % LN, GL), :] = high[GL * c:GL * (c + 1)]
                t = z[...].T
                parts.append([(pltpu.roll(t, LN - SB * c, 1) if c else t).reshape(2 * SB, SB, LN) for c in PLANES])
            lane = lanes_of((SB * KR, LN))
            ghost = jnp.logical_or(lane < GL, lane >= LN - GL)
            rows = pl.ds(2 * SB, SB * KR)
            for c in PLANES:
                new = jnp.concatenate([part[c] for part in parts], axis=1).reshape(SB * KR, LN)
                ref[dst, c, rows, :] = sel(ghost, new, ref[dst, c, rows, :])

        def unpack_rows(ref, dst, fr, p):
            lane = lanes_of((GL, LN))
            keep = jnp.logical_and(jnp.logical_or(lane >= GL, end_valid(0, 0)),
                                   jnp.logical_or(lane < LN - GL, end_valid(0, 1)))
            for c in PLANES:
                for side, first, s in ((0, 0, 0), (1, KR - H, SB - 1)):
                    v = merged(fr, p, side, c)
                    for n in PLANES:
                        rows = rows_at(first, s, n)
                        ref[dst, c, rows, :] = sel(keep, v[GL * n:GL * (n + 1)], ref[dst, c, rows, :])

        def pad_rows(ref):
            at = pl.ds(0, NPAN)
            ref[at, :, pl.ds(0, 2 * SB), :] = ref[at, :, pl.ds(SB * KR - 1, 2 * SB), :]
            ref[at, :, pl.ds(SB * (KR + 2), 2 * SB), :] = ref[at, :, pl.ds(2 * SB + 1, 2 * SB), :]

        def corner_case(fn):
            for sa, sb in corners:
                @pl.when(jnp.logical_and(at_edge(sa), at_edge(2 + sb)))
                def _():
                    fn(sa, sb)

        def quad_geom(sa, sb):
            k0, s = (0, 0) if sa == 0 else (KR - H, SB - 1)
            lane0 = 0 if sb == 0 else LN - GL
            lane, idx = lanes_of((H, LN)), rows_of((H, LN))
            col = idx if sa == sb else H - 1 - idx
            masks = [NC * (lane - lane0) + c == col for c in PLANES]
            return k0, s, lane, masks, pl.ds(SB * (k0 + 2) + s, H, stride=SB)

        def beta_column(ref, first, sa, sb, r):
            k0, s, lane, masks, rows = quad_geom(sa, sb)
            kr = H + r if sa == 0 else KR - H - 1 - r
            tot = jnp.zeros((NPAN, H, LN), F32)
            for c in PLANES:
                line = ref[pl.ds(first, NPAN), c, pl.ds(SB * (kr + 2) + s, 1), :]
                tot = sel(wide(masks[c]), jnp.broadcast_to(line, tot.shape), tot)
            l_to, c_to = (GL - 1, NC - 1 - r) if sb == 0 else (LN - GL, r)
            return jnp.broadcast_to(jnp.sum(tot, axis=2, keepdims=True), tot.shape), wide(lane == l_to), c_to, rows

        def alpha_lines(ref, first, sa, sb, r):
            _, _, lane, masks, rows = quad_geom(sa, sb)
            l_from, c_from = (GL, r) if sb == 0 else (LN - GL - 1, NC - 1 - r)
            zero = jnp.zeros((NPAN, H, LN), F32)
            col = jnp.sum(sel(wide(lane == l_from), ref[pl.ds(first, NPAN), c_from, rows, :], zero), axis=2, keepdims=True)
            col = jnp.broadcast_to(col, zero.shape)
            return [jnp.sum(sel(wide(mask), col, zero), axis=1, keepdims=True) for mask in masks]

        def wide(mask):
            return jnp.broadcast_to(mask[None], (NPAN, *mask.shape))

        def fill_quadrant(src, sa, sb):
            columns = [beta_column(src, 0, sa, sb, r) for r in range(2)]
            lines = [alpha_lines(src, 0, sa, sb, r) for r in range(2)]
            for r in range(2):
                col, mask, c_to, rows = columns[r]
                src[:, c_to, rows, :] = sel(mask, col, src[:, c_to, rows, :])
                for c in PLANES:
                    CQ[:, r, c] = jnp.broadcast_to(lines[r][c], (NPAN, SB, LN))

        def fill_winds(sa, sb):
            sign = -1.0 if sa == sb else 1.0
            col, mask, c_to, rows = beta_column(WW, WA, sa, sb, 0)
            line = alpha_lines(WW, WB, sa, sb, 0)
            to_b, to_a = pl.ds(WB, NPAN), pl.ds(WA, NPAN)
            WW[to_b, c_to, rows, :] = sel(mask, sign * col, WW[to_b, c_to, rows, :])
            row_lane = lanes_of((NPAN, 1, LN))
            inside = row_lane < GL if sb == 0 else row_lane >= LN - GL
            row = pl.ds(SB * (H + 1), 1) if sa == 0 else pl.ds(SB * (KR - H + 3) - 1, 1)
            for c in PLANES:
                WW[to_a, c, row, :] = sel(inside, sign * line[c], WW[to_a, c, row, :])

        def roll_down(v):
            return pltpu.roll(v, LN - 1, 1)

        def roll_up(v):
            return pltpu.roll(v, 1, 1)

        def beta_rows(src, p, k0, scale):
            rows = pl.ds(SB * (k0 + 2), SB * BETA_ROWS)
            a0, a1, a2 = (src[p, c, rows, :] for c in PLANES)
            a2l, a0r, a1r = roll_up(a2), roll_down(a0), roll_down(a1)
            e0, e1, e2 = a2l + a1, a0 + a2, a1 + a0r
            g0, g1, g2 = 8.0 * a0 - e0, 8.0 * a1 - e1, 8.0 * a2 - e2
            g0r = 8.0 * a0r - (a2 + a1r)
            x0 = WW[WB + p, 0, rows, :] * (g0 + g1)
            x1 = WW[WB + p, 1, rows, :] * (g1 + g2)
            x2 = WW[WB + p, 2, rows, :] * (g2 + g0r)
            x2l = roll_up(x2)
            return jnp.stack([x0 - x2l, x1 - x0, x2 - x1]), jnp.stack([e0, e1, e2])

        def row_group(ref, p, k):
            return ref[p, :, pl.ds(SB * (k + 2), SB), :]

        def panel_pass(src, dst, p, scale, second):
            lane, sub = lanes_of((NC, SB, LN)), rows_of((NC, SB, LN))
            ghost_lane = jnp.logical_or(jnp.logical_and(at_edge(2), lane < GL),
                                        jnp.logical_and(at_edge(3), lane >= LN - GL))
            in_low = jnp.logical_and(ghost_lane, jnp.logical_and(at_edge(0), sub == 0))
            in_high = jnp.logical_and(ghost_lane, jnp.logical_and(at_edge(1), sub == SB - 1))

            def load(k):
                v = row_group(src, p, k)
                if k in (H - 2, H - 1):
                    return sel(in_low, CQ[p, H - 1 - k], v)
                if k in (KR - H, KR - H + 1):
                    return sel(in_high, CQ[p, k - (KR - H)], v)
                return v

            qm, q0, q1 = load(-2), load(-1), load(0)
            q2 = load(1)
            g0 = 8.0 * q0 - (qm + q1)
            e1 = q0 + q2
            g1 = 8.0 * q1 - e1
            x_low = row_group(WW, WA + p, -1) * (g0 + g1)
            q_now, e_now, g_now, q_next = q1, e1, g1, q2
            beta = None
            for k in range(KR):
                if k % BETA_ROWS == 0:
                    beta = beta_rows(src, p, k, scale)
                at = SB * (k % BETA_ROWS)
                tb, eb = (v[:, at:at + SB] for v in beta)
                q_far = load(k + 2)
                e_next = q_now + q_far
                g_next = 8.0 * q_next - e_next
                x_high = row_group(WW, WA + p, k) * (g_now + g_next)
                u = scale * (x_high - x_low + tb) - (e_now + eb)
                new = KK[1, :, pl.ds(SB * k, SB), :] * q_now - KK[0, :, pl.ds(SB * k, SB), :] * u
                if second:
                    new = 0.5 * (row_group(dst, p, k) + new)
                dst[p, :, pl.ds(SB * (k + 2), SB), :] = new
                x_low, q_now, e_now, g_now, q_next = x_high, q_next, e_next, g_next, q_far

        def stage(src, dst, scale, second, more, after=None):
            pad_rows(src)

            @pl.when(more)
            def _():
                corner_case(lambda sa, sb: fill_quadrant(src, sa, sb))

            @pl.loop(0, NPAN)
            def _(p):
                panel_pass(src, dst, p, scale, second)
                if after is not None:
                    after(p)

        load_fields([(a_in, WW, WA), (b_in, WW, WB)])
        is_cc = jnp.logical_and(jnp.logical_or(at_edge(0), at_edge(1)), jnp.logical_or(at_edge(2), at_edge(3)))
        pl.semaphore_wait(barrier, SB * NPAN - NPAN * sel(is_cc, 1, 0))

        @pl.loop(1, 3)
        def _(f):
            @pl.loop(0, NPAN)
            def _(p):
                send_panel(WW, (f - 1) * NPAN + p, WW, (2 - f) * NPAN + p, f, f + 1, p, True)
        load_fields([(q_in, QA, 0)])

        def finish_winds():
            metric()

            @pl.loop(1, 3)
            def _(f):
                for p in slots:
                    wait_copies(RECV, CRECV, recv_sem, crecv_sem, f + 1, p)

                @pl.loop(0, NPAN)
                def _(p):
                    unpack_cols(WW, (2 - f) * NPAN + p, f + 1, p)

            @pl.loop(1, 3)
            def _(f):
                @pl.loop(0, NPAN)
                def _(p):
                    unpack_rows(WW, (f - 1) * NPAN + p, f + 1, p)
                for p in slots:
                    wait_copies(SEND, CSEND, send_sem, csend_sem, f, p)
            corner_case(fill_winds)
            pad_rows(WW)
            face_scale = 0.5 / (12.0 * 0.5 * C_SPEED)

            @pl.loop(0, NPAN)
            def _(p):
                for c in PLANES:
                    low, high = pl.ds(SB, SB * (KR + 1)), pl.ds(2 * SB, SB * (KR + 1))
                    WW[WA + p, c, low, :] = face_scale * (WW[WA + p, c, low, :] + WW[WA + p, c, high, :])
                rows = pl.ds(2 * SB, SB * KR)
                b0, b1, b2 = (WW[WB + p, c, rows, :] for c in PLANES)
                WW[WB + p, 0, rows, :] = face_scale * (b0 + b1)
                WW[WB + p, 1, rows, :] = face_scale * (b1 + b2)
                WW[WB + p, 2, rows, :] = face_scale * (b2 + roll_down(b0))

        def metric():
            ridx = rows_of((SB * KR, LN))
            gi = tx * tile_rows + lax.rem(ridx, SB) * KR + lax.div(ridx, SB) - H
            gi = sel(gi < 0, -1 - gi, sel(gi >= cells, 2 * cells - 1 - gi, gi))
            tan_a = small_tan((gi.astype(F32) + 0.5) * dalpha - 0.25 * math.pi)
            for c in PLANES:
                gj = ty * tile_rows + 3 * lanes_of((SB, LN)) + c - H
                gj = sel(gj < 0, -1 - gj, sel(gj >= cells, 2 * cells - 1 - gj, gj))
                tan_b = small_tan((gj.astype(F32) + 0.5) * dalpha - 0.25 * math.pi)[0:1, :]
                a_sq, b_sq = tan_a * tan_a, tan_b * tan_b
                r_sq = 1.0 + a_sq + b_sq
                sqrt_g = (1.0 + a_sq) * (1.0 + b_sq) / (r_sq * jnp.sqrt(r_sq))
                KK[0, c] = (0.5 * C_SPEED * CFL_STEP) / sqrt_g
                KK[1, c] = 1.0 - 4.0 * KK[0, c]

        @pl.loop(0, n_blocks)
        def _(b):
            fr = lax.rem(b, 2)

            @pl.when(b == 0)
            def _():
                @pl.loop(0, NPAN)
                def _(p):
                    send_panel(QA, p, QA, p, 0, 0, p, False)

            @pl.when(b == 0)
            def _():
                finish_winds()

            for p in slots:
                wait_copies(RECV, CRECV, recv_sem, crecv_sem, fr, p)
                unpack_cols(QA, p, fr, p)
                unpack_rows(QA, p, fr, p)
            for p in slots:
                wait_copies(SEND, CSEND, send_sem, csend_sem, 0, p)
            end = lax.div((b + 1) * steps, n_blocks)

            @pl.loop(lax.div(b * steps, n_blocks), end)
            def _(t):
                scale = ws_ref[t]
                stage(QA, QB, scale, False, True)

                def after(p):
                    @pl.when(jnp.logical_and(t + 1 == end, b + 1 < n_blocks))
                    def _():
                        send_panel(QA, p, QA, p, 0, 1 - fr, p, False)
                stage(QB, QA, scale, True, t + 1 < end, after)

        store_field(QA)

    return kernel


def solution(mesh):
    tile_count = mesh.shape['tx']
    field_spec = P(('member', 'panel'), 'tx', 'ty')
    wind_spec = P('panel', 'tx', 'ty')

    def local_run(tracer, wind_a, wind_b, wind_scale):
        steps = wind_scale.shape[0]
        n_blocks = -(-steps // STEPS_PER_BLOCK)
        ext = SB * KR
        block = pl.BlockSpec((NPAN, ext, ext), lambda n: (0, 0, 0))
        dma = pltpu.SemaphoreType.DMA
        return pl.pallas_call(
            make_kernel(tile_count, steps, n_blocks, tracer.shape[1]),
            grid=(1,),
            out_shape=jax.ShapeDtypeStruct(tracer.shape, F32),
            in_specs=[pl.BlockSpec(memory_space=pltpu.SMEM), block, block, block],
            out_specs=block,
            scratch_shapes=[
                pltpu.VMEM((NPAN, NC, ext + 32, LN), F32),
                pltpu.VMEM((NPAN, NC, ext + 32, LN), F32),
                pltpu.VMEM((2 * NPAN, NC, ext + 32, LN), F32),
                pltpu.VMEM((NPAN, 2, NC, SB, LN), F32),
                pltpu.VMEM((2, NC, ext, LN), F32),
                pltpu.VMEM((2 * NC, ext + 32, LN), F32),
                pltpu.VMEM((2 * NC, ext + 32, LN), F32),
                pltpu.VMEM((9, LN, LN), F32),
                pltpu.VMEM((3, NPAN, 4, NC, H, LN), F32),
                pltpu.VMEM((4, NPAN, 4, NC, H, LN), F32),
                pltpu.VMEM((3, NPAN, 4, H, LN), F32),
                pltpu.VMEM((4, NPAN, 4, H, LN), F32),
                *[dma((n, NPAN, 4)) for n in (3, 4, 3, 4)],
            ],
            compiler_params=pltpu.CompilerParams(collective_id=0, has_side_effects=True, vmem_limit_bytes=60 * 1024 * 1024),
            cost_estimate=pl.CostEstimate(flops=10 ** 9, bytes_accessed=10 ** 7, transcendentals=0),
        )(wind_scale, tracer, wind_a, wind_b)

    return jax.shard_map(local_run, mesh=mesh, in_specs=(field_spec, wind_spec, wind_spec, P()),
                         out_specs=field_spec, check_vma=False)
```

```python
import math
import jax
import numpy as np
import jax.numpy as jnp
from jax import lax
from jax.experimental import pallas as pl
from jax.experimental.pallas import tpu as pltpu
from jax.sharding import PartitionSpec as P

C_SPEED = 2.5
CFL_STEP = 0.12
EDGE_CODE = (
    (310, 100, 530, 420), (10, 200, 511, 410), (110, 300, 521, 431),
    (210, 0, 500, 401), (331, 130, 30, 231), (320, 121, 221, 20),
)
H = 12
KR = 48
NPAN = 3
NC = 3
SB = 8
LN = 128
GL = 4
BETA_SHIFT = 71
STEPS_PER_BLOCK = 3
BETA_ROWS = 4
F32 = jnp.float32
PLANES = range(NC)
SIDES = range(4)


def turned_sign(side_id, edge_id):
    return int(side_id % 2 == edge_id % 2)


def small_tan(v):
    sq = v * v
    sin_sum, cos_sum = jnp.full_like(v, 1.0), jnp.full_like(v, 1.0)
    for n in (6, 5, 4, 3, 2, 1):
        sin_sum = 1.0 - sq * sin_sum * (1.0 / (2 * n * (2 * n + 1)))
        cos_sum = 1.0 - sq * cos_sum * (1.0 / (2 * n * (2 * n - 1)))
    return v * sin_sum / cos_sum


def sel(pred, yes, no):
    yes, no = (np.int32(v) if isinstance(v, int) else v for v in (yes, no))
    same = jnp.shape(yes) == jnp.shape(no) and jnp.shape(pred) in ((), jnp.shape(yes))
    return lax.select(pred, yes, no) if same else jnp.where(pred, yes, no)


def lanes_of(shape):
    return lax.broadcasted_iota(jnp.int32, shape, len(shape) - 1)


def rows_of(shape):
    return lax.broadcasted_iota(jnp.int32, shape, len(shape) - 2)


def make_kernel(tile_count, steps, n_blocks, tile_rows):
    last = tile_count - 1
    cells = tile_rows * tile_count
    dalpha = 0.5 * math.pi / cells

    def kernel(ws_ref, q_in, a_in, b_in, out_ref, QA, QB, WW, CQ, KK, NN, TT, ZS, SEND, RECV, CSEND, CRECV,
               send_sem, recv_sem, csend_sem, crecv_sem):
        dev = lax.axis_index('panel')
        tx = lax.axis_index('tx')
        ty = lax.axis_index('ty')
        WA, WB = 0, NPAN

        def at_edge(side):
            return (tx == 0, tx == last, ty == 0, ty == last)[side]

        def pick(v0, v1):
            return v0 if v0 == v1 else v0 + dev * (v1 - v0)

        def neighbour(p, side):
            codes = [EDGE_CODE[NPAN * dv + p][side] for dv in (0, 1)]
            panels = [code // 100 for code in codes]
            edges = [code // 10 % 10 for code in codes]
            return (pick(*[n // NPAN for n in panels]), pick(*[n % NPAN for n in panels]), pick(*edges),
                    pick(*[code % 10 for code in codes]), pick(*[turned_sign(side, e) for e in edges]))

        def dest(p, side, off):
            along = (ty if side < 2 else tx) + off
            edge = at_edge(side)
            d_dev, d_slot, dside, flip, _ = neighbour(p, side)
            al = along + flip * (last - 2 * along)
            c_tx = sel(dside == 0, 0, sel(dside == 1, last, al))
            c_ty = sel(dside == 2, 0, sel(dside == 3, last, al))
            step = 2 * (side % 2) - 1
            in_tx, in_ty = (tx + step, ty + off) if side < 2 else (tx + off, ty + step)
            device = {'tx': sel(edge, c_tx, in_tx), 'ty': sel(edge, c_ty, in_ty),
                      'panel': sel(edge, d_dev, dev)}
            return device, sel(edge, d_slot, p), sel(edge, dside, side ^ 1), sel(edge, flip, 0)

        def corner_plan(p, sa, sb):
            out_b = at_edge(2 + sb)
            plans = []
            for side, end, off in ((sa, sb, 2 * sb - 1), (2 + sb, sa, 2 * sa - 1)):
                device, slot, dside, flip = dest(p, side, off)
                x = end + flip * (1 - 2 * end)
                e = 1 - x
                plans.append((device, slot, sel(dside < 2, 2 * dside + e, 2 * e + (dside - 2)), side, x,
                              sel(dside < 2, 0, 1)))
            device = {key: sel(out_b, plans[1][0][key], plans[0][0][key]) for key in plans[0][0]}
            return (device, *[sel(out_b, second, first) for first, second in zip(plans[0][1:], plans[1][1:])])

        def has_corner(sa, sb):
            return jnp.logical_not(jnp.logical_and(at_edge(sa), at_edge(2 + sb)))

        def is_here(device):
            return jnp.logical_and(jnp.logical_and(device['tx'] == tx, device['ty'] == ty), device['panel'] == dev)

        corners = [(sa, sb) for sa in range(2) for sb in range(2)]
        slots = range(NPAN)
        strip_to = [[dest(p, side, 0)[:3] for side in SIDES] for p in slots]
        stays = [[sel(is_here(plan[0]), 1, 0) for plan in row] for row in strip_to]
        corner_to = [[corner_plan(p, sa, sb) for sa, sb in corners] for p in slots]
        flips = [[sel(at_edge(side), neighbour(p, side)[3], 0) for side in SIDES] for p in slots]
        turns = [[sel(at_edge(side), neighbour(p, side)[4], 0) for side in SIDES] for p in slots]

        def at_slot(p, table):
            first = table[0]
            if isinstance(first, dict):
                return {key: at_slot(p, [row[key] for row in table]) for key in first}
            if isinstance(first, (tuple, list)):
                return [at_slot(p, [row[n] for row in table]) for n in range(len(first))]
            return sel(p == 0, first, sel(p == 1, table[1], table[2]))
        mesh_ids = pl.DeviceIdType.MESH

        barrier = pltpu.get_barrier_semaphore()

        for p in slots:
            for side in SIDES:
                pl.semaphore_signal(barrier, inc=1, device_id=strip_to[p][side][0], device_id_type=mesh_ids)
            for (sa, sb), plan in zip(corners, corner_to[p]):
                @pl.when(has_corner(sa, sb))
                def _():
                    pl.semaphore_signal(barrier, inc=1, device_id=plan[0], device_id_type=mesh_ids)

        def load_fields(jobs):
            @pl.loop(0, NPAN)
            def _(p):
                for f, (in_ref, _, _) in enumerate(jobs):
                    for it in PLANES:
                        for jt in PLANES:
                            TT[NC * f + it, pl.ds(H + LN * jt, LN), :] = in_ref[p, pl.ds(LN * it, LN), pl.ds(LN * jt, LN)].T
                        for c in PLANES:
                            NN[NC * f + c, pl.ds(H + LN * it, LN), :] = TT[NC * f + it, pl.ds(c, LN, stride=NC), :].T
                for f, (_, dst, base) in enumerate(jobs):
                    for c in PLANES:
                        for k in range(KR):
                            dst[base + p, c, pl.ds(SB * (k + 2), SB), :] = NN[NC * f + c, pl.ds(k, SB, stride=KR), :]

        def store_field(src):
            @pl.loop(0, NPAN)
            def _(p):
                for c in PLANES:
                    for k in range(KR):
                        NN[c, pl.ds(k, SB, stride=KR), :] = src[p, c, pl.ds(SB * (k + 2), SB), :]
                for it in PLANES:
                    for c in PLANES:
                        TT[it, pl.ds(c, LN, stride=NC), :] = NN[c, pl.ds(H + LN * it, LN), :].T
                    for jt in PLANES:
                        out_ref[p, pl.ds(LN * it, LN), pl.ds(LN * jt, LN)] = TT[it, pl.ds(H + LN * jt, LN), :].T

        def quarter(n):
            return pl.ds(GL * n, GL)

        def rows_at(first, s, n):
            return pl.ds(SB * (first + 2 + n) + s, GL, stride=NC * SB)

        def pack_strips(row_ref, row_at, col_ref, col_at, f, p):
            for c in PLANES:
                for n in PLANES:
                    SEND[f, p, 0, c, quarter(n), :] = row_ref[row_at, c, rows_at(H, 0, n), :]
                    SEND[f, p, 1, c, quarter(n), :] = row_ref[row_at, c, rows_at(KR - 2 * H, SB - 1, n), :]
            lane = lanes_of((LN, LN))

            def window(first):
                return jnp.logical_and(lane >= first, lane < first + GL)
            planes = [col_ref[col_at, c, pl.ds(2 * SB, SB * KR), :].reshape(2 * SB, NC * SB, LN) for c in PLANES]
            for cp in PLANES:
                mix = None
                for c in PLANES:
                    blk = planes[c][:, SB * cp:SB * (cp + 1)].reshape(LN, LN)
                    if c == 0:
                        mix = blk
                    else:
                        mine = jnp.logical_or(window(GL + SB * c), window(SB * (c - 1)))
                        mix = sel(mine, pltpu.roll(blk, SB * c, 1), mix)
                t = mix.T
                for c in PLANES:
                    low, high = GL + SB * c, (LN - SB + SB * c) % LN
                    SEND[f, p, 2, cp, quarter(c), :] = t[low:low + GL]
                    SEND[f, p, 3, cp, quarter(c), :] = t[high:high + GL]

        def beta_order(lane):
            return 2 * SB * lax.rem(lane, SB) + lax.div(lane, SB)

        def beta_lane(n):
            return SB * lax.rem(n, 2 * SB) + lax.div(n, 2 * SB)

        def turn_strips(f, p, winds):
            flip_at, turn_at, to = at_slot(p, flips), at_slot(p, turns), at_slot(p, strip_to)
            for side in SIDES:
                to_beta = to[side][2] >= 2
                moved = jnp.logical_not(to_beta) if side >= 2 else to_beta

                @pl.when(jnp.logical_or(flip_at[side] == 1, moved))
                def _():
                    back = flip_at[side] == 1
                    at = lanes_of((NC * H, LN))
                    at = beta_order(at) if side >= 2 else at
                    inside = jnp.logical_and(at >= GL, at < LN - GL)
                    now = [SEND[f, p, side, c] for c in PLANES]
                    old = jnp.concatenate([sel(back, now[NC - 1 - c], now[c]) for c in PLANES], axis=0)
                    come = lanes_of((LN, LN))
                    come = sel(to_beta, beta_order(come), come)
                    come = sel(back, LN - 1 - come, come)
                    come = beta_lane(come) if side >= 2 else come
                    place = (rows_of((LN, LN)) == come).astype(F32)
                    new = jnp.dot(sel(inside, old, jnp.zeros_like(old)), place, precision=lax.Precision.HIGHEST,
                                  preferred_element_type=F32)
                    for c in PLANES:
                        SEND[f, p, side, c] = new[H * c:H * (c + 1)]
                    if winds:
                        @pl.when(jnp.logical_and(f == 2, back))
                        def _():
                            for c in PLANES:
                                SEND[f, p, side, c] = -SEND[f, p, side, c]

                @pl.when(turn_at[side] == 1)
                def _():
                    for c in PLANES:
                        v = SEND[f, p, side, c]
                        if winds:
                            v = sel(f == 1, -v, v)
                        for m in range(H):
                            SEND[f, p, side, c, m:m + 1, :] = v[H - 1 - m:H - m, :]

        def pack_corners(f, p, plan):
            lane = lanes_of((H, LN))
            for cid, (_, _, _, side, x, to_beta) in enumerate(plan):
                beta, high = to_beta == 1, x == 1
                key = sel(beta, lax.rem(lane, SB), lane)
                key = sel(high, key, sel(beta, SB - 1, LN - 1) - key)
                step = sel(beta, 1, GL)
                first = sel(beta, LN - BETA_SHIFT, SB)
                msg = None
                for c in PLANES:
                    shift = sel(high, first + step * c, LN - first - step * c)
                    v = pltpu.roll(SEND[f, p, side, c], shift, 1)
                    msg = v if c == 0 else sel(key >= step * c, v, msg)
                CSEND[f, p, cid] = msg

        def send_panel(row_ref, row_at, col_ref, col_at, f, fr, p, winds):
            pack_strips(row_ref, row_at, col_ref, col_at, f, p)
            turn_strips(f, p, winds)
            plan = at_slot(p, corner_to)
            pack_corners(f, p, plan)
            to, here_at = at_slot(p, strip_to), at_slot(p, stays)
            for side in SIDES:
                device, slot, dside = to[side]

                @pl.when(here_at[side] == 1)
                def _():
                    RECV[fr, slot, dside] = SEND[f, p, side]

                @pl.when(here_at[side] == 0)
                def _():
                    pltpu.make_async_remote_copy(
                        src_ref=SEND.at[f, p, side], dst_ref=RECV.at[fr, slot, dside], send_sem=send_sem.at[f, p, side],
                        recv_sem=recv_sem.at[fr, slot, dside], device_id=device, device_id_type=mesh_ids).start()
            for cid, (sa, sb) in enumerate(corners):
                @pl.when(has_corner(sa, sb))
                def _():
                    device, slot, dcorner = plan[cid][:3]
                    pltpu.make_async_remote_copy(
                        src_ref=CSEND.at[f, p, cid], dst_ref=CRECV.at[fr, slot, dcorner], send_sem=csend_sem.at[f, p, cid],
                        recv_sem=crecv_sem.at[fr, slot, dcorner], device_id=device, device_id_type=mesh_ids).start()

        def wait_copies(strips, blocks, sem, csem, f, p):
            for side in SIDES:
                @pl.when(stays[p][side] == 0)
                def _():
                    pltpu.make_async_copy(strips.at[f, p, side], strips.at[f, p, side], sem.at[f, p, side]).wait()
            for cid, (sa, sb) in enumerate(corners):
                @pl.when(has_corner(sa, sb))
                def _():
                    pltpu.make_async_copy(blocks.at[f, p, cid], blocks.at[f, p, cid], csem.at[f, p, cid]).wait()

        def end_valid(side, e):
            if side < 2:
                return jnp.logical_not(at_edge(2 + e))
            return jnp.logical_and(jnp.logical_not(at_edge(e)), at_edge(side))

        def merged(fr, p, side, c):
            lane = lanes_of((H, LN))
            v = RECV[fr, p, side, c]
            for e in range(2):
                cid = 2 * side + e if side < 2 else 2 * e + side - 2
                msg = CRECV[fr, p, cid]
                step = c if side >= 2 else GL * c
                if c:
                    msg = pltpu.roll(msg, step if e else LN - step, 1)
                at = beta_order(lane) if side >= 2 else lane
                inside = at >= LN - GL if e else at < GL
                v = sel(jnp.logical_and(inside, end_valid(side, e)), msg, v)
            return v

        def unpack_cols(ref, dst, fr, p):
            parts = []
            for cp in PLANES:
                low, high = merged(fr, p, 2, cp), merged(fr, p, 3, cp)
                z = ZS.at[NC * p + cp]
                for c in PLANES:
                    z[pl.ds(SB * c, GL), :] = low[GL * c:GL * (c + 1)]
                    z[pl.ds((SB * c - GL) % LN, GL), :] = high[GL * c:GL * (c + 1)]
                t = z[...].T
                parts.append([(pltpu.roll(t, LN - SB * c, 1) if c else t).reshape(2 * SB, SB, LN) for c in PLANES])
            lane = lanes_of((SB * KR, LN))
            ghost = jnp.logical_or(lane < GL, lane >= LN - GL)
            rows = pl.ds(2 * SB, SB * KR)
            for c in PLANES:
                new = jnp.concatenate([part[c] for part in parts], axis=1).reshape(SB * KR, LN)
                ref[dst, c, rows, :] = sel(ghost, new, ref[dst, c, rows, :])

        def unpack_rows(ref, dst, fr, p):
            lane = lanes_of((GL, LN))
            keep = jnp.logical_and(jnp.logical_or(lane >= GL, end_valid(0, 0)),
                                   jnp.logical_or(lane < LN - GL, end_valid(0, 1)))
            for c in PLANES:
                for side, first, s in ((0, 0, 0), (1, KR - H, SB - 1)):
                    v = merged(fr, p, side, c)
                    for n in PLANES:
                        rows = rows_at(first, s, n)
                        ref[dst, c, rows, :] = sel(keep, v[GL * n:GL * (n + 1)], ref[dst, c, rows, :])

        def pad_rows(ref):
            at = pl.ds(0, NPAN)
            ref[at, :, pl.ds(0, 2 * SB), :] = ref[at, :, pl.ds(SB * KR - 1, 2 * SB), :]
            ref[at, :, pl.ds(SB * (KR + 2), 2 * SB), :] = ref[at, :, pl.ds(2 * SB + 1, 2 * SB), :]

        def corner_case(fn):
            for sa, sb in corners:
                @pl.when(jnp.logical_and(at_edge(sa), at_edge(2 + sb)))
                def _():
                    fn(sa, sb)

        def quad_geom(sa, sb):
            k0, s = (0, 0) if sa == 0 else (KR - H, SB - 1)
            lane0 = 0 if sb == 0 else LN - GL
            lane, idx = lanes_of((H, LN)), rows_of((H, LN))
            col = idx if sa == sb else H - 1 - idx
            masks = [NC * (lane - lane0) + c == col for c in PLANES]
            return k0, s, lane, masks, pl.ds(SB * (k0 + 2) + s, H, stride=SB)

        def beta_column(ref, first, sa, sb, r):
            k0, s, lane, masks, rows = quad_geom(sa, sb)
            kr = H + r if sa == 0 else KR - H - 1 - r
            tot = jnp.zeros((NPAN, H, LN), F32)
            for c in PLANES:
                line = ref[pl.ds(first, NPAN), c, pl.ds(SB * (kr + 2) + s, 1), :]
                tot = sel(wide(masks[c]), jnp.broadcast_to(line, tot.shape), tot)
            l_to, c_to = (GL - 1, NC - 1 - r) if sb == 0 else (LN - GL, r)
            return jnp.broadcast_to(jnp.sum(tot, axis=2, keepdims=True), tot.shape), wide(lane == l_to), c_to, rows

        def alpha_lines(ref, first, sa, sb, r):
            _, _, lane, masks, rows = quad_geom(sa, sb)
            l_from, c_from = (GL, r) if sb == 0 else (LN - GL - 1, NC - 1 - r)
            zero = jnp.zeros((NPAN, H, LN), F32)
            col = jnp.sum(sel(wide(lane == l_from), ref[pl.ds(first, NPAN), c_from, rows, :], zero), axis=2, keepdims=True)
            col = jnp.broadcast_to(col, zero.shape)
            return [jnp.sum(sel(wide(mask), col, zero), axis=1, keepdims=True) for mask in masks]

        def wide(mask):
            return jnp.broadcast_to(mask[None], (NPAN, *mask.shape))

        def fill_quadrant(src, sa, sb):
            columns = [beta_column(src, 0, sa, sb, r) for r in range(2)]
            lines = [alpha_lines(src, 0, sa, sb, r) for r in range(2)]
            for r in range(2):
                col, mask, c_to, rows = columns[r]
                src[:, c_to, rows, :] = sel(mask, col, src[:, c_to, rows, :])
                for c in PLANES:
                    CQ[:, r, c] = jnp.broadcast_to(lines[r][c], (NPAN, SB, LN))

        def fill_winds(sa, sb):
            sign = -1.0 if sa == sb else 1.0
            col, mask, c_to, rows = beta_column(WW, WA, sa, sb, 0)
            line = alpha_lines(WW, WB, sa, sb, 0)
            to_b, to_a = pl.ds(WB, NPAN), pl.ds(WA, NPAN)
            WW[to_b, c_to, rows, :] = sel(mask, sign * col, WW[to_b, c_to, rows, :])
            row_lane = lanes_of((NPAN, 1, LN))
            inside = row_lane < GL if sb == 0 else row_lane >= LN - GL
            row = pl.ds(SB * (H + 1), 1) if sa == 0 else pl.ds(SB * (KR - H + 3) - 1, 1)
            for c in PLANES:
                WW[to_a, c, row, :] = sel(inside, sign * line[c], WW[to_a, c, row, :])

        def roll_down(v):
            return pltpu.roll(v, LN - 1, 1)

        def roll_up(v):
            return pltpu.roll(v, 1, 1)

        def beta_rows(src, p, k0, scale):
            rows = pl.ds(SB * (k0 + 2), SB * BETA_ROWS)
            a0, a1, a2 = (src[p, c, rows, :] for c in PLANES)
            a2l, a0r, a1r = roll_up(a2), roll_down(a0), roll_down(a1)
            e0, e1, e2 = a2l + a1, a0 + a2, a1 + a0r
            g0, g1, g2 = 8.0 * a0 - e0, 8.0 * a1 - e1, 8.0 * a2 - e2
            g0r = 8.0 * a0r - (a2 + a1r)
            x0 = WW[WB + p, 0, rows, :] * (g0 + g1)
            x1 = WW[WB + p, 1, rows, :] * (g1 + g2)
            x2 = WW[WB + p, 2, rows, :] * (g2 + g0r)
            x2l = roll_up(x2)
            return jnp.stack([x0 - x2l, x1 - x0, x2 - x1]), jnp.stack([e0, e1, e2])

        def row_group(ref, p, k):
            return ref[p, :, pl.ds(SB * (k + 2), SB), :]

        def panel_pass(src, dst, p, scale, second):
            lane, sub = lanes_of((NC, SB, LN)), rows_of((NC, SB, LN))
            ghost_lane = jnp.logical_or(jnp.logical_and(at_edge(2), lane < GL),
                                        jnp.logical_and(at_edge(3), lane >= LN - GL))
            in_low = jnp.logical_and(ghost_lane, jnp.logical_and(at_edge(0), sub == 0))
            in_high = jnp.logical_and(ghost_lane, jnp.logical_and(at_edge(1), sub == SB - 1))

            def load(k):
                v = row_group(src, p, k)
                if k in (H - 2, H - 1):
                    return sel(in_low, CQ[p, H - 1 - k], v)
                if k in (KR - H, KR - H + 1):
                    return sel(in_high, CQ[p, k - (KR - H)], v)
                return v

            qm, q0, q1 = load(-2), load(-1), load(0)
            q2 = load(1)
            g0 = 8.0 * q0 - (qm + q1)
            e1 = q0 + q2
            g1 = 8.0 * q1 - e1
            x_low = row_group(WW, WA + p, -1) * (g0 + g1)
            q_now, e_now, g_now, q_next = q1, e1, g1, q2
            beta = None
            for k in range(KR):
                if k % BETA_ROWS == 0:
                    beta = beta_rows(src, p, k, scale)
                at = SB * (k % BETA_ROWS)
                tb, eb = (v[:, at:at + SB] for v in beta)
                q_far = load(k + 2)
                e_next = q_now + q_far
                g_next = 8.0 * q_next - e_next
                x_high = row_group(WW, WA + p, k) * (g_now + g_next)
                u = scale * (x_high - x_low + tb) - (e_now + eb)
                new = KK[1, :, pl.ds(SB * k, SB), :] * q_now - KK[0, :, pl.ds(SB * k, SB), :] * u
                if second:
                    new = 0.5 * (row_group(dst, p, k) + new)
                dst[p, :, pl.ds(SB * (k + 2), SB), :] = new
                x_low, q_now, e_now, g_now, q_next = x_high, q_next, e_next, g_next, q_far

        def stage(src, dst, scale, second, more, after=None):
            pad_rows(src)

            @pl.when(more)
            def _():
                corner_case(lambda sa, sb: fill_quadrant(src, sa, sb))

            @pl.loop(0, NPAN)
            def _(p):
                panel_pass(src, dst, p, scale, second)
                if after is not None:
                    after(p)

        load_fields([(a_in, WW, WA), (b_in, WW, WB)])
        is_cc = jnp.logical_and(jnp.logical_or(at_edge(0), at_edge(1)), jnp.logical_or(at_edge(2), at_edge(3)))
        pl.semaphore_wait(barrier, SB * NPAN - NPAN * sel(is_cc, 1, 0))

        @pl.loop(1, 3)
        def _(f):
            @pl.loop(0, NPAN)
            def _(p):
                send_panel(WW, (f - 1) * NPAN + p, WW, (2 - f) * NPAN + p, f, f + 1, p, True)
        load_fields([(q_in, QA, 0)])

        def finish_winds():
            metric()

            @pl.loop(1, 3)
            def _(f):
                for p in slots:
                    wait_copies(RECV, CRECV, recv_sem, crecv_sem, f + 1, p)
                    unpack_cols(WW, (2 - f) * NPAN + p, f + 1, p)

            @pl.loop(1, 3)
            def _(f):
                @pl.loop(0, NPAN)
                def _(p):
                    unpack_rows(WW, (f - 1) * NPAN + p, f + 1, p)
                for p in slots:
                    wait_copies(SEND, CSEND, send_sem, csend_sem, f, p)
            corner_case(fill_winds)
            pad_rows(WW)
            face_scale = 0.5 / (12.0 * 0.5 * C_SPEED)

            @pl.loop(0, NPAN)
            def _(p):
                for c in PLANES:
                    low, high = pl.ds(SB, SB * (KR + 1)), pl.ds(2 * SB, SB * (KR + 1))
                    WW[WA + p, c, low, :] = face_scale * (WW[WA + p, c, low, :] + WW[WA + p, c, high, :])
                rows = pl.ds(2 * SB, SB * KR)
                b0, b1, b2 = (WW[WB + p, c, rows, :] for c in PLANES)
                WW[WB + p, 0, rows, :] = face_scale * (b0 + b1)
                WW[WB + p, 1, rows, :] = face_scale * (b1 + b2)
                WW[WB + p, 2, rows, :] = face_scale * (b2 + roll_down(b0))

        def metric():
            ridx = rows_of((SB * KR, LN))
            gi = tx * tile_rows + lax.rem(ridx, SB) * KR + lax.div(ridx, SB) - H
            gi = sel(gi < 0, -1 - gi, sel(gi >= cells, 2 * cells - 1 - gi, gi))
            tan_a = small_tan((gi.astype(F32) + 0.5) * dalpha - 0.25 * math.pi)
            for c in PLANES:
                gj = ty * tile_rows + 3 * lanes_of((SB, LN)) + c - H
                gj = sel(gj < 0, -1 - gj, sel(gj >= cells, 2 * cells - 1 - gj, gj))
                tan_b = small_tan((gj.astype(F32) + 0.5) * dalpha - 0.25 * math.pi)[0:1, :]
                a_sq, b_sq = tan_a * tan_a, tan_b * tan_b
                r_sq = 1.0 + a_sq + b_sq
                sqrt_g = (1.0 + a_sq) * (1.0 + b_sq) / (r_sq * jnp.sqrt(r_sq))
                KK[0, c] = (0.5 * C_SPEED * CFL_STEP) / sqrt_g
                KK[1, c] = 1.0 - 4.0 * KK[0, c]

        @pl.loop(0, n_blocks)
        def _(b):
            fr = lax.rem(b, 2)

            @pl.when(b == 0)
            def _():
                @pl.loop(0, NPAN)
                def _(p):
                    send_panel(QA, p, QA, p, 0, 0, p, False)

            @pl.when(b == 0)
            def _():
                finish_winds()

            for p in slots:
                wait_copies(RECV, CRECV, recv_sem, crecv_sem, fr, p)
                unpack_cols(QA, p, fr, p)
                unpack_rows(QA, p, fr, p)
            for p in slots:
                wait_copies(SEND, CSEND, send_sem, csend_sem, 0, p)
            end = lax.div((b + 1) * steps, n_blocks)

            @pl.loop(lax.div(b * steps, n_blocks), end)
            def _(t):
                scale = ws_ref[t]
                stage(QA, QB, scale, False, True)

                def after(p):
                    @pl.when(jnp.logical_and(t + 1 == end, b + 1 < n_blocks))
                    def _():
                        send_panel(QA, p, QA, p, 0, 1 - fr, p, False)
                stage(QB, QA, scale, True, t + 1 < end, after)

        store_field(QA)

    return kernel


def solution(mesh):
    tile_count = mesh.shape['tx']
    field_spec = P(('member', 'panel'), 'tx', 'ty')
    wind_spec = P('panel', 'tx', 'ty')

    def local_run(tracer, wind_a, wind_b, wind_scale):
        steps = wind_scale.shape[0]
        n_blocks = -(-steps // STEPS_PER_BLOCK)
        ext = SB * KR
        block = pl.BlockSpec((NPAN, ext, ext), lambda n: (0, 0, 0))
        dma = pltpu.SemaphoreType.DMA
        return pl.pallas_call(
            make_kernel(tile_count, steps, n_blocks, tracer.shape[1]),
            grid=(1,),
            out_shape=jax.ShapeDtypeStruct(tracer.shape, F32),
            in_specs=[pl.BlockSpec(memory_space=pltpu.SMEM), block, block, block],
            out_specs=block,
            scratch_shapes=[
                pltpu.VMEM((NPAN, NC, ext + 32, LN), F32),
                pltpu.VMEM((NPAN, NC, ext + 32, LN), F32),
                pltpu.VMEM((2 * NPAN, NC, ext + 32, LN), F32),
                pltpu.VMEM((NPAN, 2, NC, SB, LN), F32),
                pltpu.VMEM((2, NC, ext, LN), F32),
                pltpu.VMEM((2 * NC, ext + 32, LN), F32),
                pltpu.VMEM((2 * NC, ext + 32, LN), F32),
                pltpu.VMEM((9, LN, LN), F32),
                pltpu.VMEM((3, NPAN, 4, NC, H, LN), F32),
                pltpu.VMEM((4, NPAN, 4, NC, H, LN), F32),
                pltpu.VMEM((3, NPAN, 4, H, LN), F32),
                pltpu.VMEM((4, NPAN, 4, H, LN), F32),
                *[dma((n, NPAN, 4)) for n in (3, 4, 3, 4)],
            ],
            compiler_params=pltpu.CompilerParams(collective_id=0, has_side_effects=True, vmem_limit_bytes=60 * 1024 * 1024),
            cost_estimate=pl.CostEstimate(flops=10 ** 9, bytes_accessed=10 ** 7, transcendentals=0),
        )(wind_scale, tracer, wind_a, wind_b)

    return jax.shard_map(local_run, mesh=mesh, in_specs=(field_spec, wind_spec, wind_spec, P()),
                         out_specs=field_spec, check_vma=False)
```

```python
import math
import jax
import numpy as np
import jax.numpy as jnp
from jax import lax
from jax.experimental import pallas as pl
from jax.experimental.pallas import tpu as pltpu
from jax.sharding import PartitionSpec as P

C_SPEED = 2.5
CFL_STEP = 0.12
EDGE_CODE = (
    (310, 100, 530, 420), (10, 200, 511, 410), (110, 300, 521, 431),
    (210, 0, 500, 401), (331, 130, 30, 231), (320, 121, 221, 20),
)
H = 12
KR = 48
NPAN = 3
NC = 3
SB = 8
LN = 128
GL = 4
BETA_SHIFT = 71
STEPS_PER_BLOCK = 3
BETA_ROWS = 4
F32 = jnp.float32
PLANES = range(NC)
SIDES = range(4)


def turned_sign(side_id, edge_id):
    return int(side_id % 2 == edge_id % 2)


def small_tan(v):
    sq = v * v
    sin_sum, cos_sum = jnp.full_like(v, 1.0), jnp.full_like(v, 1.0)
    for n in (6, 5, 4, 3, 2, 1):
        sin_sum = 1.0 - sq * sin_sum * (1.0 / (2 * n * (2 * n + 1)))
        cos_sum = 1.0 - sq * cos_sum * (1.0 / (2 * n * (2 * n - 1)))
    return v * sin_sum / cos_sum


def sel(pred, yes, no):
    yes, no = (np.int32(v) if isinstance(v, int) else v for v in (yes, no))
    same = jnp.shape(yes) == jnp.shape(no) and jnp.shape(pred) in ((), jnp.shape(yes))
    return lax.select(pred, yes, no) if same else jnp.where(pred, yes, no)


def lanes_of(shape):
    return lax.broadcasted_iota(jnp.int32, shape, len(shape) - 1)


def rows_of(shape):
    return lax.broadcasted_iota(jnp.int32, shape, len(shape) - 2)


def make_kernel(tile_count, steps, n_blocks, tile_rows):
    last = tile_count - 1
    cells = tile_rows * tile_count
    dalpha = 0.5 * math.pi / cells

    def kernel(ws_ref, q_in, a_in, b_in, out_ref, QA, QB, WW, CQ, KK, NN, TT, ZS, SEND, RECV, CSEND, CRECV,
               send_sem, recv_sem, csend_sem, crecv_sem):
        dev = lax.axis_index('panel')
        tx = lax.axis_index('tx')
        ty = lax.axis_index('ty')
        WA, WB = 0, NPAN

        def at_edge(side):
            return (tx == 0, tx == last, ty == 0, ty == last)[side]

        def pick(v0, v1):
            return v0 if v0 == v1 else v0 + dev * (v1 - v0)

        def neighbour(p, side):
            codes = [EDGE_CODE[NPAN * dv + p][side] for dv in (0, 1)]
            panels = [code // 100 for code in codes]
            edges = [code // 10 % 10 for code in codes]
            return (pick(*[n // NPAN for n in panels]), pick(*[n % NPAN for n in panels]), pick(*edges),
                    pick(*[code % 10 for code in codes]), pick(*[turned_sign(side, e) for e in edges]))

        def dest(p, side, off):
            along = (ty if side < 2 else tx) + off
            edge = at_edge(side)
            d_dev, d_slot, dside, flip, _ = neighbour(p, side)
            al = along + flip * (last - 2 * along)
            c_tx = sel(dside == 0, 0, sel(dside == 1, last, al))
            c_ty = sel(dside == 2, 0, sel(dside == 3, last, al))
            step = 2 * (side % 2) - 1
            in_tx, in_ty = (tx + step, ty + off) if side < 2 else (tx + off, ty + step)
            device = {'tx': sel(edge, c_tx, in_tx), 'ty': sel(edge, c_ty, in_ty),
                      'panel': sel(edge, d_dev, dev)}
            return device, sel(edge, d_slot, p), sel(edge, dside, side ^ 1), sel(edge, flip, 0)

        def corner_plan(p, sa, sb):
            out_b = at_edge(2 + sb)
            plans = []
            for side, end, off in ((sa, sb, 2 * sb - 1), (2 + sb, sa, 2 * sa - 1)):
                device, slot, dside, flip = dest(p, side, off)
                x = end + flip * (1 - 2 * end)
                e = 1 - x
                plans.append((device, slot, sel(dside < 2, 2 * dside + e, 2 * e + (dside - 2)), side, x,
                              sel(dside < 2, 0, 1)))
            device = {key: sel(out_b, plans[1][0][key], plans[0][0][key]) for key in plans[0][0]}
            return (device, *[sel(out_b, second, first) for first, second in zip(plans[0][1:], plans[1][1:])])

        def has_corner(sa, sb):
            return jnp.logical_not(jnp.logical_and(at_edge(sa), at_edge(2 + sb)))

        def is_here(device):
            return jnp.logical_and(jnp.logical_and(device['tx'] == tx, device['ty'] == ty), device['panel'] == dev)

        corners = [(sa, sb) for sa in range(2) for sb in range(2)]
        slots = range(NPAN)
        strip_to = [[dest(p, side, 0)[:3] for side in SIDES] for p in slots]
        stays = [[sel(is_here(plan[0]), 1, 0) for plan in row] for row in strip_to]
        corner_to = [[corner_plan(p, sa, sb) for sa, sb in corners] for p in slots]
        flips = [[sel(at_edge(side), neighbour(p, side)[3], 0) for side in SIDES] for p in slots]
        turns = [[sel(at_edge(side), neighbour(p, side)[4], 0) for side in SIDES] for p in slots]

        def at_slot(p, table):
            first = table[0]
            if isinstance(first, dict):
                return {key: at_slot(p, [row[key] for row in table]) for key in first}
            if isinstance(first, (tuple, list)):
                return [at_slot(p, [row[n] for row in table]) for n in range(len(first))]
            return sel(p == 0, first, sel(p == 1, table[1], table[2]))
        mesh_ids = pl.DeviceIdType.MESH

        barrier = pltpu.get_barrier_semaphore()

        for p in slots:
            for side in SIDES:
                pl.semaphore_signal(barrier, inc=1, device_id=strip_to[p][side][0], device_id_type=mesh_ids)
            for (sa, sb), plan in zip(corners, corner_to[p]):
                @pl.when(has_corner(sa, sb))
                def _():
                    pl.semaphore_signal(barrier, inc=1, device_id=plan[0], device_id_type=mesh_ids)

        def load_fields(jobs):
            @pl.loop(0, NPAN)
            def _(p):
                for f, (in_ref, _, _) in enumerate(jobs):
                    for it in PLANES:
                        for jt in PLANES:
                            TT[NC * f + it, pl.ds(H + LN * jt, LN), :] = in_ref[p, pl.ds(LN * it, LN), pl.ds(LN * jt, LN)].T
                        for c in PLANES:
                            NN[NC * f + c, pl.ds(H + LN * it, LN), :] = TT[NC * f + it, pl.ds(c, LN, stride=NC), :].T
                for f, (_, dst, base) in enumerate(jobs):
                    for c in PLANES:
                        for k in range(KR):
                            dst[base + p, c, pl.ds(SB * (k + 2), SB), :] = NN[NC * f + c, pl.ds(k, SB, stride=KR), :]

        def store_field(src):
            @pl.loop(0, NPAN)
            def _(p):
                @pl.loop(0, KR // SB)
                def _(kb):
                    for c in PLANES:
                        for k in range(SB):
                            NN[c, pl.ds(SB * kb + k, SB, stride=KR), :] = src[p, c, pl.ds(pl.multiple_of(64 * kb + SB * (k + 2), SB), SB), :]
                for it in PLANES:
                    for c in PLANES:
                        TT[it, pl.ds(c, LN, stride=NC), :] = NN[c, pl.ds(H + LN * it, LN), :].T
                    for jt in PLANES:
                        out_ref[p, pl.ds(LN * it, LN), pl.ds(LN * jt, LN)] = TT[it, pl.ds(H + LN * jt, LN), :].T

        def quarter(n):
            return pl.ds(GL * n, GL)

        def rows_at(first, s, n):
            return pl.ds(SB * (first + 2 + n) + s, GL, stride=NC * SB)

        def pack_strips(row_ref, row_at, col_ref, col_at, f, p):
            for c in PLANES:
                for n in PLANES:
                    SEND[f, p, 0, c, quarter(n), :] = row_ref[row_at, c, rows_at(H, 0, n), :]
                    SEND[f, p, 1, c, quarter(n), :] = row_ref[row_at, c, rows_at(KR - 2 * H, SB - 1, n), :]
            lane = lanes_of((LN, LN))

            def window(first):
                return jnp.logical_and(lane >= first, lane < first + GL)
            planes = [col_ref[col_at, c, pl.ds(2 * SB, SB * KR), :].reshape(2 * SB, NC * SB, LN) for c in PLANES]
            for cp in PLANES:
                mix = None
                for c in PLANES:
                    blk = planes[c][:, SB * cp:SB * (cp + 1)].reshape(LN, LN)
                    if c == 0:
                        mix = blk
                    else:
                        mine = jnp.logical_or(window(GL + SB * c), window(SB * (c - 1)))
                        mix = sel(mine, pltpu.roll(blk, SB * c, 1), mix)
                t = mix.T
                for c in PLANES:
                    low, high = GL + SB * c, (LN - SB + SB * c) % LN
                    SEND[f, p, 2, cp, quarter(c), :] = t[low:low + GL]
                    SEND[f, p, 3, cp, quarter(c), :] = t[high:high + GL]

        def beta_order(lane):
            return 2 * SB * lax.rem(lane, SB) + lax.div(lane, SB)

        def beta_lane(n):
            return SB * lax.rem(n, 2 * SB) + lax.div(n, 2 * SB)

        def turn_strips(f, p, winds):
            flip_at, turn_at, to = at_slot(p, flips), at_slot(p, turns), at_slot(p, strip_to)
            for side in SIDES:
                to_beta = to[side][2] >= 2
                moved = jnp.logical_not(to_beta) if side >= 2 else to_beta

                @pl.when(jnp.logical_or(flip_at[side] == 1, moved))
                def _():
                    back = flip_at[side] == 1
                    at = lanes_of((NC * H, LN))
                    at = beta_order(at) if side >= 2 else at
                    inside = jnp.logical_and(at >= GL, at < LN - GL)
                    now = [SEND[f, p, side, c] for c in PLANES]
                    old = jnp.concatenate([sel(back, now[NC - 1 - c], now[c]) for c in PLANES], axis=0)
                    come = lanes_of((LN, LN))
                    come = sel(to_beta, beta_order(come), come)
                    come = sel(back, LN - 1 - come, come)
                    come = beta_lane(come) if side >= 2 else come
                    place = (rows_of((LN, LN)) == come).astype(F32)
                    new = jnp.dot(sel(inside, old, jnp.zeros_like(old)), place, precision=lax.Precision.HIGHEST,
                                  preferred_element_type=F32)
                    for c in PLANES:
                        SEND[f, p, side, c] = new[H * c:H * (c + 1)]
                    if winds:
                        @pl.when(jnp.logical_and(f == 2, back))
                        def _():
                            for c in PLANES:
                                SEND[f, p, side, c] = -SEND[f, p, side, c]

                @pl.when(turn_at[side] == 1)
                def _():
                    for c in PLANES:
                        v = SEND[f, p, side, c]
                        if winds:
                            v = sel(f == 1, -v, v)
                        for m in range(H):
                            SEND[f, p, side, c, m:m + 1, :] = v[H - 1 - m:H - m, :]

        def pack_corners(f, p, plan):
            lane = lanes_of((H, LN))
            for cid, (_, _, _, side, x, to_beta) in enumerate(plan):
                beta, high = to_beta == 1, x == 1
                key = sel(beta, lax.rem(lane, SB), lane)
                key = sel(high, key, sel(beta, SB - 1, LN - 1) - key)
                step = sel(beta, 1, GL)
                first = sel(beta, LN - BETA_SHIFT, SB)
                msg = None
                for c in PLANES:
                    shift = sel(high, first + step * c, LN - first - step * c)
                    v = pltpu.roll(SEND[f, p, side, c], shift, 1)
                    msg = v if c == 0 else sel(key >= step * c, v, msg)
                CSEND[f, p, cid] = msg

        def send_panel(row_ref, row_at, col_ref, col_at, f, fr, p, winds):
            pack_strips(row_ref, row_at, col_ref, col_at, f, p)
            turn_strips(f, p, winds)
            to, here_at = at_slot(p, strip_to), at_slot(p, stays)
            for side in SIDES:
                device, slot, dside = to[side]

                @pl.when(here_at[side] == 1)
                def _():
                    RECV[fr, slot, dside] = SEND[f, p, side]

                @pl.when(here_at[side] == 0)
                def _():
                    pltpu.make_async_remote_copy(
                        src_ref=SEND.at[f, p, side], dst_ref=RECV.at[fr, slot, dside], send_sem=send_sem.at[f, p, side],
                        recv_sem=recv_sem.at[fr, slot, dside], device_id=device, device_id_type=mesh_ids).start()
            plan = at_slot(p, corner_to)
            pack_corners(f, p, plan)
            for cid, (sa, sb) in enumerate(corners):
                @pl.when(has_corner(sa, sb))
                def _():
                    device, slot, dcorner = plan[cid][:3]
                    pltpu.make_async_remote_copy(
                        src_ref=CSEND.at[f, p, cid], dst_ref=CRECV.at[fr, slot, dcorner], send_sem=csend_sem.at[f, p, cid],
                        recv_sem=crecv_sem.at[fr, slot, dcorner], device_id=device, device_id_type=mesh_ids).start()

        def wait_copies(strips, blocks, sem, csem, f, p):
            for side in SIDES:
                @pl.when(stays[p][side] == 0)
                def _():
                    pltpu.make_async_copy(strips.at[f, p, side], strips.at[f, p, side], sem.at[f, p, side]).wait()
            for cid, (sa, sb) in enumerate(corners):
                @pl.when(has_corner(sa, sb))
                def _():
                    pltpu.make_async_copy(blocks.at[f, p, cid], blocks.at[f, p, cid], csem.at[f, p, cid]).wait()

        def end_valid(side, e):
            if side < 2:
                return jnp.logical_not(at_edge(2 + e))
            return jnp.logical_and(jnp.logical_not(at_edge(e)), at_edge(side))

        def merged(fr, p, side, c):
            lane = lanes_of((H, LN))
            v = RECV[fr, p, side, c]
            for e in range(2):
                cid = 2 * side + e if side < 2 else 2 * e + side - 2
                msg = CRECV[fr, p, cid]
                step = c if side >= 2 else GL * c
                if c:
                    msg = pltpu.roll(msg, step if e else LN - step, 1)
                at = beta_order(lane) if side >= 2 else lane
                inside = at >= LN - GL if e else at < GL
                v = sel(jnp.logical_and(inside, end_valid(side, e)), msg, v)
            return v

        def unpack_cols(ref, dst, fr, p):
            parts = []
            for cp in PLANES:
                low, high = merged(fr, p, 2, cp), merged(fr, p, 3, cp)
                z = ZS.at[NC * p + cp]
                for c in PLANES:
                    z[pl.ds(SB * c, GL), :] = low[GL * c:GL * (c + 1)]
                    z[pl.ds((SB * c - GL) % LN, GL), :] = high[GL * c:GL * (c + 1)]
                t = z[...].T
                parts.append([(pltpu.roll(t, LN - SB * c, 1) if c else t).reshape(2 * SB, SB, LN) for c in PLANES])
            lane = lanes_of((SB * KR, LN))
            ghost = jnp.logical_or(lane < GL, lane >= LN - GL)
            rows = pl.ds(2 * SB, SB * KR)
            for c in PLANES:
                new = jnp.concatenate([part[c] for part in parts], axis=1).reshape(SB * KR, LN)
                ref[dst, c, rows, :] = sel(ghost, new, ref[dst, c, rows, :])

        def unpack_rows(ref, dst, fr, p):
            lane = lanes_of((GL, LN))
            keep = jnp.logical_and(jnp.logical_or(lane >= GL, end_valid(0, 0)),
                                   jnp.logical_or(lane < LN - GL, end_valid(0, 1)))
            for c in PLANES:
                for side, first, s in ((0, 0, 0), (1, KR - H, SB - 1)):
                    v = merged(fr, p, side, c)
                    for n in PLANES:
                        rows = rows_at(first, s, n)
                        ref[dst, c, rows, :] = sel(keep, v[GL * n:GL * (n + 1)], ref[dst, c, rows, :])

        def pad_rows(ref):
            at = pl.ds(0, NPAN)
            ref[at, :, pl.ds(0, 2 * SB), :] = ref[at, :, pl.ds(SB * KR - 1, 2 * SB), :]
            ref[at, :, pl.ds(SB * (KR + 2), 2 * SB), :] = ref[at, :, pl.ds(2 * SB + 1, 2 * SB), :]

        def corner_case(fn):
            for sa, sb in corners:
                @pl.when(jnp.logical_and(at_edge(sa), at_edge(2 + sb)))
                def _():
                    fn(sa, sb)

        def quad_geom(sa, sb):
            k0, s = (0, 0) if sa == 0 else (KR - H, SB - 1)
            lane0 = 0 if sb == 0 else LN - GL
            lane, idx = lanes_of((H, LN)), rows_of((H, LN))
            col = idx if sa == sb else H - 1 - idx
            masks = [NC * (lane - lane0) + c == col for c in PLANES]
            return k0, s, lane, masks, pl.ds(SB * (k0 + 2) + s, H, stride=SB)

        def beta_column(ref, first, sa, sb, r):
            k0, s, lane, masks, rows = quad_geom(sa, sb)
            kr = H + r if sa == 0 else KR - H - 1 - r
            tot = jnp.zeros((NPAN, H, LN), F32)
            for c in PLANES:
                line = ref[pl.ds(first, NPAN), c, pl.ds(SB * (kr + 2) + s, 1), :]
                tot = sel(wide(masks[c]), jnp.broadcast_to(line, tot.shape), tot)
            l_to, c_to = (GL - 1, NC - 1 - r) if sb == 0 else (LN - GL, r)
            return jnp.broadcast_to(jnp.sum(tot, axis=2, keepdims=True), tot.shape), wide(lane == l_to), c_to, rows

        def alpha_lines(ref, first, sa, sb, r):
            _, _, lane, masks, rows = quad_geom(sa, sb)
            l_from, c_from = (GL, r) if sb == 0 else (LN - GL - 1, NC - 1 - r)
            zero = jnp.zeros((NPAN, H, LN), F32)
            col = jnp.sum(sel(wide(lane == l_from), ref[pl.ds(first, NPAN), c_from, rows, :], zero), axis=2, keepdims=True)
            col = jnp.broadcast_to(col, zero.shape)
            return [jnp.sum(sel(wide(mask), col, zero), axis=1, keepdims=True) for mask in masks]

        def wide(mask):
            return jnp.broadcast_to(mask[None], (NPAN, *mask.shape))

        def fill_quadrant(src, sa, sb):
            columns = [beta_column(src, 0, sa, sb, r) for r in range(2)]
            lines = [alpha_lines(src, 0, sa, sb, r) for r in range(2)]
            for r in range(2):
                col, mask, c_to, rows = columns[r]
                src[:, c_to, rows, :] = sel(mask, col, src[:, c_to, rows, :])
                for c in PLANES:
                    CQ[:, r, c] = jnp.broadcast_to(lines[r][c], (NPAN, SB, LN))

        def fill_winds(sa, sb):
            sign = -1.0 if sa == sb else 1.0
            col, mask, c_to, rows = beta_column(WW, WA, sa, sb, 0)
            line = alpha_lines(WW, WB, sa, sb, 0)
            to_b, to_a = pl.ds(WB, NPAN), pl.ds(WA, NPAN)
            WW[to_b, c_to, rows, :] = sel(mask, sign * col, WW[to_b, c_to, rows, :])
            row_lane = lanes_of((NPAN, 1, LN))
            inside = row_lane < GL if sb == 0 else row_lane >= LN - GL
            row = pl.ds(SB * (H + 1), 1) if sa == 0 else pl.ds(SB * (KR - H + 3) - 1, 1)
            for c in PLANES:
                WW[to_a, c, row, :] = sel(inside, sign * line[c], WW[to_a, c, row, :])

        def roll_down(v):
            return pltpu.roll(v, LN - 1, 1)

        def roll_up(v):
            return pltpu.roll(v, 1, 1)

        def beta_rows(src, p, k0, scale):
            rows = pl.ds(SB * (k0 + 2), SB * BETA_ROWS)
            a0, a1, a2 = (src[p, c, rows, :] for c in PLANES)
            a2l, a0r, a1r = roll_up(a2), roll_down(a0), roll_down(a1)
            e0, e1, e2 = a2l + a1, a0 + a2, a1 + a0r
            g0, g1, g2 = 8.0 * a0 - e0, 8.0 * a1 - e1, 8.0 * a2 - e2
            g0r = 8.0 * a0r - (a2 + a1r)
            x0 = WW[WB + p, 0, rows, :] * (g0 + g1)
            x1 = WW[WB + p, 1, rows, :] * (g1 + g2)
            x2 = WW[WB + p, 2, rows, :] * (g2 + g0r)
            x2l = roll_up(x2)
            return jnp.stack([x0 - x2l, x1 - x0, x2 - x1]), jnp.stack([e0, e1, e2])

        def row_group(ref, p, k):
            return ref[p, :, pl.ds(SB * (k + 2), SB), :]

        def panel_pass(src, dst, p, scale, second):
            lane, sub = lanes_of((NC, SB, LN)), rows_of((NC, SB, LN))
            ghost_lane = jnp.logical_or(jnp.logical_and(at_edge(2), lane < GL),
                                        jnp.logical_and(at_edge(3), lane >= LN - GL))
            in_low = jnp.logical_and(ghost_lane, jnp.logical_and(at_edge(0), sub == 0))
            in_high = jnp.logical_and(ghost_lane, jnp.logical_and(at_edge(1), sub == SB - 1))

            def load(k):
                v = row_group(src, p, k)
                if k in (H - 2, H - 1):
                    return sel(in_low, CQ[p, H - 1 - k], v)
                if k in (KR - H, KR - H + 1):
                    return sel(in_high, CQ[p, k - (KR - H)], v)
                return v

            qm, q0, q1 = load(-2), load(-1), load(0)
            q2 = load(1)
            g0 = 8.0 * q0 - (qm + q1)
            e1 = q0 + q2
            g1 = 8.0 * q1 - e1
            x_low = row_group(WW, WA + p, -1) * (g0 + g1)
            q_now, e_now, g_now, q_next = q1, e1, g1, q2
            beta = None
            for k in range(KR):
                if k % BETA_ROWS == 0:
                    beta = beta_rows(src, p, k, scale)
                at = SB * (k % BETA_ROWS)
                tb, eb = (v[:, at:at + SB] for v in beta)
                q_far = load(k + 2)
                e_next = q_now + q_far
                g_next = 8.0 * q_next - e_next
                x_high = row_group(WW, WA + p, k) * (g_now + g_next)
                u = scale * (x_high - x_low + tb) - (e_now + eb)
                new = KK[1, :, pl.ds(SB * k, SB), :] * q_now - KK[0, :, pl.ds(SB * k, SB), :] * u
                if second:
                    new = 0.5 * (row_group(dst, p, k) + new)
                dst[p, :, pl.ds(SB * (k + 2), SB), :] = new
                x_low, q_now, e_now, g_now, q_next = x_high, q_next, e_next, g_next, q_far

        def stage(src, dst, scale, second, more, after=None):
            pad_rows(src)

            @pl.when(more)
            def _():
                corner_case(lambda sa, sb: fill_quadrant(src, sa, sb))

            @pl.loop(0, NPAN)
            def _(p):
                panel_pass(src, dst, p, scale, second)
                if after is not None:
                    after(p)

        load_fields([(a_in, WW, WA), (b_in, WW, WB)])
        is_cc = jnp.logical_and(jnp.logical_or(at_edge(0), at_edge(1)), jnp.logical_or(at_edge(2), at_edge(3)))
        pl.semaphore_wait(barrier, SB * NPAN - NPAN * sel(is_cc, 1, 0))

        @pl.loop(1, 3)
        def _(f):
            @pl.loop(0, NPAN)
            def _(p):
                send_panel(WW, (f - 1) * NPAN + p, WW, (2 - f) * NPAN + p, f, f + 1, p, True)
        load_fields([(q_in, QA, 0)])

        def finish_winds():
            metric()

            @pl.loop(1, 3)
            def _(f):
                for p in slots:
                    wait_copies(RECV, CRECV, recv_sem, crecv_sem, f + 1, p)

                @pl.loop(0, NPAN)
                def _(p):
                    unpack_cols(WW, (2 - f) * NPAN + p, f + 1, p)

            @pl.loop(1, 3)
            def _(f):
                @pl.loop(0, NPAN)
                def _(p):
                    unpack_rows(WW, (f - 1) * NPAN + p, f + 1, p)
                for p in slots:
                    wait_copies(SEND, CSEND, send_sem, csend_sem, f, p)
            corner_case(fill_winds)
            pad_rows(WW)
            face_scale = 0.5 / (12.0 * 0.5 * C_SPEED)

            @pl.loop(0, NPAN)
            def _(p):
                for c in PLANES:
                    low, high = pl.ds(SB, SB * (KR + 1)), pl.ds(2 * SB, SB * (KR + 1))
                    WW[WA + p, c, low, :] = face_scale * (WW[WA + p, c, low, :] + WW[WA + p, c, high, :])
                rows = pl.ds(2 * SB, SB * KR)
                b0, b1, b2 = (WW[WB + p, c, rows, :] for c in PLANES)
                WW[WB + p, 0, rows, :] = face_scale * (b0 + b1)
                WW[WB + p, 1, rows, :] = face_scale * (b1 + b2)
                WW[WB + p, 2, rows, :] = face_scale * (b2 + roll_down(b0))

        def metric():
            ridx = rows_of((SB * KR, LN))
            gi = tx * tile_rows + lax.rem(ridx, SB) * KR + lax.div(ridx, SB) - H
            gi = sel(gi < 0, -1 - gi, sel(gi >= cells, 2 * cells - 1 - gi, gi))
            tan_a = small_tan((gi.astype(F32) + 0.5) * dalpha - 0.25 * math.pi)
            for c in PLANES:
                gj = ty * tile_rows + 3 * lanes_of((SB, LN)) + c - H
                gj = sel(gj < 0, -1 - gj, sel(gj >= cells, 2 * cells - 1 - gj, gj))
                tan_b = small_tan((gj.astype(F32) + 0.5) * dalpha - 0.25 * math.pi)[0:1, :]
                a_sq, b_sq = tan_a * tan_a, tan_b * tan_b
                r_sq = 1.0 + a_sq + b_sq
                sqrt_g = (1.0 + a_sq) * (1.0 + b_sq) / (r_sq * jnp.sqrt(r_sq))
                KK[0, c] = (0.5 * C_SPEED * CFL_STEP) / sqrt_g
                KK[1, c] = 1.0 - 4.0 * KK[0, c]

        @pl.loop(0, n_blocks)
        def _(b):
            fr = lax.rem(b, 2)

            @pl.when(b == 0)
            def _():
                @pl.loop(0, NPAN)
                def _(p):
                    send_panel(QA, p, QA, p, 0, 0, p, False)

            @pl.when(b == 0)
            def _():
                finish_winds()

            for p in slots:
                wait_copies(RECV, CRECV, recv_sem, crecv_sem, fr, p)
                unpack_cols(QA, p, fr, p)
                unpack_rows(QA, p, fr, p)
            for p in slots:
                wait_copies(SEND, CSEND, send_sem, csend_sem, 0, p)
            end = lax.div((b + 1) * steps, n_blocks)

            @pl.loop(lax.div(b * steps, n_blocks), end)
            def _(t):
                scale = ws_ref[t]
                stage(QA, QB, scale, False, True)

                def after(p):
                    @pl.when(jnp.logical_and(t + 1 == end, b + 1 < n_blocks))
                    def _():
                        send_panel(QA, p, QA, p, 0, 1 - fr, p, False)
                stage(QB, QA, scale, True, t + 1 < end, after)

        store_field(QA)

    return kernel


def solution(mesh):
    tile_count = mesh.shape['tx']
    field_spec = P(('member', 'panel'), 'tx', 'ty')
    wind_spec = P('panel', 'tx', 'ty')

    def local_run(tracer, wind_a, wind_b, wind_scale):
        steps = wind_scale.shape[0]
        n_blocks = -(-steps // STEPS_PER_BLOCK)
        ext = SB * KR
        block = pl.BlockSpec((NPAN, ext, ext), lambda n: (0, 0, 0))
        dma = pltpu.SemaphoreType.DMA
        return pl.pallas_call(
            make_kernel(tile_count, steps, n_blocks, tracer.shape[1]),
            grid=(1,),
            out_shape=jax.ShapeDtypeStruct(tracer.shape, F32),
            in_specs=[pl.BlockSpec(memory_space=pltpu.SMEM), block, block, block],
            out_specs=block,
            scratch_shapes=[
                pltpu.VMEM((NPAN, NC, ext + 32, LN), F32),
                pltpu.VMEM((NPAN, NC, ext + 32, LN), F32),
                pltpu.VMEM((2 * NPAN, NC, ext + 32, LN), F32),
                pltpu.VMEM((NPAN, 2, NC, SB, LN), F32),
                pltpu.VMEM((2, NC, ext, LN), F32),
                pltpu.VMEM((2 * NC, ext + 32, LN), F32),
                pltpu.VMEM((2 * NC, ext + 32, LN), F32),
                pltpu.VMEM((9, LN, LN), F32),
                pltpu.VMEM((3, NPAN, 4, NC, H, LN), F32),
                pltpu.VMEM((4, NPAN, 4, NC, H, LN), F32),
                pltpu.VMEM((3, NPAN, 4, H, LN), F32),
                pltpu.VMEM((4, NPAN, 4, H, LN), F32),
                *[dma((n, NPAN, 4)) for n in (3, 4, 3, 4)],
            ],
            compiler_params=pltpu.CompilerParams(collective_id=0, has_side_effects=True, vmem_limit_bytes=60 * 1024 * 1024),
            cost_estimate=pl.CostEstimate(flops=10 ** 9, bytes_accessed=10 ** 7, transcendentals=0),
        )(wind_scale, tracer, wind_a, wind_b)

    return jax.shard_map(local_run, mesh=mesh, in_specs=(field_spec, wind_spec, wind_spec, P()),
                         out_specs=field_spec, check_vma=False)
```
